64 devices in a mesh: dp: 4 (over x, y), cp: 16 (over z, core).
Axes of the slice: x: 2, y: 2, z: 8, core: 2. Of those that a mesh axis runs over, the one named last changes fastest.
The devices are a block of a 4x4x8 slice.
Arguments:
- tokens: bfloat16 [8, 3072, 2048], P('dp', 'cp'), parts along dimension 0
- positions: int32 [8, 3072], P('dp', 'cp'), parts along dimension 0
- norm_gain: float32 [2048], replicated
- w_query: bfloat16 [2048, 2048], replicated
- w_key: bfloat16 [2048, 256], replicated
- w_value: bfloat16 [2048, 256], replicated
- w_out: bfloat16 [2048, 2048], replicated
- d_out: bfloat16 [8, 3072, 2048], P('dp', 'cp'), parts along dimension 0
Outputs:
- output 1: bfloat16 [8, 3072, 2048], P('dp', 'cp'), parts along dimension 0
- output 2: bfloat16 [8, 3072, 2048], P('dp', 'cp'), parts along dimension 0
- output 3: float32 [8192, 2048], P('dp'), parts along dimension 0
- output 4: float32 [8192, 256], P('dp'), parts along dimension 0
- output 5: float32 [8192, 256], P('dp'), parts along dimension 0
- output 6: float32 [8192, 2048], P('dp'), parts along dimension 0
- output 7: float32 [8192], P('dp'), parts along dimension 0
There are 4 independent parts. The reference program is written for one: setup_inputs(seed, part) draws one part's arguments, and reference() takes and returns one part's arrays. A program takes and returns all parts, laid end to end along the dimension named above; an argument that names none is the same for every part.
All inputs are finite; a program needn't handle non-finite values.
Results may differ from the reference program's by a relative error of at most 0.012375.
Values are sent between devices in bfloat16 or wider.
A program may use at most 768 MiB of HBM per device.

```python
import jax
import jax.numpy as jnp
from jax import lax

SEQ_COUNT = 2
SEQ_LEN = 3072
MODEL_DIM = 2048
NUM_HEADS = 8
HEAD_DIM = 256
GROUP_SIZE = 16
QUERY_BLOCK = 32
PIECE_LEN = SEQ_LEN // (2 * GROUP_SIZE)
NORM_EPS = 1e-6
ROPE_BASE = 10000.0
NEG_BIG = -1e30


def setup_inputs(seed: int = 0, part: int = 0) -> dict:
    root_key = jax.random.key(seed)
    part_key = jax.random.fold_in(root_key, part)
    key_x, key_pos, key_dy = jax.random.split(part_key, 3)
    key_gain, key_q, key_k, key_v, key_o = jax.random.split(jax.random.fold_in(root_key, 100003), 5)
    tokens = jax.random.normal(key_x, (SEQ_COUNT, SEQ_LEN, MODEL_DIM), jnp.float32).astype(jnp.bfloat16)
    pos_gaps = jax.random.randint(key_pos, (SEQ_COUNT, SEQ_LEN), 1, 3, dtype=jnp.int32)
    true_pos = jnp.cumsum(pos_gaps, axis=1) - 1
    pieces = true_pos.reshape(SEQ_COUNT, 2 * GROUP_SIZE, PIECE_LEN)
    front_pieces = pieces[:, :GROUP_SIZE]
    back_pieces = pieces[:, GROUP_SIZE:][:, ::-1]
    positions = jnp.stack([front_pieces, back_pieces], axis=2).reshape(SEQ_COUNT, SEQ_LEN).astype(jnp.int32)
    in_scale = MODEL_DIM ** -0.5
    q_width = NUM_HEADS * HEAD_DIM
    norm_gain = jax.random.uniform(key_gain, (MODEL_DIM,), jnp.float32, 0.5, 1.5)
    w_query = (jax.random.normal(key_q, (MODEL_DIM, q_width), jnp.float32) * (2.0 * in_scale)).astype(jnp.bfloat16)
    w_key = (jax.random.normal(key_k, (MODEL_DIM, HEAD_DIM), jnp.float32) * (2.0 * in_scale)).astype(jnp.bfloat16)
    w_value = (jax.random.normal(key_v, (MODEL_DIM, HEAD_DIM), jnp.float32) * (2.0 * in_scale)).astype(jnp.bfloat16)
    w_out = (jax.random.normal(key_o, (q_width, MODEL_DIM), jnp.float32) * q_width ** -0.5).astype(jnp.bfloat16)
    d_out = jax.random.normal(key_dy, (SEQ_COUNT, SEQ_LEN, MODEL_DIM), jnp.float32).astype(jnp.bfloat16)
    return {'tokens': tokens, 'positions': positions, 'norm_gain': norm_gain, 'w_query': w_query, 'w_key': w_key, 'w_value': w_value, 'w_out': w_out, 'd_out': d_out}


def layer_norm(tokens, norm_gain):
    x_float = tokens.astype(jnp.float32)
    centered = x_float - jnp.mean(x_float, axis=-1, keepdims=True)
    inv_std = lax.rsqrt(jnp.mean(centered * centered, axis=-1, keepdims=True) + NORM_EPS)
    x_hat = centered * inv_std
    return (x_hat * norm_gain).astype(jnp.bfloat16), x_hat, inv_std


def layer_norm_grad(d_h, x_hat, inv_std, norm_gain):
    d_hat = d_h * norm_gain
    mean_d = jnp.mean(d_hat, axis=-1, keepdims=True)
    mean_dx = jnp.mean(d_hat * x_hat, axis=-1, keepdims=True)
    return inv_std * (d_hat - mean_d - x_hat * mean_dx)


def rope_tables(positions, head_dim):
    half_dim = head_dim // 2
    inv_freq = ROPE_BASE ** (-(jnp.arange(half_dim, dtype=jnp.float32) * (2.0 / head_dim)))
    angles = positions.astype(jnp.float32)[..., None] * inv_freq
    return jnp.cos(angles), jnp.sin(angles)


def rotate(values, cos_t, sin_t):
    half_dim = values.shape[-1] // 2
    front_half, back_half = values[..., :half_dim], values[..., half_dim:]
    return jnp.concatenate([front_half * cos_t - back_half * sin_t, back_half * cos_t + front_half * sin_t], axis=-1)


def rotate_back(grad_vals, cos_t, sin_t):
    half_dim = grad_vals.shape[-1] // 2
    front_half, back_half = grad_vals[..., :half_dim], grad_vals[..., half_dim:]
    return jnp.concatenate([front_half * cos_t + back_half * sin_t, back_half * cos_t - front_half * sin_t], axis=-1)


def seq_attention(seq_in):
    q_seq, k_seq, v_seq, pos_seq, da_seq = seq_in
    seq_len, num_heads, head_dim = q_seq.shape
    n_blocks = seq_len // QUERY_BLOCK
    score_scale = head_dim ** -0.5
    k_float = k_seq.astype(jnp.float32)
    v_float = v_seq.astype(jnp.float32)
    q_blocks = q_seq.reshape(n_blocks, QUERY_BLOCK, num_heads, head_dim)
    pos_blocks = pos_seq.reshape(n_blocks, QUERY_BLOCK)
    da_blocks = da_seq.reshape(n_blocks, QUERY_BLOCK, num_heads, head_dim)

    def block_scores(q_blk, pos_blk):
        scores = jnp.einsum('qhd,kd->qhk', q_blk.astype(jnp.float32), k_float) * score_scale
        key_mask = pos_seq[None, None, :] <= pos_blk[:, None, None]
        return jnp.where(key_mask, scores, NEG_BIG)

    def fwd_block(blk_in):
        q_blk, pos_blk = blk_in
        scores = block_scores(q_blk, pos_blk)
        row_max = jnp.max(scores, axis=-1)
        exp_scores = jnp.exp(scores - row_max[..., None])
        row_sum = jnp.sum(exp_scores, axis=-1)
        weighted = jnp.einsum('qhk,kd->qhd', exp_scores.astype(jnp.bfloat16).astype(jnp.float32), v_float)
        return (weighted / row_sum[..., None]).astype(jnp.bfloat16), row_max, row_sum

    attn_blocks, max_blocks, sum_blocks = lax.map(fwd_block, (q_blocks, pos_blocks))

    def bwd_block(kv_grads, blk_in):
        dk_acc, dv_acc = kv_grads
        q_blk, pos_blk, da_blk, attn_blk, max_blk, sum_blk = blk_in
        scores = block_scores(q_blk, pos_blk)
        attn_p = jnp.exp(scores - max_blk[..., None]) / sum_blk[..., None]
        da_float = da_blk.astype(jnp.float32)
        d_probs = jnp.einsum('qhd,kd->qhk', da_float, v_float)
        out_delta = jnp.sum(da_float * attn_blk.astype(jnp.float32), axis=-1)
        d_scores = (attn_p * (d_probs - out_delta[..., None])).astype(jnp.bfloat16).astype(jnp.float32)
        dq_blk = jnp.einsum('qhk,kd->qhd', d_scores, k_float) * score_scale
        dk_acc = dk_acc + jnp.einsum('qhk,qhd->kd', d_scores, q_blk.astype(jnp.float32)) * score_scale
        dv_acc = dv_acc + jnp.einsum('qhk,qhd->kd', attn_p.astype(jnp.bfloat16).astype(jnp.float32), da_float)
        return (dk_acc, dv_acc), dq_blk

    zero_kv = jnp.zeros((seq_len, head_dim), jnp.float32)
    scan_out = lax.scan(bwd_block, (zero_kv, zero_kv), (q_blocks, pos_blocks, da_blocks, attn_blocks, max_blocks, sum_blocks))
    dk_acc, dv_acc = scan_out[0]
    dq_blocks = scan_out[1]
    return (attn_blocks.reshape(seq_len, num_heads, head_dim), dq_blocks.reshape(seq_len, num_heads, head_dim), dk_acc, dv_acc)


def reference(tokens, positions, norm_gain, w_query, w_key, w_value, w_out, d_out):
    n_seq, seq_len, model_dim = tokens.shape
    head_dim = w_key.shape[1]
    num_heads = w_query.shape[1] // head_dim
    q_width = num_heads * head_dim
    n_rows = n_seq * seq_len
    h_norm, x_hat, inv_std = layer_norm(tokens, norm_gain)
    h_flat = h_norm.reshape(n_rows, model_dim)
    cos_t, sin_t = rope_tables(positions, head_dim)
    cos_h, sin_h = cos_t[:, :, None, :], sin_t[:, :, None, :]
    q_lin = jnp.dot(h_flat, w_query, preferred_element_type=jnp.float32).reshape(n_seq, seq_len, num_heads, head_dim)
    q_rot = rotate(q_lin, cos_h, sin_h).astype(jnp.bfloat16)
    k_lin = jnp.dot(h_flat, w_key, preferred_element_type=jnp.float32).reshape(n_seq, seq_len, head_dim)
    k_rot = rotate(k_lin, cos_t, sin_t).astype(jnp.bfloat16)
    v_proj = jnp.dot(h_flat, w_value, preferred_element_type=jnp.float32).astype(jnp.bfloat16).reshape(n_seq, seq_len, head_dim)
    dy_flat = d_out.reshape(n_rows, model_dim)
    d_attn = jnp.dot(dy_flat, w_out.T, preferred_element_type=jnp.float32).astype(jnp.bfloat16).reshape(n_seq, seq_len, num_heads, head_dim)
    attn_out, dq_acc, dk_acc, dv_acc = lax.map(seq_attention, (q_rot, k_rot, v_proj, positions, d_attn))
    attn_flat = attn_out.reshape(n_rows, q_width)
    o_proj = jnp.dot(attn_flat, w_out, preferred_element_type=jnp.float32).astype(jnp.bfloat16)
    out_y = (tokens.astype(jnp.float32) + o_proj.reshape(n_seq, seq_len, model_dim).astype(jnp.float32)).astype(jnp.bfloat16)
    grad_wo = jnp.dot(attn_flat.T, dy_flat, preferred_element_type=jnp.float32)
    dq_pre = rotate_back(dq_acc, cos_h, sin_h).astype(jnp.bfloat16).reshape(n_rows, q_width)
    dk_pre = rotate_back(dk_acc, cos_t, sin_t).astype(jnp.bfloat16).reshape(n_rows, head_dim)
    dv_pre = dv_acc.astype(jnp.bfloat16).reshape(n_rows, head_dim)
    grad_wq = jnp.dot(h_flat.T, dq_pre, preferred_element_type=jnp.float32)
    grad_wk = jnp.dot(h_flat.T, dk_pre, preferred_element_type=jnp.float32)
    grad_wv = jnp.dot(h_flat.T, dv_pre, preferred_element_type=jnp.float32)
    d_h = (jnp.dot(dq_pre, w_query.T, preferred_element_type=jnp.float32) + jnp.dot(dk_pre, w_key.T, preferred_element_type=jnp.float32) + jnp.dot(dv_pre, w_value.T, preferred_element_type=jnp.float32)).reshape(n_seq, seq_len, model_dim)
    grad_x = (d_out.astype(jnp.float32) + layer_norm_grad(d_h, x_hat, inv_std, norm_gain)).astype(jnp.bfloat16)
    grad_gain = jnp.sum(d_h * x_hat, axis=(0, 1))
    return out_y, grad_x, grad_wq, grad_wk, grad_wv, grad_wo, grad_gain
```

```python
import functools

import jax
import jax.numpy as jnp
from jax import lax
from jax.experimental import pallas as pl
from jax.experimental.pallas import tpu as pltpu
from jax.sharding import PartitionSpec as P

NORM_EPS = 1e-6
ROPE_BASE = 10000.0
NEG_BIG = -1e30
LOG2_E = 1.4426950408889634
PIECES_PER_BLOCK = 4
VMEM_LIMIT = 60 * 1024 * 1024

NT = (((1,), (1,)), ((), ()))
TN = (((0,), (0,)), ((), ()))
NN = (((1,), (0,)), ((), ()))


def dot(lhs, rhs, dims):
    return lax.dot_general(lhs, rhs, dims, preferred_element_type=jnp.float32)


def rope_tables(positions, head_dim):
    half_dim = head_dim // 2
    inv_freq = ROPE_BASE ** (-(jnp.arange(half_dim, dtype=jnp.float32) * (2.0 / head_dim)))
    angles = positions.astype(jnp.float32)[..., None] * inv_freq
    return jnp.cos(angles), jnp.sin(angles)


def rotate(values, cos_t, sin_t):
    half_dim = values.shape[-1] // 2
    front_half, back_half = values[..., :half_dim], values[..., half_dim:]
    return jnp.concatenate([front_half * cos_t - back_half * sin_t, back_half * cos_t + front_half * sin_t], axis=-1)


def rotate_back(grad_vals, cos_t, sin_t):
    half_dim = grad_vals.shape[-1] // 2
    front_half, back_half = grad_vals[..., :half_dim], grad_vals[..., half_dim:]
    return jnp.concatenate([front_half * cos_t + back_half * sin_t, back_half * cos_t - front_half * sin_t], axis=-1)


def norm_kv_kernel(x_ref, gain_ref, wk_ref, wv_ref, cos_ref, sin_ref, h_ref, kv_ref):
    head_dim = wk_ref.shape[1]
    x_float = x_ref[...].astype(jnp.float32)
    centered = x_float - jnp.mean(x_float, axis=-1, keepdims=True)
    inv_std = lax.rsqrt(jnp.mean(centered * centered, axis=-1, keepdims=True) + NORM_EPS)
    h_norm = (centered * inv_std * gain_ref[...]).astype(jnp.bfloat16)
    h_ref[...] = h_norm
    k_lin = dot(h_norm, wk_ref[...], NN)
    kv_ref[:, :head_dim] = rotate(k_lin, cos_ref[...], sin_ref[...]).astype(jnp.bfloat16)
    kv_ref[:, head_dim:] = dot(h_norm, wv_ref[...], NN).astype(jnp.bfloat16)


def entry_barrier(peers):
    barrier = pltpu.get_barrier_semaphore()
    for peer in peers:
        pl.semaphore_signal(barrier, inc=1, device_id={'cp': peer}, device_id_type=pl.DeviceIdType.MESH)
    pl.semaphore_wait(barrier, len(peers))


def remote(src, dst, send_sem, recv_sem, peer):
    return pltpu.make_async_remote_copy(src_ref=src, dst_ref=dst, send_sem=send_sem, recv_sem=recv_sem,
                                        device_id={'cp': peer}, device_id_type=pl.DeviceIdType.MESH)


def ring_place(n_dev):
    me = lax.axis_index('cp')
    n_chip = n_dev // 2
    chip, core = lax.div(me, 2), lax.rem(me, 2)
    after = lax.rem(chip + 1, n_chip) * 2 + core
    before = lax.rem(chip + n_chip - 1, n_chip) * 2 + core
    partner = chip * 2 + 1 - core
    return n_chip, chip, core, (after, before), partner


def chunk_at(chip, step, way, n_chip):
    if way == 0:
        return lax.rem(chip + 2 * n_chip - 1 - step, n_chip)
    return lax.rem(chip + 1 + step, n_chip)


class RingReduce:
    def __init__(self, n_chip, peers, make_local, local_scr, slots, send_sems, recv_sems):
        self.n_chip, self.peers, self.make_local = n_chip, peers, make_local
        self.local_scr, self.slots, self.send_sems, self.recv_sems = local_scr, slots, send_sems, recv_sems
        self.each = [(sub, way) for sub in range(slots.shape[2]) for way in range(2)]

    def hop(self, step, way, sub, first=False):
        src = self.local_scr.at[way, sub] if first else self.slots.at[way, step - 1, sub]
        return remote(src, self.slots.at[way, step, sub], self.send_sems.at[way, sub], self.recv_sems.at[way, step, sub], self.peers[way])

    def first(self):
        self.make_local(0)
        for sub, way in self.each:
            self.hop(0, way, sub, True).start()

    def middle(self, step, last=False):
        for sub, way in self.each:
            self.hop(step - 1, way, sub, isinstance(step, int) and step == 1).wait_send()
        self.make_local(step)
        for sub, way in self.each:
            self.hop(step - 1, way, sub, isinstance(step, int) and step == 1).wait_recv()
            self.slots[way, step - 1, sub] = self.slots[way, step - 1, sub] + self.local_scr[way, sub]
            if not last:
                self.hop(step, way, sub).start()

    def last(self):
        self.middle(self.n_chip - 1, True)


class RingGather:
    def __init__(self, n_chip, peers, partner, own, place, n_sub, send_sems, recv_sems, mate_send, mate_recv):
        self.n_chip, self.peers, self.partner, self.own, self.place = n_chip, peers, partner, own, place
        self.send_sems, self.recv_sems, self.mate_send, self.mate_recv = send_sems, recv_sems, mate_send, mate_recv
        self.each = [(sub, way) for sub in range(n_sub) for way in range(2)]

    def onward(self, step, way, sub, first=False):
        src = self.own(way, sub) if first else self.place(step, way, sub)
        return remote(src, self.place(step, way, sub), self.send_sems.at[way, sub], self.recv_sems.at[way, step, sub], self.peers[way])

    def across(self, step, way, sub, first=False):
        src = self.own(way, sub) if first else self.place(step, way, sub)
        return remote(src, self.place(step, way, sub), self.mate_send.at[way, sub], self.mate_recv.at[way, step, sub], self.partner)

    def first(self):
        for sub, way in self.each:
            self.onward(0, way, sub, True).start()
            self.across(0, way, sub, True).start()

    def middle(self, step, last=False):
        after_first = isinstance(step, int) and step == 1
        for sub, way in self.each:
            self.onward(step - 1, way, sub, after_first).wait_send()
            self.onward(step - 1, way, sub, after_first).wait_recv()
            if not last:
                self.onward(step, way, sub).start()
            self.across(step - 1, way, sub, after_first).wait_send()
            self.across(step, way, sub).start()

    def last(self):
        self.middle(self.n_chip - 1, True)

    def drain(self):
        for sub, way in self.each:
            self.across(self.n_chip - 1, way, sub).wait_send()

        def body(step, _):
            for sub, way in self.each:
                self.across(step, way, sub).wait_recv()

        lax.fori_loop(0, self.n_chip, body, None)


def owner_at(chip, step, way, n_chip):
    if way == 0:
        return lax.rem(chip + n_chip - step, n_chip)
    return lax.rem(chip + step, n_chip)


def gather_heads_kernel(n_dev, h_ref, dy_ref, kv_ref, wq_ref, wo_ref, cos_ref, sin_ref, all_ref, q_ref, da_ref, wq_buf, wo_buf, w_sems,
                        send_sems, recv_sems, mate_send, mate_recv):
    n_chip, chip, core, peers, partner = ring_place(n_dev)
    n_seq = all_ref.shape[0]
    half_len = all_ref.shape[1] // (2 * n_dev)
    head_dim = wq_buf.shape[2]
    num_heads = q_ref.shape[1]
    q_shape = (q_ref.shape[0], half_len, head_dim)

    def weights(head, slot):
        cols = pl.ds(pl.multiple_of(head * head_dim, head_dim), head_dim)
        return (pltpu.make_async_copy(wq_ref.at[:, cols], wq_buf.at[slot], w_sems.at[0, slot]),
                pltpu.make_async_copy(wo_ref.at[cols, :], wo_buf.at[slot], w_sems.at[1, slot]))

    for copy in weights(0, 0):
        copy.start()
    entry_barrier(peers + (partner,))

    def piece_rows(dev, way):
        piece = dev if way == 0 else 2 * n_dev - 1 - dev
        return pl.ds(pl.multiple_of(piece * half_len, half_len), half_len)

    def place(step, way, seq):
        return all_ref.at[seq, piece_rows(owner_at(chip, step, way, n_chip) * 2 + core, way)]

    def own(way, seq):
        return kv_ref.at[pl.ds((2 * seq + way) * half_len, half_len)]

    ring = RingGather(n_chip, peers, partner, own, place, n_seq, send_sems, recv_sems, mate_send, mate_recv)
    ring.first()
    me = chip * 2 + core
    for seq in range(n_seq):
        for way in range(2):
            all_ref[seq, piece_rows(me, way), :] = kv_ref[(2 * seq + way) * half_len:(2 * seq + way + 1) * half_len, :]

    def project(head, slot):
        @pl.when(head < num_heads)
        def _():
            for copy in weights(head, slot):
                copy.wait()

            @pl.when(head + 1 < num_heads)
            def _():
                for copy in weights(head + 1, 1 - slot):
                    copy.start()

            q_lin = dot(h_ref[...], wq_buf[slot], NN)
            q_ref[:, head] = rotate(q_lin, cos_ref[...], sin_ref[...]).astype(jnp.bfloat16).reshape(q_shape)
            da_ref[:, head] = dot(dy_ref[...], wo_buf[slot], NT).astype(jnp.bfloat16).reshape(q_shape)

    project(0, 0)
    ring.middle(1)

    def body(step, _):
        project(step - 1, lax.rem(step - 1, 2))
        ring.middle(step)

    lax.fori_loop(2, n_chip - 1, body, None)
    project(n_chip - 2, (n_chip - 2) % 2)
    ring.last()
    project(n_chip - 1, (n_chip - 1) % 2)
    ring.drain()


def causal_mask(shape, key_start, query_start, half_len):
    key_idx = key_start + lax.broadcasted_iota(jnp.int32, shape, 0)
    query_idx = query_start + lax.rem(lax.broadcasted_iota(jnp.int32, shape, 1), half_len)
    return key_idx <= query_idx


def attend_kernel(n_dev, q_ref, kv_ref, da_ref, a_ref, lse_ref, delta_ref, acc_scr, max_scr, sum_scr):
    rows, head_dim = q_ref.shape[1:]
    half_len = kv_ref.shape[1] // (2 * n_dev)
    num_heads = rows // half_len
    key_len = PIECES_PER_BLOCK * half_len
    scale = LOG2_E * head_dim ** -0.5
    me = lax.axis_index('cp')
    for group in range(2):
        piece = me if group == 0 else 2 * n_dev - 1 - me
        last = lax.div(piece, PIECES_PER_BLOCK)
        max_scr[...] = jnp.full_like(max_scr, NEG_BIG)
        sum_scr[...] = jnp.zeros_like(sum_scr)
        acc_scr[...] = jnp.zeros_like(acc_scr)

        def block(step, masked, group=group, piece=piece):
            start = pl.multiple_of(step * key_len, key_len)
            keys = pl.ds(start, key_len)
            scores = dot(kv_ref[0, keys, :head_dim], q_ref[group], NT) * scale
            if masked:
                scores = jnp.where(causal_mask(scores.shape, start, piece * half_len, half_len), scores, NEG_BIG)
            old_max = max_scr[...]
            new_max = jnp.maximum(old_max, jnp.max(scores, axis=0, keepdims=True))
            rescale = jnp.exp2(old_max - new_max)
            probs = jnp.exp2(scores - new_max)
            max_scr[...] = new_max
            sum_scr[...] = sum_scr[...] * rescale + jnp.sum(probs, axis=0, keepdims=True)
            acc_scr[...] = acc_scr[...] * rescale + dot(kv_ref[0, keys, head_dim:], probs.astype(jnp.bfloat16), TN)

        lax.fori_loop(0, last, lambda step, _: block(step, False), None)
        block(last, True)
        attn = (acc_scr[...] / sum_scr[...]).T.astype(jnp.bfloat16)
        lse_ref[group] = max_scr[...] + jnp.log2(sum_scr[...])
        prod = attn.astype(jnp.float32) * da_ref[group].astype(jnp.float32)
        prod = prod[:, :head_dim // 2] + prod[:, head_dim // 2:]
        delta_ref[group] = jnp.sum(prod.T, axis=0, keepdims=True)
        for head in range(num_heads):
            a_ref[group, :, head * head_dim:(head + 1) * head_dim] = attn[head * half_len:(head + 1) * half_len, :]


def attend_grad_kernel(n_dev, q_ref, kv_ref, da_ref, lse_ref, delta_ref, cos_ref, sin_ref, a_ref, dy_ref, z_ref, wo_ref,
                       q_scr, da_scr, kv_scr, dq_scr, dkv_scr, mate_scr, kv_local, kv_slots, a_scr, dy_scr, wo_local, wo_slots,
                       load_sems, swap_send, swap_recv, kv_send, kv_recv, mate_send, mate_recv, wo_send, wo_recv):
    n_chip, chip, core, peers, partner = ring_place(n_dev)
    me = chip * 2 + core
    rows, head_dim = q_scr.shape[1:]
    n_seq, seq_len, kv_width = dkv_scr.shape
    half_len = seq_len // (2 * n_dev)
    num_heads = rows // half_len
    q_width = num_heads * head_dim
    n_rows = a_ref.shape[0]
    key_len = PIECES_PER_BLOCK * half_len
    scale = LOG2_E * head_dim ** -0.5
    dy_cols = dy_scr.shape[1]
    mine, other = pl.ds(0, n_rows), pl.ds(n_rows, n_rows)

    def cols(which, size):
        return pl.ds(pl.multiple_of(which * size, size), size)

    loads = [
        pltpu.make_async_copy(a_ref, a_scr.at[mine], load_sems.at[0]),
        pltpu.make_async_copy(dy_ref.at[:, cols(core, dy_cols)], dy_scr.at[mine], load_sems.at[1]),
        pltpu.make_async_copy(q_ref, q_scr, load_sems.at[2]),
        pltpu.make_async_copy(da_ref, da_scr, load_sems.at[3]),
        pltpu.make_async_copy(kv_ref, kv_scr, load_sems.at[4]),
    ]
    for load in loads:
        load.start()
    entry_barrier(peers + (partner,))
    swaps = [
        remote(a_ref, a_scr.at[other], swap_send.at[0], swap_recv.at[0], partner),
        remote(dy_ref.at[:, cols(1 - core, dy_cols)], dy_scr.at[other], swap_send.at[1], swap_recv.at[1], partner),
    ]
    for swap in swaps:
        swap.start()
    dkv_scr[...] = jnp.zeros_like(dkv_scr)
    loads[0].wait()
    loads[1].wait()
    for swap in swaps:
        swap.wait_recv()

    def wo_local_term(step):
        n_sub, sub_len = wo_local.shape[1:3]
        way_len = n_sub * sub_len
        for way in range(2):
            first = chunk_at(chip, step, way, n_chip) * (2 * way_len) + way * way_len
            part = dot(a_scr[:, pl.ds(pl.multiple_of(first, way_len), way_len)], dy_scr[...], TN)
            for sub in range(n_sub):
                wo_local[way, sub] = part[sub * sub_len:(sub + 1) * sub_len, :]

    def piece_rows(dev, sub):
        piece = dev if sub == 0 else 2 * n_dev - 1 - dev
        return pl.ds(pl.multiple_of(piece * half_len, half_len), half_len)

    def mate_copy(step, way, sub):
        dev = chunk_at(chip, step, way, n_chip) * 2 + 1 - core
        return remote(dkv_scr.at[way, piece_rows(dev, sub)], mate_scr.at[way, step, sub], mate_send.at[way, step, sub], mate_recv.at[way, step, sub], partner)

    def kv_local_term(step):
        for sub in range(2):
            for way in range(2):
                mate_copy(step, way, sub).wait_recv()
                dev = chunk_at(chip, step, way, n_chip) * 2 + core
                kv_local[way, sub] = dkv_scr[way, piece_rows(dev, sub), :] + mate_scr[way, step, sub]

    wo_ring = RingReduce(n_chip, peers, wo_local_term, wo_local, wo_slots, wo_send, wo_recv)
    kv_ring = RingReduce(n_chip, peers, kv_local_term, kv_local, kv_slots, kv_send, kv_recv)

    def attend_seq(seq):
        def one_group(group, _):
            index = 2 * seq + group
            piece = me + group * (2 * n_dev - 1 - 2 * me)
            last = lax.div(piece, PIECES_PER_BLOCK)
            dq_scr[...] = jnp.zeros_like(dq_scr)

            def block(step, masked):
                start = pl.multiple_of(step * key_len, key_len)
                keys = pl.ds(start, key_len)
                k_blk, v_blk = kv_scr[seq, keys, :head_dim], kv_scr[seq, keys, head_dim:]
                probs = jnp.exp2(dot(k_blk, q_scr[index], NT) * scale - lse_ref[index])
                if masked:
                    probs = jnp.where(causal_mask(probs.shape, start, piece * half_len, half_len), probs, 0.0)
                d_scores = (probs * (dot(v_blk, da_scr[index], NT) - delta_ref[index])).astype(jnp.bfloat16)
                dq_scr[...] += dot(k_blk, d_scores, TN)
                dkv_scr[seq, keys, :head_dim] += dot(d_scores, q_scr[index], NN) * head_dim ** -0.5
                dkv_scr[seq, keys, head_dim:] += dot(probs.astype(jnp.bfloat16), da_scr[index], NN)

            lax.fori_loop(0, last, lambda step, _: block(step, False), None)
            block(last, True)
            dq = dq_scr[...].T * head_dim ** -0.5
            out_rows = pl.ds(pl.multiple_of(index * half_len, half_len), half_len)
            cos_t, sin_t = cos_ref[out_rows, :], sin_ref[out_rows, :]
            for head in range(num_heads):
                dq_head = dq[head * half_len:(head + 1) * half_len, :]
                z_ref[out_rows, head * head_dim:(head + 1) * head_dim] = rotate_back(dq_head, cos_t, sin_t).astype(jnp.bfloat16)

        lax.fori_loop(0, 2, one_group, None)

        def send_mate(step, _):
            for sub in range(2):
                mate_copy(step, seq, sub).start()

        lax.fori_loop(0, n_chip, send_mate, None)

    wo_ring.first()
    for load in loads[2:]:
        load.wait()
    attend_seq(0)
    wo_ring.middle(1)
    attend_seq(1)
    wo_ring.middle(2)
    kv_ring.first()
    wo_ring.middle(3)
    kv_ring.middle(1)

    def both(step, _):
        wo_ring.middle(step + 2)
        kv_ring.middle(step)

    lax.fori_loop(2, n_chip - 3, both, None)
    wo_ring.last()
    for way in range(2):
        for sub in range(wo_local.shape[1]):
            wo_ref[way, sub] = wo_slots[way, n_chip - 2, sub]
    kv_ring.middle(n_chip - 3)
    kv_ring.middle(n_chip - 2)
    kv_ring.last()
    for way in range(2):
        for sub in range(2):
            out_rows = slice((2 * way + sub) * half_len, (2 * way + sub + 1) * half_len)
            total = kv_slots[way, n_chip - 2, sub]
            z_ref[out_rows, q_width:q_width + head_dim] = rotate_back(total[:, :head_dim], cos_ref[out_rows, :], sin_ref[out_rows, :]).astype(jnp.bfloat16)
            z_ref[out_rows, q_width + head_dim:] = total[:, head_dim:].astype(jnp.bfloat16)

    def mates_sent(step, _):
        for way in range(2):
            for sub in range(2):
                mate_copy(step, way, sub).wait_send()

    lax.fori_loop(0, n_chip, mates_sent, None)
    for swap in swaps:
        swap.wait_send()


def finish_kernel(n_dev, h_ref, z_ref, wo_part_ref, a_ref, x_ref, dy_ref, gain_ref, wq_ref, wo_ref, wk_ref, wv_ref,
                  gz_ref, gwo_ref, y_ref, dx_ref, ggain_ref,
                  h_scr, z_scr, zf_scr, a_scr, x_scr, dy_scr, dh_scr, wq_buf, wo_buf, gain_slots, local_scr, slots,
                  load_sems, w_sems, swap_send, swap_recv, send_sems, recv_sems, g1_send, g1_recv, m1_send, m1_recv,
                  g2_send, g2_recv, m2_send, m2_recv, keep_sems, gain_send, gain_recv):
    n_chip, chip, core, peers, partner = ring_place(n_dev)
    me = chip * 2 + core
    n_rows, model_dim = h_ref.shape
    core_width = z_scr.shape[1]
    q_width = a_ref.shape[1]
    head_dim = wk_ref.shape[1]
    n_sub, sub_len = local_scr.shape[1:3]
    way_len = n_sub * sub_len
    wo_sub_len, wo_width = wo_part_ref.shape[2:]
    wo_way_len = n_sub * wo_sub_len
    blk = model_dim // n_chip
    mine, other = pl.ds(0, n_rows), pl.ds(n_rows, n_rows)

    def cols(which, size):
        return pl.ds(pl.multiple_of(which * size, size), size)

    def wq_load(index, slot):
        return pltpu.make_async_copy(wq_ref.at[cols(index, blk), :], wq_buf.at[slot], w_sems.at[0, slot])

    def wo_load(index, slot):
        return pltpu.make_async_copy(wo_ref.at[:, cols(index, blk)], wo_buf.at[slot], w_sems.at[1, slot])

    loads = [
        pltpu.make_async_copy(h_ref, h_scr.at[mine], load_sems.at[0]),
        pltpu.make_async_copy(z_ref.at[:, cols(core, core_width)], z_scr.at[mine], load_sems.at[1]),
        pltpu.make_async_copy(z_ref, zf_scr, load_sems.at[2]),
        pltpu.make_async_copy(a_ref, a_scr, load_sems.at[3]),
        pltpu.make_async_copy(x_ref, x_scr, load_sems.at[4]),
        pltpu.make_async_copy(dy_ref, dy_scr, load_sems.at[5]),
    ]
    for load in loads:
        load.start()
    wq_load(0, 0).start()
    wo_load(0, 0).start()
    barrier = pltpu.get_barrier_semaphore()
    for offset in range(1, n_dev):
        pl.semaphore_signal(barrier, inc=1, device_id={'cp': lax.rem(me + offset, n_dev)}, device_id_type=pl.DeviceIdType.MESH)
    pl.semaphore_wait(barrier, n_dev - 1)

    def wo_place(step, way, sub):
        first = owner_at(chip, step, way, n_chip) * (2 * wo_way_len) + way * wo_way_len + sub * wo_sub_len
        return gwo_ref.at[pl.ds(pl.multiple_of(first, wo_sub_len), wo_sub_len), cols(core, wo_width)]

    def z_place(step, way, sub):
        first = owner_at(chip, step, way, n_chip) * (2 * way_len) + way * way_len + sub * sub_len
        return gz_ref.at[pl.ds(pl.multiple_of(first, sub_len), sub_len), cols(core, core_width)]

    swaps = [
        remote(h_ref, h_scr.at[other], swap_send.at[0], swap_recv.at[0], partner),
        remote(z_ref.at[:, cols(1 - core, core_width)], z_scr.at[other], swap_send.at[1], swap_recv.at[1], partner),
    ]
    for swap in swaps:
        swap.start()
    wo_gather = RingGather(n_chip, peers, partner, lambda way, sub: wo_part_ref.at[way, sub], wo_place, n_sub, g1_send, g1_recv, m1_send, m1_recv)
    z_gather = RingGather(n_chip, peers, partner, lambda way, sub: slots.at[way, n_chip - 2, sub], z_place, n_sub, g2_send, g2_recv, m2_send, m2_recv)
    keeps = ([pltpu.make_async_copy(wo_part_ref.at[way, sub], wo_place(0, way, sub), keep_sems.at[0, way, sub]) for sub, way in wo_gather.each],
             [pltpu.make_async_copy(slots.at[way, n_chip - 2, sub], z_place(0, way, sub), keep_sems.at[1, way, sub]) for sub, way in wo_gather.each])
    wo_gather.first()
    for keep in keeps[0]:
        keep.start()

    def local_term(step):
        for way in range(2):
            first = chunk_at(chip, step, way, n_chip) * (2 * way_len) + way * way_len
            part = dot(h_scr[:, pl.ds(pl.multiple_of(first, way_len), way_len)], z_scr[...], TN)
            for sub in range(n_sub):
                local_scr[way, sub] = part[sub * sub_len:(sub + 1) * sub_len, :]

    z_ring = RingReduce(n_chip, peers, local_term, local_scr, slots, send_sems, recv_sems)

    def d_hidden(index, slot):
        wq_load(index, slot).wait()

        @pl.when(index + 1 < n_chip)
        def _():
            wq_load(index + 1, 1 - slot).start()

        rows = cols(index, blk)
        dh_scr[:, rows] = (dot(zf_scr[:, :q_width], wq_buf[slot], NT) + dot(zf_scr[:, q_width:q_width + head_dim], wk_ref[rows, :], NT)
                           + dot(zf_scr[:, q_width + head_dim:], wv_ref[rows, :], NT))

    def out_block(index, slot):
        wo_load(index, slot).wait()

        @pl.when(index + 1 < n_chip)
        def _():
            wo_load(index + 1, 1 - slot).start()

        where = cols(index, blk)
        o_blk = dot(a_scr[...], wo_buf[slot], NN).astype(jnp.bfloat16)
        y_ref[:, where] = (x_scr[:, where].astype(jnp.float32) + o_blk.astype(jnp.float32)).astype(jnp.bfloat16)

    def norm_grad(index, _):
        rows = pl.ds(pl.multiple_of(index * 32, 32), 32)
        x_float = x_scr[rows, :].astype(jnp.float32)
        centered = x_float - jnp.mean(x_float, axis=-1, keepdims=True)
        inv_std = lax.rsqrt(jnp.mean(centered * centered, axis=-1, keepdims=True) + NORM_EPS)
        x_hat = centered * inv_std
        d_h = dh_scr[rows, :]
        gain_slots[me] += jnp.sum(d_h * x_hat, axis=0, keepdims=True)
        d_hat = d_h * gain_ref[...]
        mean_d = jnp.mean(d_hat, axis=-1, keepdims=True)
        mean_dx = jnp.mean(d_hat * x_hat, axis=-1, keepdims=True)
        dx_ref[rows, :] = (dy_scr[rows, :].astype(jnp.float32) + inv_std * (d_hat - mean_d - x_hat * mean_dx)).astype(jnp.bfloat16)

    def gain_copy(offset):
        return remote(gain_slots.at[me], gain_slots.at[me], gain_send.at[offset], gain_recv.at[offset], lax.rem(me + offset, n_dev))

    loads[0].wait()
    loads[1].wait()
    for swap in swaps:
        swap.wait_recv()
    z_ring.first()
    for load in loads[2:]:
        load.wait()
    wo_gather.middle(1)
    z_ring.middle(1)
    d_hidden(0, 0)

    def phase_one(step, _):
        wo_gather.middle(step)
        z_ring.middle(step)
        d_hidden(step - 1, lax.rem(step - 1, 2))

    lax.fori_loop(2, n_chip - 1, phase_one, None)
    wo_gather.last()
    z_ring.last()
    z_gather.first()
    for keep in keeps[1]:
        keep.start()
    d_hidden(n_chip - 2, (n_chip - 2) % 2)
    d_hidden(n_chip - 1, (n_chip - 1) % 2)
    gain_slots[me] = jnp.zeros(gain_slots.shape[1:], jnp.float32)
    lax.fori_loop(0, n_rows // 32, norm_grad, None)
    for offset in range(1, n_dev):
        gain_copy(offset).start()
    z_gather.middle(1)
    out_block(0, 0)
    out_block(1, 1)

    def phase_two(step, _):
        z_gather.middle(step)
        out_block(step, lax.rem(step, 2))

    lax.fori_loop(2, n_chip - 1, phase_two, None)
    out_block(n_chip - 1, (n_chip - 1) % 2)
    z_gather.last()
    for offset in range(1, n_dev):
        gain_copy(offset).wait_recv()
    total = gain_slots[0]
    for dev in range(1, n_dev):
        total = total + gain_slots[dev]
    ggain_ref[...] = total
    wo_gather.drain()
    z_gather.drain()
    for keep in keeps[0] + keeps[1]:
        keep.wait()
    for swap in swaps:
        swap.wait_send()
    for offset in range(1, n_dev):
        gain_copy(offset).wait_send()


def solution(mesh):
    n_dev = mesh.shape['cp']
    n_chip, n_sub = n_dev // 2, 2

    def local_fn(tokens, positions, norm_gain, w_query, w_key, w_value, w_out, d_out):
        n_seq, blk_len, model_dim = tokens.shape
        head_dim = w_key.shape[1]
        num_heads = w_query.shape[1] // head_dim
        q_width, kv_width = num_heads * head_dim, 2 * head_dim
        half_len, half = blk_len // 2, head_dim // 2
        n_rows, n_groups = n_seq * blk_len, 2 * n_seq
        rows = num_heads * half_len
        seq_len = n_dev * blk_len
        bf16, f32 = jnp.bfloat16, jnp.float32
        dma = pltpu.SemaphoreType.DMA
        vmem = pl.BlockSpec(memory_space=pltpu.VMEM)
        hbm = pl.BlockSpec(memory_space=pl.ANY)
        params = pltpu.CompilerParams(vmem_limit_bytes=VMEM_LIMIT)

        def comm(ident):
            return pltpu.CompilerParams(vmem_limit_bytes=VMEM_LIMIT, collective_id=ident, has_side_effects=True)

        def shape(*dims, dtype=bf16):
            return jax.ShapeDtypeStruct(dims, dtype)

        def gather_sems():
            return [dma((2, n_sub)), dma((2, n_chip - 1, n_sub)), dma((2, n_sub)), dma((2, n_chip, n_sub))]

        x_flat = tokens.reshape(n_rows, model_dim)
        dy_flat = d_out.reshape(n_rows, model_dim)
        gain_row = norm_gain.reshape(1, model_dim)
        cos_t, sin_t = rope_tables(positions.reshape(n_rows), head_dim)
        h_flat, kv_flat = pl.pallas_call(
            norm_kv_kernel,
            out_shape=(shape(n_rows, model_dim), shape(n_rows, kv_width)),
            compiler_params=params, name='norm_kv',
        )(x_flat, gain_row, w_key, w_value, cos_t, sin_t)

        kv_all, q_heads, da_heads = pl.pallas_call(
            functools.partial(gather_heads_kernel, n_dev),
            in_specs=[vmem, vmem, vmem, hbm, hbm, vmem, vmem],
            out_specs=[vmem, vmem, vmem],
            out_shape=(shape(n_seq, seq_len, kv_width), shape(n_groups, num_heads, half_len, head_dim), shape(n_groups, num_heads, half_len, head_dim)),
            scratch_shapes=[pltpu.VMEM((2, model_dim, head_dim), bf16), pltpu.VMEM((2, head_dim, model_dim), bf16), dma((2, 2))] + gather_sems(),
            compiler_params=comm(0), name='gather_heads',
        )(h_flat, dy_flat, kv_flat, w_query, w_out, cos_t, sin_t)
        q_rows = q_heads.reshape(n_groups, rows, head_dim)
        da_rows = da_heads.reshape(n_groups, rows, head_dim)

        q_spec = pl.BlockSpec((2, rows, head_dim), lambda s: (s, 0, 0))
        kv_spec = pl.BlockSpec((1, seq_len, kv_width), lambda s: (s, 0, 0))
        tok_spec = pl.BlockSpec((2, half_len, q_width), lambda s: (s, 0, 0))
        stat_spec = pl.BlockSpec((2, 1, rows), lambda s: (s, 0, 0))
        attn, lse, delta = pl.pallas_call(
            functools.partial(attend_kernel, n_dev),
            grid=(n_seq,),
            in_specs=[q_spec, kv_spec, q_spec],
            out_specs=[tok_spec, stat_spec, stat_spec],
            out_shape=(shape(n_groups, half_len, q_width), shape(n_groups, 1, rows, dtype=f32), shape(n_groups, 1, rows, dtype=f32)),
            scratch_shapes=[pltpu.VMEM((head_dim, rows), f32), pltpu.VMEM((1, rows), f32), pltpu.VMEM((1, rows), f32)],
            compiler_params=params, name='attend',
        )(q_rows, kv_all, da_rows)
        attn_flat = attn.reshape(n_rows, q_width)

        z_width = q_width + kv_width
        wo_cols, wo_sub = model_dim // 2, q_width // (2 * n_chip * n_sub)
        z_flat, wo_part = pl.pallas_call(
            functools.partial(attend_grad_kernel, n_dev),
            in_specs=[hbm, hbm, hbm, vmem, vmem, vmem, vmem, hbm, hbm],
            out_specs=[vmem, vmem],
            out_shape=(shape(n_rows, z_width), shape(2, n_sub, wo_sub, wo_cols, dtype=f32)),
            scratch_shapes=[pltpu.VMEM((n_groups, rows, head_dim), bf16), pltpu.VMEM((n_groups, rows, head_dim), bf16),
                            pltpu.VMEM((n_seq, seq_len, kv_width), bf16), pltpu.VMEM((head_dim, rows), f32),
                            pltpu.VMEM((n_seq, seq_len, kv_width), f32), pltpu.VMEM((2, n_chip, 2, half_len, kv_width), f32),
                            pltpu.VMEM((2, 2, half_len, kv_width), f32), pltpu.VMEM((2, n_chip - 1, 2, half_len, kv_width), f32),
                            pltpu.VMEM((2 * n_rows, q_width), bf16), pltpu.VMEM((2 * n_rows, wo_cols), bf16),
                            pltpu.VMEM((2, n_sub, wo_sub, wo_cols), f32), pltpu.VMEM((2, n_chip - 1, n_sub, wo_sub, wo_cols), f32),
                            dma((5,)), dma((2,)), dma((2,)), dma((2, 2)), dma((2, n_chip - 1, 2)), dma((2, n_chip, 2)), dma((2, n_chip, 2)),
                            dma((2, n_sub)), dma((2, n_chip - 1, n_sub))],
            compiler_params=comm(1), name='attend_grad',
        )(q_rows, kv_all, da_rows, lse, delta, cos_t, sin_t, attn_flat, dy_flat)

        core_width, sub_len = z_width // 2, model_dim // (2 * n_chip * n_sub)
        blk = model_dim // n_chip
        grad_z, grad_wo, out_y, grad_x, grad_gain = pl.pallas_call(
            functools.partial(finish_kernel, n_dev),
            in_specs=[hbm] * 6 + [vmem, hbm, hbm, vmem, vmem],
            out_specs=[hbm, hbm, vmem, vmem, vmem],
            out_shape=(shape(model_dim, z_width, dtype=f32), shape(q_width, model_dim, dtype=f32), shape(n_rows, model_dim), shape(n_rows, model_dim),
                       shape(1, model_dim, dtype=f32)),
            scratch_shapes=[pltpu.VMEM((2 * n_rows, model_dim), bf16), pltpu.VMEM((2 * n_rows, core_width), bf16), pltpu.VMEM((n_rows, z_width), bf16),
                            pltpu.VMEM((n_rows, q_width), bf16), pltpu.VMEM((n_rows, model_dim), bf16), pltpu.VMEM((n_rows, model_dim), bf16),
                            pltpu.VMEM((n_rows, model_dim), f32), pltpu.VMEM((2, blk, q_width), bf16), pltpu.VMEM((2, q_width, blk), bf16),
                            pltpu.VMEM((n_dev, 1, model_dim), f32), pltpu.VMEM((2, n_sub, sub_len, core_width), f32),
                            pltpu.VMEM((2, n_chip - 1, n_sub, sub_len, core_width), f32),
                            dma((6,)), dma((2, 2)), dma((2,)), dma((2,)), dma((2, n_sub)), dma((2, n_chip - 1, n_sub))]
            + gather_sems() + gather_sems() + [dma((2, 2, n_sub)), dma((n_dev,)), dma((n_dev,))],
            compiler_params=comm(2), name='finish',
        )(h_flat, z_flat, wo_part, attn_flat, x_flat, dy_flat, gain_row, w_query, w_out, w_key, w_value)
        grad_wq, grad_wk, grad_wv = grad_z[:, :q_width], grad_z[:, q_width:q_width + head_dim], grad_z[:, q_width + head_dim:]
        return out_y.reshape(tokens.shape), grad_x.reshape(tokens.shape), grad_wq, grad_wk, grad_wv, grad_wo, grad_gain.reshape(model_dim)

    seq_spec = P('dp', 'cp', None)
    rep_spec = P(None, None)
    part_spec = P('dp', None)
    return jax.shard_map(local_fn, mesh=mesh,
                         in_specs=(seq_spec, P('dp', 'cp'), P(None), rep_spec, rep_spec, rep_spec, rep_spec, seq_spec),
                         out_specs=(seq_spec, seq_spec, part_spec, part_spec, part_spec, part_spec, P('dp')),
                         check_vma=False)
```

```python
import functools

import jax
import jax.numpy as jnp
from jax import lax
from jax.experimental import pallas as pl
from jax.experimental.pallas import tpu as pltpu
from jax.sharding import PartitionSpec as P

NORM_EPS = 1e-6
ROPE_BASE = 10000.0
NEG_BIG = -1e30
LOG2_E = 1.4426950408889634
PIECES_PER_BLOCK = 4
VMEM_LIMIT = 60 * 1024 * 1024

NT = (((1,), (1,)), ((), ()))
TN = (((0,), (0,)), ((), ()))
NN = (((1,), (0,)), ((), ()))


def dot(lhs, rhs, dims):
    return lax.dot_general(lhs, rhs, dims, preferred_element_type=jnp.float32)


def rope_tables(positions, head_dim):
    half_dim = head_dim // 2
    inv_freq = ROPE_BASE ** (-(jnp.arange(half_dim, dtype=jnp.float32) * (2.0 / head_dim)))
    angles = positions.astype(jnp.float32)[..., None] * inv_freq
    return jnp.cos(angles), jnp.sin(angles)


def rotate(values, cos_t, sin_t):
    half_dim = values.shape[-1] // 2
    front_half, back_half = values[..., :half_dim], values[..., half_dim:]
    return jnp.concatenate([front_half * cos_t - back_half * sin_t, back_half * cos_t + front_half * sin_t], axis=-1)


def rotate_back(grad_vals, cos_t, sin_t):
    half_dim = grad_vals.shape[-1] // 2
    front_half, back_half = grad_vals[..., :half_dim], grad_vals[..., half_dim:]
    return jnp.concatenate([front_half * cos_t + back_half * sin_t, back_half * cos_t - front_half * sin_t], axis=-1)


def norm_kv_kernel(x_ref, gain_ref, wk_ref, wv_ref, cos_ref, sin_ref, h_ref, kv_ref):
    head_dim = wk_ref.shape[1]
    x_float = x_ref[...].astype(jnp.float32)
    centered = x_float - jnp.mean(x_float, axis=-1, keepdims=True)
    inv_std = lax.rsqrt(jnp.mean(centered * centered, axis=-1, keepdims=True) + NORM_EPS)
    h_norm = (centered * inv_std * gain_ref[...]).astype(jnp.bfloat16)
    h_ref[...] = h_norm
    k_lin = dot(h_norm, wk_ref[...], NN)
    kv_ref[:, :head_dim] = rotate(k_lin, cos_ref[...], sin_ref[...]).astype(jnp.bfloat16)
    kv_ref[:, head_dim:] = dot(h_norm, wv_ref[...], NN).astype(jnp.bfloat16)


def entry_barrier(peers):
    barrier = pltpu.get_barrier_semaphore()
    for peer in peers:
        pl.semaphore_signal(barrier, inc=1, device_id={'cp': peer}, device_id_type=pl.DeviceIdType.MESH)
    pl.semaphore_wait(barrier, len(peers))


def remote(src, dst, send_sem, recv_sem, peer):
    return pltpu.make_async_remote_copy(src_ref=src, dst_ref=dst, send_sem=send_sem, recv_sem=recv_sem,
                                        device_id={'cp': peer}, device_id_type=pl.DeviceIdType.MESH)


def ring_place(n_dev):
    me = lax.axis_index('cp')
    n_chip = n_dev // 2
    chip, core = lax.div(me, 2), lax.rem(me, 2)
    after = lax.rem(chip + 1, n_chip) * 2 + core
    before = lax.rem(chip + n_chip - 1, n_chip) * 2 + core
    partner = chip * 2 + 1 - core
    return n_chip, chip, core, (after, before), partner


def chunk_at(chip, step, way, n_chip):
    if way == 0:
        return lax.rem(chip + 2 * n_chip - 1 - step, n_chip)
    return lax.rem(chip + 1 + step, n_chip)


class RingReduce:
    def __init__(self, n_chip, peers, make_local, local_scr, slots, send_sems, recv_sems):
        self.n_chip, self.peers, self.make_local = n_chip, peers, make_local
        self.local_scr, self.slots, self.send_sems, self.recv_sems = local_scr, slots, send_sems, recv_sems
        self.each = [(sub, way) for sub in range(slots.shape[2]) for way in range(2)]

    def hop(self, step, way, sub, first=False):
        src = self.local_scr.at[way, sub] if first else self.slots.at[way, step - 1, sub]
        return remote(src, self.slots.at[way, step, sub], self.send_sems.at[way, sub], self.recv_sems.at[way, step, sub], self.peers[way])

    def first(self):
        self.make_local(0)
        for sub, way in self.each:
            self.hop(0, way, sub, True).start()

    def middle(self, step, last=False):
        for sub, way in self.each:
            self.hop(step - 1, way, sub, isinstance(step, int) and step == 1).wait_send()
        self.make_local(step)
        for sub, way in self.each:
            self.hop(step - 1, way, sub, isinstance(step, int) and step == 1).wait_recv()
            self.slots[way, step - 1, sub] = self.slots[way, step - 1, sub] + self.local_scr[way, sub]
            if not last:
                self.hop(step, way, sub).start()

    def last(self):
        self.middle(self.n_chip - 1, True)


class RingGather:
    def __init__(self, n_chip, peers, partner, own, place, n_sub, send_sems, recv_sems, mate_send, mate_recv):
        self.n_chip, self.peers, self.partner, self.own, self.place = n_chip, peers, partner, own, place
        self.send_sems, self.recv_sems, self.mate_send, self.mate_recv = send_sems, recv_sems, mate_send, mate_recv
        self.each = [(sub, way) for sub in range(n_sub) for way in range(2)]

    def onward(self, step, way, sub, first=False):
        src = self.own(way, sub) if first else self.place(step, way, sub)
        return remote(src, self.place(step, way, sub), self.send_sems.at[way, sub], self.recv_sems.at[way, step, sub], self.peers[way])

    def across(self, step, way, sub, first=False):
        src = self.own(way, sub) if first else self.place(step, way, sub)
        return remote(src, self.place(step, way, sub), self.mate_send.at[way, sub], self.mate_recv.at[way, step, sub], self.partner)

    def first(self):
        for sub, way in self.each:
            self.onward(0, way, sub, True).start()
            self.across(0, way, sub, True).start()

    def middle(self, step, last=False):
        after_first = isinstance(step, int) and step == 1
        for sub, way in self.each:
            self.onward(step - 1, way, sub, after_first).wait_send()
            self.onward(step - 1, way, sub, after_first).wait_recv()
            if not last:
                self.onward(step, way, sub).start()
            self.across(step - 1, way, sub, after_first).wait_send()
            self.across(step, way, sub).start()

    def last(self):
        self.middle(self.n_chip - 1, True)

    def drain(self):
        for sub, way in self.each:
            self.across(self.n_chip - 1, way, sub).wait_send()

        def body(step, _):
            for sub, way in self.each:
                self.across(step, way, sub).wait_recv()

        lax.fori_loop(0, self.n_chip, body, None)


def owner_at(chip, step, way, n_chip):
    if way == 0:
        return lax.rem(chip + n_chip - step, n_chip)
    return lax.rem(chip + step, n_chip)


def causal_mask(shape, key_start, query_start, half_len):
    key_idx = key_start + lax.broadcasted_iota(jnp.int32, shape, 0)
    query_idx = query_start + lax.rem(lax.broadcasted_iota(jnp.int32, shape, 1), half_len)
    return key_idx <= query_idx


def forward_kernel(n_dev, kv_ref, cos_ref, sin_ref, h_ref, dy_ref, wq_ref, wo_ref, all_ref, q_ref, da_ref, a_ref, lse_ref, delta_ref,
                   h_scr, dy_scr, kv_scr, q_scr, da_scr, qt_scr, a_scr, acc_scr, max_scr, sum_scr, wq_buf, wo_buf,
                   load_sems, out_sems, w_sems, send_sems, recv_sems, mate_send, mate_recv):
    n_chip, chip, core, peers, partner = ring_place(n_dev)
    me = chip * 2 + core
    n_seq, seq_len, kv_width = kv_scr.shape
    half_len = seq_len // (2 * n_dev)
    n_groups, rows, head_dim = q_scr.shape
    num_heads = rows // half_len
    key_len = 2 * half_len
    scale = LOG2_E * head_dim ** -0.5

    def weights(head, slot):
        cols = pl.ds(pl.multiple_of(head * head_dim, head_dim), head_dim)
        return (pltpu.make_async_copy(wq_ref.at[:, cols], wq_buf.at[slot], w_sems.at[0, slot]),
                pltpu.make_async_copy(wo_ref.at[cols, :], wo_buf.at[slot], w_sems.at[1, slot]))

    loads = [pltpu.make_async_copy(h_ref, h_scr, load_sems.at[0]), pltpu.make_async_copy(dy_ref, dy_scr, load_sems.at[1])]
    for load in loads:
        load.start()
    for copy in weights(0, 0):
        copy.start()
    entry_barrier(peers + (partner,))

    def piece_rows(dev, way):
        piece = dev if way == 0 else 2 * n_dev - 1 - dev
        return pl.ds(pl.multiple_of(piece * half_len, half_len), half_len)

    def place(step, way, seq):
        return kv_scr.at[seq, piece_rows(owner_at(chip, step, way, n_chip) * 2 + core, way)]

    def own(way, seq):
        return kv_ref.at[pl.ds((2 * seq + way) * half_len, half_len)]

    ring = RingGather(n_chip, peers, partner, own, place, n_seq, send_sems, recv_sems, mate_send, mate_recv)
    ring.first()
    for seq in range(n_seq):
        for way in range(2):
            kv_scr[seq, piece_rows(me, way), :] = kv_ref[(2 * seq + way) * half_len:(2 * seq + way + 1) * half_len, :]
    max_scr[...] = jnp.full_like(max_scr, NEG_BIG)
    sum_scr[...] = jnp.zeros_like(sum_scr)
    acc_scr[...] = jnp.zeros_like(acc_scr)
    for load in loads:
        load.wait()

    def project(head, slot):
        @pl.when(head < num_heads)
        def _():
            for copy in weights(head, slot):
                copy.wait()

            @pl.when(head + 1 < num_heads)
            def _():
                for copy in weights(head + 1, 1 - slot):
                    copy.start()

            head_rows = pl.ds(pl.multiple_of(head * half_len, half_len), half_len)
            q_new = rotate(dot(h_scr[...], wq_buf[slot], NN), cos_ref[...], sin_ref[...]).astype(jnp.bfloat16)
            da_new = dot(dy_scr[...], wo_buf[slot], NT).astype(jnp.bfloat16)
            for group in range(n_groups):
                q_scr[group, head_rows, :] = q_new[group * half_len:(group + 1) * half_len, :]
                da_scr[group, head_rows, :] = da_new[group * half_len:(group + 1) * half_len, :]

    def block(seq, group, start, masked):
        index = 2 * seq + group
        keys = pl.ds(pl.multiple_of(start, half_len), key_len)
        scores = dot(kv_scr[seq, keys, :head_dim], qt_scr[index], NN) * scale
        if masked:
            piece = me if group == 0 else 2 * n_dev - 1 - me
            scores = jnp.where(causal_mask(scores.shape, start, piece * half_len, half_len), scores, NEG_BIG)
        old_max = max_scr[index]
        new_max = jnp.maximum(old_max, jnp.max(scores, axis=0, keepdims=True))
        rescale = jnp.exp2(old_max - new_max)
        probs = jnp.exp2(scores - new_max)
        max_scr[index] = new_max
        sum_scr[index] = sum_scr[index] * rescale + jnp.sum(probs, axis=0, keepdims=True)
        acc_scr[index] = acc_scr[index] * rescale + dot(kv_scr[seq, keys, head_dim:], probs.astype(jnp.bfloat16), TN)

    def arrived(step, seq, masked):
        for way in range(2):
            ring.across(step, way, seq).wait_recv()
        front = owner_at(chip, step, 0, n_chip)
        back = owner_at(chip, step, 1, n_chip)
        front_start = front * key_len
        back_start = (n_dev - 1 - back) * key_len

        @pl.when(step <= chip)
        def _():
            block(seq, 0, front_start, masked)

        block(seq, 1, front_start, False)

        @pl.when(chip + step < n_chip)
        def _():
            block(seq, 1, back_start, masked)

    def attend(step, _):
        lax.fori_loop(0, n_seq, lambda seq, _: arrived(step, seq, False), None)

    def project_two(step):
        lax.fori_loop(2 * step, 2 * step + 2, lambda head, _: project(head, lax.rem(head, 2)), None)

    project_two(0)
    ring.middle(1)

    def projecting(step, _):
        project_two(step)
        ring.middle(step + 1)

    lax.fori_loop(1, 3, projecting, None)
    lax.fori_loop(6, max(num_heads, 6), lambda head, _: project(head, lax.rem(head, 2)), None)
    for group in range(n_groups):
        qt_scr[group] = q_scr[group].T
    ring.middle(4)
    saves = [pltpu.make_async_copy(q_scr, q_ref, out_sems.at[0]), pltpu.make_async_copy(da_scr, da_ref, out_sems.at[1])]
    for save in saves:
        save.start()
    lax.fori_loop(0, n_seq, lambda seq, _: arrived(0, seq, True), None)

    def more(step, _):
        ring.middle(step)
        lax.fori_loop(2 * step - 9, 2 * step - 7, attend, None)

    lax.fori_loop(5, n_chip - 1, more, None)
    ring.last()
    lax.fori_loop(2 * n_chip - 11, n_chip, attend, None)
    for sub, way in ring.each:
        ring.across(n_chip - 1, way, sub).wait_send()
    saves.append(pltpu.make_async_copy(kv_scr, all_ref, out_sems.at[2]))
    saves[2].start()

    def finish(index, _):
        attn = (acc_scr[index] / sum_scr[index]).T.astype(jnp.bfloat16)
        lse_ref[index] = max_scr[index] + jnp.log2(sum_scr[index])
        prod = attn.astype(jnp.float32) * da_scr[index].astype(jnp.float32)
        prod = prod[:, :head_dim // 2] + prod[:, head_dim // 2:]
        delta_ref[index] = jnp.sum(prod.T, axis=0, keepdims=True)
        out_rows = pl.ds(pl.multiple_of(index * half_len, half_len), half_len)
        for head in range(num_heads):
            a_scr[out_rows, head * head_dim:(head + 1) * head_dim] = attn[head * half_len:(head + 1) * half_len, :]
        pltpu.make_async_copy(a_scr.at[out_rows], a_ref.at[out_rows], out_sems.at[3 + index]).start()

    lax.fori_loop(0, n_groups, finish, None)
    for index in range(n_groups):
        out_rows = pl.ds(index * half_len, half_len)
        pltpu.make_async_copy(a_scr.at[out_rows], a_ref.at[out_rows], out_sems.at[3 + index]).wait()
    for save in saves:
        save.wait()


def attend_grad_kernel(n_dev, q_ref, kv_ref, da_ref, lse_ref, delta_ref, cos_ref, sin_ref, a_ref, dy_ref, z_ref, wo_ref,
                       q_scr, da_scr, kv_scr, qt_scr, dat_scr, dq_scr, dkv_scr, mate_scr, kv_local, kv_slots, a_scr, dy_scr, wo_local, wo_slots,
                       load_sems, swap_send, swap_recv, kv_send, kv_recv, mate_send, mate_recv, wo_send, wo_recv):
    n_chip, chip, core, peers, partner = ring_place(n_dev)
    me = chip * 2 + core
    rows, head_dim = q_scr.shape[1:]
    n_seq, seq_len, kv_width = dkv_scr.shape
    half_len = seq_len // (2 * n_dev)
    num_heads = rows // half_len
    q_width = num_heads * head_dim
    n_rows = a_ref.shape[0]
    key_len = PIECES_PER_BLOCK * half_len
    scale = LOG2_E * head_dim ** -0.5
    dy_cols = dy_scr.shape[1]
    mine, other = pl.ds(0, n_rows), pl.ds(n_rows, n_rows)

    def cols(which, size):
        return pl.ds(pl.multiple_of(which * size, size), size)

    loads = [
        pltpu.make_async_copy(a_ref, a_scr.at[mine], load_sems.at[0]),
        pltpu.make_async_copy(dy_ref.at[:, cols(core, dy_cols)], dy_scr.at[mine], load_sems.at[1]),
        pltpu.make_async_copy(q_ref, q_scr, load_sems.at[2]),
        pltpu.make_async_copy(da_ref, da_scr, load_sems.at[3]),
        pltpu.make_async_copy(kv_ref, kv_scr, load_sems.at[4]),
    ]
    for load in loads:
        load.start()
    entry_barrier(peers + (partner,))
    swaps = [
        remote(a_ref, a_scr.at[other], swap_send.at[0], swap_recv.at[0], partner),
        remote(dy_ref.at[:, cols(1 - core, dy_cols)], dy_scr.at[other], swap_send.at[1], swap_recv.at[1], partner),
    ]
    for swap in swaps:
        swap.start()
    dkv_scr[...] = jnp.zeros_like(dkv_scr)
    loads[0].wait()
    loads[1].wait()
    for swap in swaps:
        swap.wait_recv()

    def wo_local_term(step):
        n_sub, sub_len = wo_local.shape[1:3]
        way_len = n_sub * sub_len
        for way in range(2):
            first = chunk_at(chip, step, way, n_chip) * (2 * way_len) + way * way_len
            part = dot(a_scr[:, pl.ds(pl.multiple_of(first, way_len), way_len)], dy_scr[...], TN)
            for sub in range(n_sub):
                wo_local[way, sub] = part[sub * sub_len:(sub + 1) * sub_len, :]

    def piece_rows(dev, sub):
        piece = dev if sub == 0 else 2 * n_dev - 1 - dev
        return pl.ds(pl.multiple_of(piece * half_len, half_len), half_len)

    def mate_copy(step, way, sub):
        dev = chunk_at(chip, step, way, n_chip) * 2 + 1 - core
        return remote(dkv_scr.at[way, piece_rows(dev, sub)], mate_scr.at[way, step, sub], mate_send.at[way, step, sub], mate_recv.at[way, step, sub], partner)

    def kv_local_term(step):
        for sub in range(2):
            for way in range(2):
                mate_copy(step, way, sub).wait_recv()
                dev = chunk_at(chip, step, way, n_chip) * 2 + core
                kv_local[way, sub] = dkv_scr[way, piece_rows(dev, sub), :] + mate_scr[way, step, sub]

    wo_ring = RingReduce(n_chip, peers, wo_local_term, wo_local, wo_slots, wo_send, wo_recv)
    kv_ring = RingReduce(n_chip, peers, kv_local_term, kv_local, kv_slots, kv_send, kv_recv)

    def attend_seq(seq):
        def one_group(group, _):
            index = 2 * seq + group
            piece = me + group * (2 * n_dev - 1 - 2 * me)
            last = lax.div(piece, PIECES_PER_BLOCK)
            dq_scr[...] = jnp.zeros_like(dq_scr)
            qt_scr[...] = q_scr[index].T
            dat_scr[...] = da_scr[index].T

            def block(step, masked):
                start = pl.multiple_of(step * key_len, key_len)
                keys = pl.ds(start, key_len)
                k_blk, v_blk = kv_scr[seq, keys, :head_dim], kv_scr[seq, keys, head_dim:]
                probs = jnp.exp2(dot(k_blk, qt_scr[...], NN) * scale - lse_ref[index])
                if masked:
                    probs = jnp.where(causal_mask(probs.shape, start, piece * half_len, half_len), probs, 0.0)
                d_scores = (probs * (dot(v_blk, dat_scr[...], NN) - delta_ref[index])).astype(jnp.bfloat16)
                dq_scr[...] += dot(k_blk, d_scores, TN)
                dkv_scr[seq, keys, :head_dim] += dot(d_scores, q_scr[index], NN) * head_dim ** -0.5
                dkv_scr[seq, keys, head_dim:] += dot(probs.astype(jnp.bfloat16), da_scr[index], NN)

            lax.fori_loop(0, last, lambda step, _: block(step, False), None)
            block(last, True)
            dq = dq_scr[...].T * head_dim ** -0.5
            out_rows = pl.ds(pl.multiple_of(index * half_len, half_len), half_len)
            cos_t, sin_t = cos_ref[out_rows, :], sin_ref[out_rows, :]
            for head in range(num_heads):
                dq_head = dq[head * half_len:(head + 1) * half_len, :]
                z_ref[out_rows, head * head_dim:(head + 1) * head_dim] = rotate_back(dq_head, cos_t, sin_t).astype(jnp.bfloat16)

        lax.fori_loop(0, 2, one_group, None)

        def send_mate(step, _):
            for sub in range(2):
                mate_copy(step, seq, sub).start()

        lax.fori_loop(0, n_chip, send_mate, None)

    wo_ring.first()
    for load in loads[2:]:
        load.wait()
    attend_seq(0)
    wo_ring.middle(1)
    attend_seq(1)
    wo_ring.middle(2)
    kv_ring.first()
    wo_ring.middle(3)
    kv_ring.middle(1)

    def both(step, _):
        wo_ring.middle(step + 2)
        kv_ring.middle(step)

    lax.fori_loop(2, n_chip - 3, both, None)
    wo_ring.last()
    for way in range(2):
        for sub in range(wo_local.shape[1]):
            wo_ref[way, sub] = wo_slots[way, n_chip - 2, sub]
    kv_ring.middle(n_chip - 3)
    kv_ring.middle(n_chip - 2)
    kv_ring.last()
    for way in range(2):
        for sub in range(2):
            out_rows = slice((2 * way + sub) * half_len, (2 * way + sub + 1) * half_len)
            total = kv_slots[way, n_chip - 2, sub]
            z_ref[out_rows, q_width:q_width + head_dim] = rotate_back(total[:, :head_dim], cos_ref[out_rows, :], sin_ref[out_rows, :]).astype(jnp.bfloat16)
            z_ref[out_rows, q_width + head_dim:] = total[:, head_dim:].astype(jnp.bfloat16)

    def mates_sent(step, _):
        for way in range(2):
            for sub in range(2):
                mate_copy(step, way, sub).wait_send()

    lax.fori_loop(0, n_chip, mates_sent, None)
    for swap in swaps:
        swap.wait_send()


def finish_kernel(n_dev, h_ref, z_ref, wo_part_ref, a_ref, x_ref, dy_ref, gain_ref, wq_ref, wo_ref, wk_ref, wv_ref,
                  gz_ref, gwo_ref, y_ref, dx_ref, ggain_ref,
                  h_scr, z_scr, zf_scr, a_scr, x_scr, dy_scr, dh_scr, wq_buf, wo_buf, gain_slots, local_scr, slots,
                  load_sems, w_sems, swap_send, swap_recv, send_sems, recv_sems, g1_send, g1_recv, m1_send, m1_recv,
                  g2_send, g2_recv, m2_send, m2_recv, keep_sems, gain_send, gain_recv):
    n_chip, chip, core, peers, partner = ring_place(n_dev)
    me = chip * 2 + core
    n_rows, model_dim = h_ref.shape
    core_width = z_scr.shape[1]
    q_width = a_ref.shape[1]
    head_dim = wk_ref.shape[1]
    n_sub, sub_len = local_scr.shape[1:3]
    way_len = n_sub * sub_len
    wo_sub_len, wo_width = wo_part_ref.shape[2:]
    wo_way_len = n_sub * wo_sub_len
    blk = model_dim // n_chip
    mine, other = pl.ds(0, n_rows), pl.ds(n_rows, n_rows)

    def cols(which, size):
        return pl.ds(pl.multiple_of(which * size, size), size)

    def wq_load(index, slot):
        return pltpu.make_async_copy(wq_ref.at[cols(index, blk), :], wq_buf.at[slot], w_sems.at[0, slot])

    def wo_load(index, slot):
        return pltpu.make_async_copy(wo_ref.at[:, cols(index, blk)], wo_buf.at[slot], w_sems.at[1, slot])

    loads = [
        pltpu.make_async_copy(h_ref, h_scr.at[mine], load_sems.at[0]),
        pltpu.make_async_copy(z_ref.at[:, cols(core, core_width)], z_scr.at[mine], load_sems.at[1]),
        pltpu.make_async_copy(z_ref, zf_scr, load_sems.at[2]),
        pltpu.make_async_copy(a_ref, a_scr, load_sems.at[3]),
        pltpu.make_async_copy(x_ref, x_scr, load_sems.at[4]),
        pltpu.make_async_copy(dy_ref, dy_scr, load_sems.at[5]),
    ]
    for load in loads:
        load.start()
    wq_load(0, 0).start()
    wo_load(0, 0).start()
    barrier = pltpu.get_barrier_semaphore()
    for offset in range(1, n_dev):
        pl.semaphore_signal(barrier, inc=1, device_id={'cp': lax.rem(me + offset, n_dev)}, device_id_type=pl.DeviceIdType.MESH)
    pl.semaphore_wait(barrier, n_dev - 1)

    def wo_place(step, way, sub):
        first = owner_at(chip, step, way, n_chip) * (2 * wo_way_len) + way * wo_way_len + sub * wo_sub_len
        return gwo_ref.at[pl.ds(pl.multiple_of(first, wo_sub_len), wo_sub_len), cols(core, wo_width)]

    def z_place(step, way, sub):
        first = owner_at(chip, step, way, n_chip) * (2 * way_len) + way * way_len + sub * sub_len
        return gz_ref.at[pl.ds(pl.multiple_of(first, sub_len), sub_len), cols(core, core_width)]

    swaps = [
        remote(h_ref, h_scr.at[other], swap_send.at[0], swap_recv.at[0], partner),
        remote(z_ref.at[:, cols(1 - core, core_width)], z_scr.at[other], swap_send.at[1], swap_recv.at[1], partner),
    ]
    for swap in swaps:
        swap.start()
    wo_gather = RingGather(n_chip, peers, partner, lambda way, sub: wo_part_ref.at[way, sub], wo_place, n_sub, g1_send, g1_recv, m1_send, m1_recv)
    z_gather = RingGather(n_chip, peers, partner, lambda way, sub: slots.at[way, n_chip - 2, sub], z_place, n_sub, g2_send, g2_recv, m2_send, m2_recv)
    keeps = ([pltpu.make_async_copy(wo_part_ref.at[way, sub], wo_place(0, way, sub), keep_sems.at[0, way, sub]) for sub, way in wo_gather.each],
             [pltpu.make_async_copy(slots.at[way, n_chip - 2, sub], z_place(0, way, sub), keep_sems.at[1, way, sub]) for sub, way in wo_gather.each])
    wo_gather.first()
    for keep in keeps[0]:
        keep.start()

    def local_term(step):
        for way in range(2):
            first = chunk_at(chip, step, way, n_chip) * (2 * way_len) + way * way_len
            part = dot(h_scr[:, pl.ds(pl.multiple_of(first, way_len), way_len)], z_scr[...], TN)
            for sub in range(n_sub):
                local_scr[way, sub] = part[sub * sub_len:(sub + 1) * sub_len, :]

    z_ring = RingReduce(n_chip, peers, local_term, local_scr, slots, send_sems, recv_sems)

    def d_hidden(index, slot):
        wq_load(index, slot).wait()

        @pl.when(index + 1 < n_chip)
        def _():
            wq_load(index + 1, 1 - slot).start()

        rows = cols(index, blk)
        dh_scr[:, rows] = (dot(zf_scr[:, :q_width], wq_buf[slot], NT) + dot(zf_scr[:, q_width:q_width + head_dim], wk_ref[rows, :], NT)
                           + dot(zf_scr[:, q_width + head_dim:], wv_ref[rows, :], NT))

    def out_block(index, slot):
        wo_load(index, slot).wait()

        @pl.when(index + 1 < n_chip)
        def _():
            wo_load(index + 1, 1 - slot).start()

        where = cols(index, blk)
        o_blk = dot(a_scr[...], wo_buf[slot], NN).astype(jnp.bfloat16)
        y_ref[:, where] = (x_scr[:, where].astype(jnp.float32) + o_blk.astype(jnp.float32)).astype(jnp.bfloat16)

    def norm_grad(index, _):
        rows = pl.ds(pl.multiple_of(index * 32, 32), 32)
        x_float = x_scr[rows, :].astype(jnp.float32)
        centered = x_float - jnp.mean(x_float, axis=-1, keepdims=True)
        inv_std = lax.rsqrt(jnp.mean(centered * centered, axis=-1, keepdims=True) + NORM_EPS)
        x_hat = centered * inv_std
        d_h = dh_scr[rows, :]
        gain_slots[me] += jnp.sum(d_h * x_hat, axis=0, keepdims=True)
        d_hat = d_h * gain_ref[...]
        mean_d = jnp.mean(d_hat, axis=-1, keepdims=True)
        mean_dx = jnp.mean(d_hat * x_hat, axis=-1, keepdims=True)
        dx_ref[rows, :] = (dy_scr[rows, :].astype(jnp.float32) + inv_std * (d_hat - mean_d - x_hat * mean_dx)).astype(jnp.bfloat16)

    def gain_copy(offset):
        return remote(gain_slots.at[me], gain_slots.at[me], gain_send.at[offset], gain_recv.at[offset], lax.rem(me + offset, n_dev))

    loads[0].wait()
    loads[1].wait()
    for swap in swaps:
        swap.wait_recv()
    z_ring.first()
    for load in loads[2:]:
        load.wait()
    wo_gather.middle(1)
    z_ring.middle(1)
    d_hidden(0, 0)

    def phase_one(step, _):
        wo_gather.middle(step)
        z_ring.middle(step)
        d_hidden(step - 1, lax.rem(step - 1, 2))

    lax.fori_loop(2, n_chip - 1, phase_one, None)
    wo_gather.last()
    z_ring.last()
    z_gather.first()
    for keep in keeps[1]:
        keep.start()
    d_hidden(n_chip - 2, (n_chip - 2) % 2)
    d_hidden(n_chip - 1, (n_chip - 1) % 2)
    gain_slots[me] = jnp.zeros(gain_slots.shape[1:], jnp.float32)
    lax.fori_loop(0, n_rows // 32, norm_grad, None)
    for offset in range(1, n_dev):
        gain_copy(offset).start()
    z_gather.middle(1)
    out_block(0, 0)
    out_block(1, 1)

    def phase_two(step, _):
        z_gather.middle(step)
        out_block(step, lax.rem(step, 2))

    lax.fori_loop(2, n_chip - 1, phase_two, None)
    out_block(n_chip - 1, (n_chip - 1) % 2)
    z_gather.last()
    for offset in range(1, n_dev):
        gain_copy(offset).wait_recv()
    total = gain_slots[0]
    for dev in range(1, n_dev):
        total = total + gain_slots[dev]
    ggain_ref[...] = total
    wo_gather.drain()
    z_gather.drain()
    for keep in keeps[0] + keeps[1]:
        keep.wait()
    for swap in swaps:
        swap.wait_send()
    for offset in range(1, n_dev):
        gain_copy(offset).wait_send()


def deliver_kernel(gz_ref, y_ref, dx_ref, wq_out, wk_out, wv_out, y_out, dx_out, gz_buf, in_sems, out_sems):
    n_blk, blk_len, _ = gz_buf.shape
    q_width, head_dim = wq_out.shape[1], wk_out.shape[1]
    reads = [pltpu.make_async_copy(gz_ref.at[pl.ds(i * blk_len, blk_len)], gz_buf.at[i], in_sems.at[i]) for i in range(n_blk)]
    for read in reads:
        read.start()
    writes = [pltpu.make_async_copy(src, out, out_sems.at[3 * n_blk + i]) for i, (src, out) in enumerate([(y_ref, y_out), (dx_ref, dx_out)])]
    for write in writes:
        write.start()
    for i in range(n_blk):
        reads[i].wait()
        rows = pl.ds(i * blk_len, blk_len)
        for j, (out, first) in enumerate([(wq_out, 0), (wk_out, q_width), (wv_out, q_width + head_dim)]):
            writes.append(pltpu.make_async_copy(gz_buf.at[i, :, pl.ds(first, out.shape[1])], out.at[rows], out_sems.at[3 * i + j]))
            writes[-1].start()
    for write in writes:
        write.wait()


def solution(mesh):
    n_dev = mesh.shape['cp']
    n_chip, n_sub = n_dev // 2, 2

    def local_fn(tokens, positions, norm_gain, w_query, w_key, w_value, w_out, d_out):
        n_seq, blk_len, model_dim = tokens.shape
        head_dim = w_key.shape[1]
        num_heads = w_query.shape[1] // head_dim
        q_width, kv_width = num_heads * head_dim, 2 * head_dim
        half_len, half = blk_len // 2, head_dim // 2
        n_rows, n_groups = n_seq * blk_len, 2 * n_seq
        rows = num_heads * half_len
        seq_len = n_dev * blk_len
        bf16, f32 = jnp.bfloat16, jnp.float32
        dma = pltpu.SemaphoreType.DMA
        vmem = pl.BlockSpec(memory_space=pltpu.VMEM)
        hbm = pl.BlockSpec(memory_space=pl.ANY)
        params = pltpu.CompilerParams(vmem_limit_bytes=VMEM_LIMIT)

        def comm(ident):
            return pltpu.CompilerParams(vmem_limit_bytes=VMEM_LIMIT, collective_id=ident, has_side_effects=True)

        def shape(*dims, dtype=bf16):
            return jax.ShapeDtypeStruct(dims, dtype)

        def gather_sems():
            return [dma((2, n_sub)), dma((2, n_chip - 1, n_sub)), dma((2, n_sub)), dma((2, n_chip, n_sub))]

        x_flat = tokens.reshape(n_rows, model_dim)
        dy_flat = d_out.reshape(n_rows, model_dim)
        gain_row = norm_gain.reshape(1, model_dim)
        cos_t, sin_t = rope_tables(positions.reshape(n_rows), head_dim)
        h_flat, kv_flat = pl.pallas_call(
            norm_kv_kernel,
            out_shape=(shape(n_rows, model_dim), shape(n_rows, kv_width)),
            compiler_params=params, name='norm_kv',
        )(x_flat, gain_row, w_key, w_value, cos_t, sin_t)

        groups = (n_groups, rows, head_dim)
        kv_all, q_rows, da_rows, attn_flat, lse, delta = pl.pallas_call(
            functools.partial(forward_kernel, n_dev),
            in_specs=[vmem, vmem, vmem, hbm, hbm, hbm, hbm],
            out_specs=[hbm, hbm, hbm, hbm, vmem, vmem],
            out_shape=(shape(n_seq, seq_len, kv_width), shape(*groups), shape(*groups), shape(n_rows, q_width),
                       shape(n_groups, 1, rows, dtype=f32), shape(n_groups, 1, rows, dtype=f32)),
            scratch_shapes=[pltpu.VMEM((n_rows, model_dim), bf16), pltpu.VMEM((n_rows, model_dim), bf16), pltpu.VMEM((n_seq, seq_len, kv_width), bf16),
                            pltpu.VMEM(groups, bf16), pltpu.VMEM(groups, bf16), pltpu.VMEM((n_groups, head_dim, rows), bf16), pltpu.VMEM((n_rows, q_width), bf16),
                            pltpu.VMEM((n_groups, head_dim, rows), f32), pltpu.VMEM((n_groups, 1, rows), f32), pltpu.VMEM((n_groups, 1, rows), f32),
                            pltpu.VMEM((2, model_dim, head_dim), bf16), pltpu.VMEM((2, head_dim, model_dim), bf16),
                            dma((2,)), dma((3 + n_groups,)), dma((2, 2))] + gather_sems(),
            compiler_params=comm(0), name='forward',
        )(kv_flat, cos_t, sin_t, h_flat, dy_flat, w_query, w_out)

        z_width = q_width + kv_width
        wo_cols, wo_sub = model_dim // 2, q_width // (2 * n_chip * n_sub)
        z_flat, wo_part = pl.pallas_call(
            functools.partial(attend_grad_kernel, n_dev),
            in_specs=[hbm, hbm, hbm, vmem, vmem, vmem, vmem, hbm, hbm],
            out_specs=[vmem, vmem],
            out_shape=(shape(n_rows, z_width), shape(2, n_sub, wo_sub, wo_cols, dtype=f32)),
            scratch_shapes=[pltpu.VMEM((n_groups, rows, head_dim), bf16), pltpu.VMEM((n_groups, rows, head_dim), bf16),
                            pltpu.VMEM((n_seq, seq_len, kv_width), bf16), pltpu.VMEM((head_dim, rows), bf16), pltpu.VMEM((head_dim, rows), bf16), pltpu.VMEM((head_dim, rows), f32),
                            pltpu.VMEM((n_seq, seq_len, kv_width), f32), pltpu.VMEM((2, n_chip, 2, half_len, kv_width), f32),
                            pltpu.VMEM((2, 2, half_len, kv_width), f32), pltpu.VMEM((2, n_chip - 1, 2, half_len, kv_width), f32),
                            pltpu.VMEM((2 * n_rows, q_width), bf16), pltpu.VMEM((2 * n_rows, wo_cols), bf16),
                            pltpu.VMEM((2, n_sub, wo_sub, wo_cols), f32), pltpu.VMEM((2, n_chip - 1, n_sub, wo_sub, wo_cols), f32),
                            dma((5,)), dma((2,)), dma((2,)), dma((2, 2)), dma((2, n_chip - 1, 2)), dma((2, n_chip, 2)), dma((2, n_chip, 2)),
                            dma((2, n_sub)), dma((2, n_chip - 1, n_sub))],
            compiler_params=comm(1), name='attend_grad',
        )(q_rows, kv_all, da_rows, lse, delta, cos_t, sin_t, attn_flat, dy_flat)

        core_width, sub_len = z_width // 2, model_dim // (2 * n_chip * n_sub)
        blk = model_dim // n_chip
        grad_z, grad_wo, out_y, grad_x, grad_gain = pl.pallas_call(
            functools.partial(finish_kernel, n_dev),
            in_specs=[hbm] * 6 + [vmem, hbm, hbm, vmem, vmem],
            out_specs=[pl.BlockSpec(memory_space=pltpu.HBM), hbm, vmem, vmem, vmem],
            out_shape=(shape(model_dim, z_width, dtype=f32), shape(q_width, model_dim, dtype=f32), shape(n_rows, model_dim), shape(n_rows, model_dim),
                       shape(1, model_dim, dtype=f32)),
            scratch_shapes=[pltpu.VMEM((2 * n_rows, model_dim), bf16), pltpu.VMEM((2 * n_rows, core_width), bf16), pltpu.VMEM((n_rows, z_width), bf16),
                            pltpu.VMEM((n_rows, q_width), bf16), pltpu.VMEM((n_rows, model_dim), bf16), pltpu.VMEM((n_rows, model_dim), bf16),
                            pltpu.VMEM((n_rows, model_dim), f32), pltpu.VMEM((2, blk, q_width), bf16), pltpu.VMEM((2, q_width, blk), bf16),
                            pltpu.VMEM((n_dev, 1, model_dim), f32), pltpu.VMEM((2, n_sub, sub_len, core_width), f32),
                            pltpu.VMEM((2, n_chip - 1, n_sub, sub_len, core_width), f32),
                            dma((6,)), dma((2, 2)), dma((2,)), dma((2,)), dma((2, n_sub)), dma((2, n_chip - 1, n_sub))]
            + gather_sems() + gather_sems() + [dma((2, 2, n_sub)), dma((n_dev,)), dma((n_dev,))],
            compiler_params=comm(2), name='finish',
        )(h_flat, z_flat, wo_part, attn_flat, x_flat, dy_flat, gain_row, w_query, w_out, w_key, w_value)
        n_blk = n_dev
        fixed = pl.BlockSpec(memory_space=pltpu.HBM)
        grad_wq, grad_wk, grad_wv, out_y, grad_x = pl.pallas_call(
            deliver_kernel,
            in_specs=[fixed, vmem, vmem],
            out_specs=[fixed] * 5,
            out_shape=(shape(model_dim, q_width, dtype=f32), shape(model_dim, head_dim, dtype=f32), shape(model_dim, head_dim, dtype=f32),
                       shape(n_rows, model_dim), shape(n_rows, model_dim)),
            scratch_shapes=[pltpu.VMEM((n_blk, model_dim // n_blk, z_width), f32), dma((n_blk,)), dma((3 * n_blk + 2,))],
            compiler_params=pltpu.CompilerParams(vmem_limit_bytes=40 * 1024 * 1024), name='deliver',
        )(grad_z, out_y, grad_x)
        return out_y.reshape(tokens.shape), grad_x.reshape(tokens.shape), grad_wq, grad_wk, grad_wv, grad_wo, grad_gain.reshape(model_dim)

    seq_spec = P('dp', 'cp', None)
    rep_spec = P(None, None)
    part_spec = P('dp', None)
    return jax.shard_map(local_fn, mesh=mesh,
                         in_specs=(seq_spec, P('dp', 'cp'), P(None), rep_spec, rep_spec, rep_spec, rep_spec, seq_spec),
                         out_specs=(seq_spec, seq_spec, part_spec, part_spec, part_spec, part_spec, P('dp')),
                         check_vma=False)
```

```python
import functools

import jax
import jax.numpy as jnp
from jax import lax
from jax.experimental import pallas as pl
from jax.experimental.pallas import tpu as pltpu
from jax.sharding import PartitionSpec as P

NORM_EPS = 1e-6
ROPE_BASE = 10000.0
NEG_BIG = -1e30
LOG2_E = 1.4426950408889634
PIECES_PER_BLOCK = 4
VMEM_LIMIT = 60 * 1024 * 1024

NT = (((1,), (1,)), ((), ()))
TN = (((0,), (0,)), ((), ()))
NN = (((1,), (0,)), ((), ()))


def dot(lhs, rhs, dims):
    return lax.dot_general(lhs, rhs, dims, preferred_element_type=jnp.float32)


def rope_tables(positions, head_dim):
    half_dim = head_dim // 2
    inv_freq = ROPE_BASE ** (-(jnp.arange(half_dim, dtype=jnp.float32) * (2.0 / head_dim)))
    angles = positions.astype(jnp.float32)[..., None] * inv_freq
    return jnp.cos(angles), jnp.sin(angles)


def rotate(values, cos_t, sin_t):
    half_dim = values.shape[-1] // 2
    front_half, back_half = values[..., :half_dim], values[..., half_dim:]
    return jnp.concatenate([front_half * cos_t - back_half * sin_t, back_half * cos_t + front_half * sin_t], axis=-1)


def rotate_back(grad_vals, cos_t, sin_t):
    half_dim = grad_vals.shape[-1] // 2
    front_half, back_half = grad_vals[..., :half_dim], grad_vals[..., half_dim:]
    return jnp.concatenate([front_half * cos_t + back_half * sin_t, back_half * cos_t - front_half * sin_t], axis=-1)


def norm_kv_kernel(x_ref, gain_ref, wk_ref, wv_ref, cos_ref, sin_ref, h_ref, kv_ref):
    head_dim = wk_ref.shape[1]
    x_float = x_ref[...].astype(jnp.float32)
    centered = x_float - jnp.mean(x_float, axis=-1, keepdims=True)
    inv_std = lax.rsqrt(jnp.mean(centered * centered, axis=-1, keepdims=True) + NORM_EPS)
    h_norm = (centered * inv_std * gain_ref[...]).astype(jnp.bfloat16)
    h_ref[...] = h_norm
    k_lin = dot(h_norm, wk_ref[...], NN)
    kv_ref[:, :head_dim] = rotate(k_lin, cos_ref[...], sin_ref[...]).astype(jnp.bfloat16)
    kv_ref[:, head_dim:] = dot(h_norm, wv_ref[...], NN).astype(jnp.bfloat16)


def entry_barrier(peers):
    barrier = pltpu.get_barrier_semaphore()
    for peer in peers:
        pl.semaphore_signal(barrier, inc=1, device_id={'cp': peer}, device_id_type=pl.DeviceIdType.MESH)
    pl.semaphore_wait(barrier, len(peers))


def remote(src, dst, send_sem, recv_sem, peer):
    return pltpu.make_async_remote_copy(src_ref=src, dst_ref=dst, send_sem=send_sem, recv_sem=recv_sem,
                                        device_id={'cp': peer}, device_id_type=pl.DeviceIdType.MESH)


def ring_place(n_dev):
    me = lax.axis_index('cp')
    n_chip = n_dev // 2
    chip, core = lax.div(me, 2), lax.rem(me, 2)
    after = lax.rem(chip + 1, n_chip) * 2 + core
    before = lax.rem(chip + n_chip - 1, n_chip) * 2 + core
    partner = chip * 2 + 1 - core
    return n_chip, chip, core, (after, before), partner


def chunk_at(chip, step, way, n_chip):
    if way == 0:
        return lax.rem(chip + 2 * n_chip - 1 - step, n_chip)
    return lax.rem(chip + 1 + step, n_chip)


class RingReduce:
    def __init__(self, n_chip, peers, make_local, local_scr, slots, send_sems, recv_sems):
        self.n_chip, self.peers, self.make_local = n_chip, peers, make_local
        self.local_scr, self.slots, self.send_sems, self.recv_sems = local_scr, slots, send_sems, recv_sems
        self.each = [(sub, way) for sub in range(slots.shape[2]) for way in range(2)]

    def hop(self, step, way, sub, first=False):
        src = self.local_scr.at[way, sub] if first else self.slots.at[way, step - 1, sub]
        return remote(src, self.slots.at[way, step, sub], self.send_sems.at[way, sub], self.recv_sems.at[way, step, sub], self.peers[way])

    def first(self):
        self.make_local(0)
        for sub, way in self.each:
            self.hop(0, way, sub, True).start()

    def middle(self, step, on_sum=None):
        after_first = isinstance(step, int) and step == 1
        if after_first:
            for sub, way in self.each:
                self.hop(0, way, sub, True).wait_send()
        self.make_local(step)
        for sub, way in self.each:
            self.hop(step - 1, way, sub, after_first).wait_recv()
            self.slots[way, step - 1, sub] = self.slots[way, step - 1, sub] + self.local_scr[way, sub]
            if not after_first:
                self.hop(step - 1, way, sub).wait_send()
            if on_sum is None:
                self.hop(step, way, sub).start()
            else:
                on_sum(way, sub)

    def last(self, on_sum):
        self.middle(self.n_chip - 1, on_sum)


class RingGather:
    def __init__(self, n_chip, peers, partner, own, place, n_sub, send_sems, recv_sems, mate_send, mate_recv):
        self.n_chip, self.peers, self.partner, self.own, self.place = n_chip, peers, partner, own, place
        self.send_sems, self.recv_sems, self.mate_send, self.mate_recv = send_sems, recv_sems, mate_send, mate_recv
        self.each = [(sub, way) for sub in range(n_sub) for way in range(2)]

    def onward(self, step, way, sub, first=False):
        src = self.own(way, sub) if first else self.place(step, way, sub)
        return remote(src, self.place(step, way, sub), self.send_sems.at[way, sub], self.recv_sems.at[way, step, sub], self.peers[way])

    def across(self, step, way, sub, first=False):
        src = self.own(way, sub) if first else self.place(step, way, sub)
        return remote(src, self.place(step, way, sub), self.mate_send.at[way, sub], self.mate_recv.at[way, step, sub], self.partner)

    def start_first(self, way, sub):
        self.onward(0, way, sub, True).start()
        self.across(0, way, sub, True).start()

    def first(self):
        for sub, way in self.each:
            self.start_first(way, sub)

    def middle(self, step, last=False):
        after_first = isinstance(step, int) and step == 1
        for sub, way in self.each:
            self.onward(step - 1, way, sub, after_first).wait_send()
            self.onward(step - 1, way, sub, after_first).wait_recv()
            if not last:
                self.onward(step, way, sub).start()
            self.across(step - 1, way, sub, after_first).wait_send()
            self.across(step, way, sub).start()

    def last(self):
        self.middle(self.n_chip - 1, True)

    def drain(self):
        for sub, way in self.each:
            self.across(self.n_chip - 1, way, sub).wait_send()

        def body(step, _):
            for sub, way in self.each:
                self.across(step, way, sub).wait_recv()

        lax.fori_loop(0, self.n_chip, body, None)


def owner_at(chip, step, way, n_chip):
    if way == 0:
        return lax.rem(chip + n_chip - step, n_chip)
    return lax.rem(chip + step, n_chip)


def causal_mask(shape, key_start, query_start, half_len):
    key_idx = key_start + lax.broadcasted_iota(jnp.int32, shape, 0)
    query_idx = query_start + lax.rem(lax.broadcasted_iota(jnp.int32, shape, 1), half_len)
    return key_idx <= query_idx


def forward_kernel(n_dev, kv_ref, cos_ref, sin_ref, h_ref, dy_ref, wq_ref, wo_ref, all_ref, q_ref, da_ref, a_ref, lse_ref, delta_ref,
                   h_scr, dy_scr, kv_scr, q_scr, da_scr, qt_scr, a_scr, acc_scr, max_scr, sum_scr, wq_buf, wo_buf,
                   load_sems, out_sems, w_sems, send_sems, recv_sems, mate_send, mate_recv):
    n_chip, chip, core, peers, partner = ring_place(n_dev)
    me = chip * 2 + core
    n_seq, seq_len, kv_width = kv_scr.shape
    half_len = seq_len // (2 * n_dev)
    n_groups, rows, head_dim = q_scr.shape
    num_heads = rows // half_len
    scale = LOG2_E * head_dim ** -0.5

    def weights(head, slot):
        cols = pl.ds(pl.multiple_of(head * head_dim, head_dim), head_dim)
        return (pltpu.make_async_copy(wq_ref.at[:, cols], wq_buf.at[slot], w_sems.at[0, slot]),
                pltpu.make_async_copy(wo_ref.at[cols, :], wo_buf.at[slot], w_sems.at[1, slot]))

    loads = [pltpu.make_async_copy(h_ref, h_scr, load_sems.at[0]), pltpu.make_async_copy(dy_ref, dy_scr, load_sems.at[1])]
    for load in loads:
        load.start()
    for copy in weights(0, 0):
        copy.start()
    entry_barrier(peers + (partner,))

    def piece_rows(dev, way):
        piece = dev if way == 0 else 2 * n_dev - 1 - dev
        return pl.ds(pl.multiple_of(piece * half_len, half_len), half_len)

    def place(step, way, seq):
        return kv_scr.at[seq, piece_rows(owner_at(chip, step, way, n_chip) * 2 + core, way)]

    def own(way, seq):
        return kv_ref.at[pl.ds((2 * seq + way) * half_len, half_len)]

    ring = RingGather(n_chip, peers, partner, own, place, n_seq, send_sems, recv_sems, mate_send, mate_recv)
    ring.first()
    for seq in range(n_seq):
        for way in range(2):
            kv_scr[seq, piece_rows(me, way), :] = kv_ref[(2 * seq + way) * half_len:(2 * seq + way + 1) * half_len, :]
    max_scr[...] = jnp.full_like(max_scr, NEG_BIG)
    sum_scr[...] = jnp.zeros_like(sum_scr)
    acc_scr[...] = jnp.zeros_like(acc_scr)
    for load in loads:
        load.wait()

    def project(head, slot):
        @pl.when(head < num_heads)
        def _():
            for copy in weights(head, slot):
                copy.wait()

            @pl.when(head + 1 < num_heads)
            def _():
                for copy in weights(head + 1, 1 - slot):
                    copy.start()

            head_rows = pl.ds(pl.multiple_of(head * half_len, half_len), half_len)
            q_new = rotate(dot(h_scr[...], wq_buf[slot], NN), cos_ref[...], sin_ref[...]).astype(jnp.bfloat16)
            da_new = dot(dy_scr[...], wo_buf[slot], NT).astype(jnp.bfloat16)
            for group in range(n_groups):
                q_scr[group, head_rows, :] = q_new[group * half_len:(group + 1) * half_len, :]
                da_scr[group, head_rows, :] = da_new[group * half_len:(group + 1) * half_len, :]

    def block(seq, group, start, key_len, masked):
        index = 2 * seq + group
        keys = pl.ds(pl.multiple_of(start, half_len), key_len)
        scores = dot(kv_scr[seq, keys, :head_dim], qt_scr[index], NN) * scale
        if masked:
            piece = me if group == 0 else 2 * n_dev - 1 - me
            scores = jnp.where(causal_mask(scores.shape, start, piece * half_len, half_len), scores, NEG_BIG)
        old_max = max_scr[index]
        new_max = jnp.maximum(old_max, jnp.max(scores, axis=0, keepdims=True))
        rescale = jnp.exp2(old_max - new_max)
        probs = jnp.exp2(scores - new_max)
        max_scr[index] = new_max
        sum_scr[index] = sum_scr[index] * rescale + jnp.sum(probs, axis=0, keepdims=True)
        acc_scr[index] = acc_scr[index] * rescale + dot(kv_scr[seq, keys, head_dim:], probs.astype(jnp.bfloat16), TN)

    def attend_pair(pair, seq):
        chip_len = 2 * half_len
        for step in range(2):
            for way in range(2):
                ring.across(2 * pair + step, way, seq).wait_recv()
        front = owner_at(chip, 2 * pair, 0, n_chip)
        before = owner_at(chip, 2 * pair + 1, 0, n_chip)
        back = chip + 2 * pair

        @pl.when(front > 0)
        def _():
            block(seq, 1, before * chip_len, 2 * chip_len, False)

        @pl.when(front == 0)
        def _():
            lax.fori_loop(0, 2, lambda i, _: block(seq, 1, (front + i * (before - front)) * chip_len, chip_len, False), None)

        @pl.when(2 * pair < chip)
        def _():
            block(seq, 0, before * chip_len, 2 * chip_len, True)

        @pl.when(2 * pair == chip)
        def _():
            block(seq, 0, front * chip_len, chip_len, True)

        @pl.when(back + 1 < n_chip)
        def _():
            block(seq, 1, (n_dev - 2 - back) * chip_len, 2 * chip_len, True)

        @pl.when(back + 1 == n_chip)
        def _():
            block(seq, 1, (n_dev - 1 - back) * chip_len, chip_len, True)

    def attend(pair, _):
        lax.fori_loop(0, n_seq, lambda seq, _: attend_pair(pair, seq), None)

    def project_two(step):
        lax.fori_loop(2 * step, 2 * step + 2, lambda head, _: project(head, lax.rem(head, 2)), None)

    project_two(0)
    ring.middle(1)

    def projecting(step, _):
        project_two(step)
        ring.middle(step + 1)

    lax.fori_loop(1, 3, projecting, None)
    lax.fori_loop(6, max(num_heads, 6), lambda head, _: project(head, lax.rem(head, 2)), None)
    for group in range(n_groups):
        qt_scr[group] = q_scr[group].T
    ring.middle(4)
    saves = [pltpu.make_async_copy(q_scr, q_ref, out_sems.at[0]), pltpu.make_async_copy(da_scr, da_ref, out_sems.at[1])]
    for save in saves:
        save.start()

    def pairs(pair, _):
        attend(pair, None)

        @pl.when(pair < n_chip - 6)
        def _():
            ring.middle(pair + 5)

        @pl.when(pair == n_chip - 6)
        def _():
            ring.last()

    lax.fori_loop(0, n_chip // 2, pairs, None)
    for sub, way in ring.each:
        ring.across(n_chip - 1, way, sub).wait_send()
    saves.append(pltpu.make_async_copy(kv_scr, all_ref, out_sems.at[2]))
    saves[2].start()

    def finish(index, _):
        attn = (acc_scr[index] / sum_scr[index]).T.astype(jnp.bfloat16)
        lse_ref[index] = max_scr[index] + jnp.log2(sum_scr[index])
        prod = attn.astype(jnp.float32) * da_scr[index].astype(jnp.float32)
        prod = prod[:, :head_dim // 2] + prod[:, head_dim // 2:]
        delta_ref[index] = jnp.sum(prod.T, axis=0, keepdims=True)
        out_rows = pl.ds(pl.multiple_of(index * half_len, half_len), half_len)
        for head in range(num_heads):
            a_scr[out_rows, head * head_dim:(head + 1) * head_dim] = attn[head * half_len:(head + 1) * half_len, :]
        pltpu.make_async_copy(a_scr.at[out_rows], a_ref.at[out_rows], out_sems.at[3 + index]).start()

    lax.fori_loop(0, n_groups, finish, None)
    for index in range(n_groups):
        out_rows = pl.ds(index * half_len, half_len)
        pltpu.make_async_copy(a_scr.at[out_rows], a_ref.at[out_rows], out_sems.at[3 + index]).wait()
    for save in saves:
        save.wait()


def attend_grad_kernel(n_dev, q_ref, kv_ref, da_ref, lse_ref, delta_ref, cos_ref, sin_ref, a_ref, dy_ref, z_ref, wo_ref,
                       q_scr, da_scr, kv_scr, qt_scr, dat_scr, dq_scr, dkv_scr, mate_scr, kv_local, kv_slots, a_scr, dy_scr, wo_local, wo_slots,
                       load_sems, swap_send, swap_recv, kv_send, kv_recv, mate_send, mate_recv, wo_send, wo_recv):
    n_chip, chip, core, peers, partner = ring_place(n_dev)
    me = chip * 2 + core
    rows, head_dim = q_scr.shape[1:]
    n_seq, seq_len, kv_width = dkv_scr.shape
    half_len = seq_len // (2 * n_dev)
    num_heads = rows // half_len
    q_width = num_heads * head_dim
    n_rows = a_ref.shape[0]
    key_len = PIECES_PER_BLOCK * half_len
    scale = LOG2_E * head_dim ** -0.5
    dy_cols = dy_scr.shape[1]
    mine, other = pl.ds(0, n_rows), pl.ds(n_rows, n_rows)

    def cols(which, size):
        return pl.ds(pl.multiple_of(which * size, size), size)

    loads = [
        pltpu.make_async_copy(a_ref, a_scr.at[mine], load_sems.at[0]),
        pltpu.make_async_copy(dy_ref.at[:, cols(core, dy_cols)], dy_scr.at[mine], load_sems.at[1]),
        pltpu.make_async_copy(q_ref, q_scr, load_sems.at[2]),
        pltpu.make_async_copy(da_ref, da_scr, load_sems.at[3]),
        pltpu.make_async_copy(kv_ref, kv_scr, load_sems.at[4]),
    ]
    for load in loads:
        load.start()
    entry_barrier(peers + (partner,))
    swaps = [
        remote(a_ref, a_scr.at[other], swap_send.at[0], swap_recv.at[0], partner),
        remote(dy_ref.at[:, cols(1 - core, dy_cols)], dy_scr.at[other], swap_send.at[1], swap_recv.at[1], partner),
    ]
    for swap in swaps:
        swap.start()
    dkv_scr[...] = jnp.zeros_like(dkv_scr)
    loads[0].wait()
    loads[1].wait()
    for swap in swaps:
        swap.wait_recv()

    def wo_local_term(step):
        n_sub, sub_len = wo_local.shape[1:3]
        way_len = n_sub * sub_len
        for way in range(2):
            first = chunk_at(chip, step, way, n_chip) * (2 * way_len) + way * way_len
            part = dot(a_scr[:, pl.ds(pl.multiple_of(first, way_len), way_len)], dy_scr[...], TN)
            for sub in range(n_sub):
                wo_local[way, sub] = part[sub * sub_len:(sub + 1) * sub_len, :]

    def piece_rows(dev, sub):
        piece = dev if sub == 0 else 2 * n_dev - 1 - dev
        return pl.ds(pl.multiple_of(piece * half_len, half_len), half_len)

    def mate_copy(step, way, sub):
        dev = chunk_at(chip, step, way, n_chip) * 2 + 1 - core
        return remote(dkv_scr.at[way, piece_rows(dev, sub)], mate_scr.at[way, step, sub], mate_send.at[way, step, sub], mate_recv.at[way, step, sub], partner)

    def kv_local_term(step):
        for sub in range(2):
            for way in range(2):
                mate_copy(step, way, sub).wait_recv()
                dev = chunk_at(chip, step, way, n_chip) * 2 + core
                kv_local[way, sub] = dkv_scr[way, piece_rows(dev, sub), :] + mate_scr[way, step, sub]

    wo_ring = RingReduce(n_chip, peers, wo_local_term, wo_local, wo_slots, wo_send, wo_recv)
    kv_ring = RingReduce(n_chip, peers, kv_local_term, kv_local, kv_slots, kv_send, kv_recv)

    def attend_seq(seq):
        def one_group(group, _):
            index = 2 * seq + group
            piece = me + group * (2 * n_dev - 1 - 2 * me)
            last = lax.div(piece, PIECES_PER_BLOCK)
            dq_scr[...] = jnp.zeros_like(dq_scr)
            qt_scr[...] = q_scr[index].T
            dat_scr[...] = da_scr[index].T

            def block(step, masked):
                start = pl.multiple_of(step * key_len, key_len)
                keys = pl.ds(start, key_len)
                k_blk, v_blk = kv_scr[seq, keys, :head_dim], kv_scr[seq, keys, head_dim:]
                probs = jnp.exp2(dot(k_blk, qt_scr[...], NN) * scale - lse_ref[index])
                if masked:
                    probs = jnp.where(causal_mask(probs.shape, start, piece * half_len, half_len), probs, 0.0)
                d_scores = (probs * (dot(v_blk, dat_scr[...], NN) - delta_ref[index])).astype(jnp.bfloat16)
                dq_scr[...] += dot(k_blk, d_scores, TN)
                dkv_scr[seq, keys, :head_dim] += dot(d_scores, q_scr[index], NN) * head_dim ** -0.5
                dkv_scr[seq, keys, head_dim:] += dot(probs.astype(jnp.bfloat16), da_scr[index], NN)

            lax.fori_loop(0, last, lambda step, _: block(step, False), None)
            block(last, True)
            dq = dq_scr[...].T * head_dim ** -0.5
            out_rows = pl.ds(pl.multiple_of(index * half_len, half_len), half_len)
            cos_t, sin_t = cos_ref[out_rows, :], sin_ref[out_rows, :]
            for head in range(num_heads):
                dq_head = dq[head * half_len:(head + 1) * half_len, :]
                z_ref[out_rows, head * head_dim:(head + 1) * head_dim] = rotate_back(dq_head, cos_t, sin_t).astype(jnp.bfloat16)

        lax.fori_loop(0, 2, one_group, None)

        def send_mate(step, _):
            for sub in range(2):
                mate_copy(step, seq, sub).start()

        lax.fori_loop(0, n_chip, send_mate, None)

    wo_ring.first()
    for load in loads[2:]:
        load.wait()
    attend_seq(0)
    wo_ring.middle(1)
    attend_seq(1)
    wo_ring.middle(2)
    kv_ring.first()
    wo_ring.middle(3)
    kv_ring.middle(1)

    def both(step, _):
        wo_ring.middle(step + 2)
        kv_ring.middle(step)

    lax.fori_loop(2, n_chip - 3, both, None)

    def keep_wo(way, sub):
        wo_ref[way, sub] = wo_slots[way, n_chip - 2, sub]

    wo_ring.last(keep_wo)
    kv_ring.middle(n_chip - 3)
    kv_ring.middle(n_chip - 2)

    def keep_kv(way, sub):
        out_rows = slice((2 * way + sub) * half_len, (2 * way + sub + 1) * half_len)
        total = kv_slots[way, n_chip - 2, sub]
        z_ref[out_rows, q_width:q_width + head_dim] = rotate_back(total[:, :head_dim], cos_ref[out_rows, :], sin_ref[out_rows, :]).astype(jnp.bfloat16)
        z_ref[out_rows, q_width + head_dim:] = total[:, head_dim:].astype(jnp.bfloat16)

    kv_ring.last(keep_kv)

    def mates_sent(step, _):
        for way in range(2):
            for sub in range(2):
                mate_copy(step, way, sub).wait_send()

    lax.fori_loop(0, n_chip, mates_sent, None)
    for swap in swaps:
        swap.wait_send()


def finish_kernel(n_dev, h_ref, z_ref, wo_part_ref, a_ref, x_ref, dy_ref, gain_ref, wq_ref, wo_ref, wk_ref, wv_ref,
                  gz_ref, gwo_ref, y_ref, dx_ref, ggain_ref,
                  h_scr, z_scr, zf_scr, a_scr, x_scr, dy_scr, dh_scr, wq_buf, wo_buf, gain_slots, local_scr, slots,
                  load_sems, w_sems, swap_send, swap_recv, send_sems, recv_sems, g1_send, g1_recv, m1_send, m1_recv,
                  g2_send, g2_recv, m2_send, m2_recv, keep_sems, gain_send, gain_recv):
    n_chip, chip, core, peers, partner = ring_place(n_dev)
    me = chip * 2 + core
    n_rows, model_dim = h_ref.shape
    core_width = z_scr.shape[1]
    q_width = a_ref.shape[1]
    head_dim = wk_ref.shape[1]
    n_sub, sub_len = local_scr.shape[1:3]
    way_len = n_sub * sub_len
    wo_sub_len, wo_width = wo_part_ref.shape[2:]
    wo_way_len = n_sub * wo_sub_len
    blk = model_dim // n_chip
    mine, other = pl.ds(0, n_rows), pl.ds(n_rows, n_rows)

    def cols(which, size):
        return pl.ds(pl.multiple_of(which * size, size), size)

    def wq_load(index, slot):
        return pltpu.make_async_copy(wq_ref.at[cols(index, blk), :], wq_buf.at[slot], w_sems.at[0, slot])

    def wo_load(index, slot):
        return pltpu.make_async_copy(wo_ref.at[:, cols(index, blk)], wo_buf.at[slot], w_sems.at[1, slot])

    loads = [
        pltpu.make_async_copy(h_ref, h_scr.at[mine], load_sems.at[0]),
        pltpu.make_async_copy(z_ref.at[:, cols(core, core_width)], z_scr.at[mine], load_sems.at[1]),
        pltpu.make_async_copy(z_ref, zf_scr, load_sems.at[2]),
        pltpu.make_async_copy(a_ref, a_scr, load_sems.at[3]),
        pltpu.make_async_copy(x_ref, x_scr, load_sems.at[4]),
        pltpu.make_async_copy(dy_ref, dy_scr, load_sems.at[5]),
    ]
    for load in loads:
        load.start()
    wq_load(0, 0).start()
    wo_load(0, 0).start()
    barrier = pltpu.get_barrier_semaphore()
    for offset in range(1, n_dev):
        pl.semaphore_signal(barrier, inc=1, device_id={'cp': lax.rem(me + offset, n_dev)}, device_id_type=pl.DeviceIdType.MESH)
    pl.semaphore_wait(barrier, n_dev - 1)

    def wo_place(step, way, sub):
        first = owner_at(chip, step, way, n_chip) * (2 * wo_way_len) + way * wo_way_len + sub * wo_sub_len
        return gwo_ref.at[pl.ds(pl.multiple_of(first, wo_sub_len), wo_sub_len), cols(core, wo_width)]

    def z_place(step, way, sub):
        first = owner_at(chip, step, way, n_chip) * (2 * way_len) + way * way_len + sub * sub_len
        return gz_ref.at[pl.ds(pl.multiple_of(first, sub_len), sub_len), cols(core, core_width)]

    swaps = [
        remote(h_ref, h_scr.at[other], swap_send.at[0], swap_recv.at[0], partner),
        remote(z_ref.at[:, cols(1 - core, core_width)], z_scr.at[other], swap_send.at[1], swap_recv.at[1], partner),
    ]
    for swap in swaps:
        swap.start()
    wo_gather = RingGather(n_chip, peers, partner, lambda way, sub: wo_part_ref.at[way, sub], wo_place, n_sub, g1_send, g1_recv, m1_send, m1_recv)
    z_gather = RingGather(n_chip, peers, partner, lambda way, sub: slots.at[way, n_chip - 2, sub], z_place, n_sub, g2_send, g2_recv, m2_send, m2_recv)
    keeps = ([pltpu.make_async_copy(wo_part_ref.at[way, sub], wo_place(0, way, sub), keep_sems.at[0, way, sub]) for sub, way in wo_gather.each],
             [pltpu.make_async_copy(slots.at[way, n_chip - 2, sub], z_place(0, way, sub), keep_sems.at[1, way, sub]) for sub, way in wo_gather.each])
    wo_gather.first()
    for keep in keeps[0]:
        keep.start()

    def local_term(step):
        for way in range(2):
            first = chunk_at(chip, step, way, n_chip) * (2 * way_len) + way * way_len
            part = dot(h_scr[:, pl.ds(pl.multiple_of(first, way_len), way_len)], z_scr[...], TN)
            for sub in range(n_sub):
                local_scr[way, sub] = part[sub * sub_len:(sub + 1) * sub_len, :]

    z_ring = RingReduce(n_chip, peers, local_term, local_scr, slots, send_sems, recv_sems)

    def d_hidden(index, slot):
        wq_load(index, slot).wait()

        @pl.when(index + 1 < n_chip)
        def _():
            wq_load(index + 1, 1 - slot).start()

        rows = cols(index, blk)
        dh_scr[:, rows] = (dot(zf_scr[:, :q_width], wq_buf[slot], NT) + dot(zf_scr[:, q_width:q_width + head_dim], wk_ref[rows, :], NT)
                           + dot(zf_scr[:, q_width + head_dim:], wv_ref[rows, :], NT))

    def out_block(index, slot):
        wo_load(index, slot).wait()

        @pl.when(index + 1 < n_chip)
        def _():
            wo_load(index + 1, 1 - slot).start()

        where = cols(index, blk)
        o_blk = dot(a_scr[...], wo_buf[slot], NN).astype(jnp.bfloat16)
        y_ref[:, where] = (x_scr[:, where].astype(jnp.float32) + o_blk.astype(jnp.float32)).astype(jnp.bfloat16)

    def norm_grad(index, _):
        rows = pl.ds(pl.multiple_of(index * 32, 32), 32)
        x_float = x_scr[rows, :].astype(jnp.float32)
        centered = x_float - jnp.mean(x_float, axis=-1, keepdims=True)
        inv_std = lax.rsqrt(jnp.mean(centered * centered, axis=-1, keepdims=True) + NORM_EPS)
        x_hat = centered * inv_std
        d_h = dh_scr[rows, :]
        gain_slots[me] += jnp.sum(d_h * x_hat, axis=0, keepdims=True)
        d_hat = d_h * gain_ref[...]
        mean_d = jnp.mean(d_hat, axis=-1, keepdims=True)
        mean_dx = jnp.mean(d_hat * x_hat, axis=-1, keepdims=True)
        dx_ref[rows, :] = (dy_scr[rows, :].astype(jnp.float32) + inv_std * (d_hat - mean_d - x_hat * mean_dx)).astype(jnp.bfloat16)

    def gain_copy(offset):
        return remote(gain_slots.at[me], gain_slots.at[me], gain_send.at[offset], gain_recv.at[offset], lax.rem(me + offset, n_dev))

    loads[0].wait()
    loads[1].wait()
    for swap in swaps:
        swap.wait_recv()
    z_ring.first()
    for load in loads[2:]:
        load.wait()
    wo_gather.middle(1)
    z_ring.middle(1)
    d_hidden(0, 0)

    def phase_one(step, _):
        wo_gather.middle(step)
        z_ring.middle(step)
        d_hidden(step - 1, lax.rem(step - 1, 2))

    lax.fori_loop(2, n_chip - 1, phase_one, None)
    wo_gather.last()

    def pass_on(way, sub):
        z_gather.start_first(way, sub)
        keeps[1][2 * sub + way].start()

    z_ring.last(pass_on)
    d_hidden(n_chip - 2, (n_chip - 2) % 2)
    d_hidden(n_chip - 1, (n_chip - 1) % 2)
    gain_slots[me] = jnp.zeros(gain_slots.shape[1:], jnp.float32)
    lax.fori_loop(0, n_rows // 32, norm_grad, None)
    for offset in range(1, n_dev):
        gain_copy(offset).start()
    z_gather.middle(1)
    out_block(0, 0)
    out_block(1, 1)

    def phase_two(step, _):
        z_gather.middle(step)
        out_block(step, lax.rem(step, 2))

    lax.fori_loop(2, n_chip - 1, phase_two, None)
    out_block(n_chip - 1, (n_chip - 1) % 2)
    z_gather.last()
    for offset in range(1, n_dev):
        gain_copy(offset).wait_recv()
    total = gain_slots[0]
    for dev in range(1, n_dev):
        total = total + gain_slots[dev]
    ggain_ref[...] = total
    wo_gather.drain()
    z_gather.drain()
    for keep in keeps[0] + keeps[1]:
        keep.wait()
    for swap in swaps:
        swap.wait_send()
    for offset in range(1, n_dev):
        gain_copy(offset).wait_send()


def deliver_kernel(gz_ref, gwo_ref, y_ref, dx_ref, wq_out, wk_out, wv_out, wo_out, y_out, dx_out, gz_buf, gwo_buf, y_buf, dx_buf, in_sems, out_sems):
    n_blk, z_len, _ = gz_buf.shape
    wo_len = gwo_buf.shape[1]
    q_width, head_dim = wq_out.shape[1], wk_out.shape[1]
    jobs = []
    for i in range(n_blk):
        rows = pl.ds(i * z_len, z_len)
        parts = [(gz_buf.at[i, :, pl.ds(first, out.shape[1])], out.at[rows]) for out, first in ((wq_out, 0), (wk_out, q_width), (wv_out, q_width + head_dim))]
        jobs.append((gz_ref.at[rows], gz_buf.at[i], parts))
        rows = pl.ds(i * wo_len, wo_len)
        jobs.append((gwo_ref.at[rows], gwo_buf.at[i], [(gwo_buf.at[i], wo_out.at[rows])]))
    for src, buf, out in ((y_ref, y_buf, y_out), (dx_ref, dx_buf, dx_out)):
        jobs.append((src, buf, [(buf, out)]))
    reads = [pltpu.make_async_copy(src, buf, in_sems.at[i]) for i, (src, buf, _) in enumerate(jobs)]
    for read in reads:
        read.start()
    writes = []
    for read, (_, _, parts) in zip(reads, jobs):
        read.wait()
        for src, dst in parts:
            writes.append(pltpu.make_async_copy(src, dst, out_sems.at[len(writes)]))
            writes[-1].start()
    for write in writes:
        write.wait()


def solution(mesh):
    n_dev = mesh.shape['cp']
    n_chip, n_sub = n_dev // 2, 2

    def local_fn(tokens, positions, norm_gain, w_query, w_key, w_value, w_out, d_out):
        n_seq, blk_len, model_dim = tokens.shape
        head_dim = w_key.shape[1]
        num_heads = w_query.shape[1] // head_dim
        q_width, kv_width = num_heads * head_dim, 2 * head_dim
        half_len, half = blk_len // 2, head_dim // 2
        n_rows, n_groups = n_seq * blk_len, 2 * n_seq
        rows = num_heads * half_len
        seq_len = n_dev * blk_len
        bf16, f32 = jnp.bfloat16, jnp.float32
        dma = pltpu.SemaphoreType.DMA
        vmem = pl.BlockSpec(memory_space=pltpu.VMEM)
        hbm = pl.BlockSpec(memory_space=pl.ANY)
        params = pltpu.CompilerParams(vmem_limit_bytes=VMEM_LIMIT)

        def comm(ident):
            return pltpu.CompilerParams(vmem_limit_bytes=VMEM_LIMIT, collective_id=ident, has_side_effects=True)

        def shape(*dims, dtype=bf16):
            return jax.ShapeDtypeStruct(dims, dtype)

        def gather_sems():
            return [dma((2, n_sub)), dma((2, n_chip - 1, n_sub)), dma((2, n_sub)), dma((2, n_chip, n_sub))]

        x_flat = tokens.reshape(n_rows, model_dim)
        dy_flat = d_out.reshape(n_rows, model_dim)
        gain_row = norm_gain.reshape(1, model_dim)
        cos_t, sin_t = rope_tables(positions.reshape(n_rows), head_dim)
        h_flat, kv_flat = pl.pallas_call(
            norm_kv_kernel,
            out_shape=(shape(n_rows, model_dim), shape(n_rows, kv_width)),
            compiler_params=params, name='norm_kv',
        )(x_flat, gain_row, w_key, w_value, cos_t, sin_t)

        groups = (n_groups, rows, head_dim)
        kv_all, q_rows, da_rows, attn_flat, lse, delta = pl.pallas_call(
            functools.partial(forward_kernel, n_dev),
            in_specs=[vmem, vmem, vmem, hbm, hbm, hbm, hbm],
            out_specs=[hbm, hbm, hbm, hbm, vmem, vmem],
            out_shape=(shape(n_seq, seq_len, kv_width), shape(*groups), shape(*groups), shape(n_rows, q_width),
                       shape(n_groups, 1, rows, dtype=f32), shape(n_groups, 1, rows, dtype=f32)),
            scratch_shapes=[pltpu.VMEM((n_rows, model_dim), bf16), pltpu.VMEM((n_rows, model_dim), bf16), pltpu.VMEM((n_seq, seq_len, kv_width), bf16),
                            pltpu.VMEM(groups, bf16), pltpu.VMEM(groups, bf16), pltpu.VMEM((n_groups, head_dim, rows), bf16), pltpu.VMEM((n_rows, q_width), bf16),
                            pltpu.VMEM((n_groups, head_dim, rows), f32), pltpu.VMEM((n_groups, 1, rows), f32), pltpu.VMEM((n_groups, 1, rows), f32),
                            pltpu.VMEM((2, model_dim, head_dim), bf16), pltpu.VMEM((2, head_dim, model_dim), bf16),
                            dma((2,)), dma((3 + n_groups,)), dma((2, 2))] + gather_sems(),
            compiler_params=comm(0), name='forward',
        )(kv_flat, cos_t, sin_t, h_flat, dy_flat, w_query, w_out)

        z_width = q_width + kv_width
        wo_cols, wo_sub = model_dim // 2, q_width // (2 * n_chip * n_sub)
        z_flat, wo_part = pl.pallas_call(
            functools.partial(attend_grad_kernel, n_dev),
            in_specs=[hbm, hbm, hbm, vmem, vmem, vmem, vmem, hbm, hbm],
            out_specs=[vmem, vmem],
            out_shape=(shape(n_rows, z_width), shape(2, n_sub, wo_sub, wo_cols, dtype=f32)),
            scratch_shapes=[pltpu.VMEM((n_groups, rows, head_dim), bf16), pltpu.VMEM((n_groups, rows, head_dim), bf16),
                            pltpu.VMEM((n_seq, seq_len, kv_width), bf16), pltpu.VMEM((head_dim, rows), bf16), pltpu.VMEM((head_dim, rows), bf16), pltpu.VMEM((head_dim, rows), f32),
                            pltpu.VMEM((n_seq, seq_len, kv_width), f32), pltpu.VMEM((2, n_chip, 2, half_len, kv_width), f32),
                            pltpu.VMEM((2, 2, half_len, kv_width), f32), pltpu.VMEM((2, n_chip - 1, 2, half_len, kv_width), f32),
                            pltpu.VMEM((2 * n_rows, q_width), bf16), pltpu.VMEM((2 * n_rows, wo_cols), bf16),
                            pltpu.VMEM((2, n_sub, wo_sub, wo_cols), f32), pltpu.VMEM((2, n_chip - 1, n_sub, wo_sub, wo_cols), f32),
                            dma((5,)), dma((2,)), dma((2,)), dma((2, 2)), dma((2, n_chip - 1, 2)), dma((2, n_chip, 2)), dma((2, n_chip, 2)),
                            dma((2, n_sub)), dma((2, n_chip - 1, n_sub))],
            compiler_params=comm(1), name='attend_grad',
        )(q_rows, kv_all, da_rows, lse, delta, cos_t, sin_t, attn_flat, dy_flat)

        core_width, sub_len = z_width // 2, model_dim // (2 * n_chip * n_sub)
        blk = model_dim // n_chip
        grad_z, grad_wo, out_y, grad_x, grad_gain = pl.pallas_call(
            functools.partial(finish_kernel, n_dev),
            in_specs=[hbm] * 6 + [vmem, hbm, hbm, vmem, vmem],
            out_specs=[pl.BlockSpec(memory_space=pltpu.HBM), hbm, vmem, vmem, vmem],
            out_shape=(shape(model_dim, z_width, dtype=f32), shape(q_width, model_dim, dtype=f32), shape(n_rows, model_dim), shape(n_rows, model_dim),
                       shape(1, model_dim, dtype=f32)),
            scratch_shapes=[pltpu.VMEM((2 * n_rows, model_dim), bf16), pltpu.VMEM((2 * n_rows, core_width), bf16), pltpu.VMEM((n_rows, z_width), bf16),
                            pltpu.VMEM((n_rows, q_width), bf16), pltpu.VMEM((n_rows, model_dim), bf16), pltpu.VMEM((n_rows, model_dim), bf16),
                            pltpu.VMEM((n_rows, model_dim), f32), pltpu.VMEM((2, blk, q_width), bf16), pltpu.VMEM((2, q_width, blk), bf16),
                            pltpu.VMEM((n_dev, 1, model_dim), f32), pltpu.VMEM((2, n_sub, sub_len, core_width), f32),
                            pltpu.VMEM((2, n_chip - 1, n_sub, sub_len, core_width), f32),
                            dma((6,)), dma((2, 2)), dma((2,)), dma((2,)), dma((2, n_sub)), dma((2, n_chip - 1, n_sub))]
            + gather_sems() + gather_sems() + [dma((2, 2, n_sub)), dma((n_dev,)), dma((n_dev,))],
            compiler_params=comm(2), name='finish',
        )(h_flat, z_flat, wo_part, attn_flat, x_flat, dy_flat, gain_row, w_query, w_out, w_key, w_value)
        n_blk = n_dev
        grad_wq, grad_wk, grad_wv, grad_wo, out_y, grad_x = pl.pallas_call(
            deliver_kernel,
            in_specs=[hbm] * 4,
            out_specs=[hbm] * 6,
            out_shape=(shape(model_dim, q_width, dtype=f32), shape(model_dim, head_dim, dtype=f32), shape(model_dim, head_dim, dtype=f32),
                       shape(q_width, model_dim, dtype=f32), shape(n_rows, model_dim), shape(n_rows, model_dim)),
            scratch_shapes=[pltpu.VMEM((n_blk, model_dim // n_blk, z_width), f32), pltpu.VMEM((n_blk, q_width // n_blk, model_dim), f32),
                            pltpu.VMEM((n_rows, model_dim), bf16), pltpu.VMEM((n_rows, model_dim), bf16),
                            dma((2 * n_blk + 2,)), dma((4 * n_blk + 2,))],
            compiler_params=params, name='deliver',
        )(grad_z, grad_wo, out_y, grad_x)
        return out_y.reshape(tokens.shape), grad_x.reshape(tokens.shape), grad_wq, grad_wk, grad_wv, grad_wo, grad_gain.reshape(model_dim)

    seq_spec = P('dp', 'cp', None)
    rep_spec = P(None, None)
    part_spec = P('dp', None)
    return jax.shard_map(local_fn, mesh=mesh,
                         in_specs=(seq_spec, P('dp', 'cp'), P(None), rep_spec, rep_spec, rep_spec, rep_spec, seq_spec),
                         out_specs=(seq_spec, seq_spec, part_spec, part_spec, part_spec, part_spec, P('dp')),
                         check_vma=False)
```

```python
import functools

import jax
import jax.numpy as jnp
from jax import lax
from jax.experimental import pallas as pl
from jax.experimental.pallas import tpu as pltpu
from jax.sharding import PartitionSpec as P

NORM_EPS = 1e-6
ROPE_BASE = 10000.0
NEG_BIG = -1e30
LOG2_E = 1.4426950408889634
PIECES_PER_BLOCK = 4
VMEM_LIMIT = 60 * 1024 * 1024

NT = (((1,), (1,)), ((), ()))
TN = (((0,), (0,)), ((), ()))
NN = (((1,), (0,)), ((), ()))


def dot(lhs, rhs, dims):
    return lax.dot_general(lhs, rhs, dims, preferred_element_type=jnp.float32)


def rope_tables(positions, head_dim):
    half_dim = head_dim // 2
    inv_freq = ROPE_BASE ** (-(jnp.arange(half_dim, dtype=jnp.float32) * (2.0 / head_dim)))
    angles = positions.astype(jnp.float32)[..., None] * inv_freq
    return jnp.cos(angles), jnp.sin(angles)


def rotate(values, cos_t, sin_t):
    half_dim = values.shape[-1] // 2
    front_half, back_half = values[..., :half_dim], values[..., half_dim:]
    return jnp.concatenate([front_half * cos_t - back_half * sin_t, back_half * cos_t + front_half * sin_t], axis=-1)


def rotate_back(grad_vals, cos_t, sin_t):
    half_dim = grad_vals.shape[-1] // 2
    front_half, back_half = grad_vals[..., :half_dim], grad_vals[..., half_dim:]
    return jnp.concatenate([front_half * cos_t + back_half * sin_t, back_half * cos_t - front_half * sin_t], axis=-1)


def norm_kv_kernel(x_ref, gain_ref, wk_ref, wv_ref, cos_ref, sin_ref, h_ref, kv_ref):
    head_dim = wk_ref.shape[1]
    x_float = x_ref[...].astype(jnp.float32)
    centered = x_float - jnp.mean(x_float, axis=-1, keepdims=True)
    inv_std = lax.rsqrt(jnp.mean(centered * centered, axis=-1, keepdims=True) + NORM_EPS)
    h_norm = (centered * inv_std * gain_ref[...]).astype(jnp.bfloat16)
    h_ref[...] = h_norm
    k_lin = dot(h_norm, wk_ref[...], NN)
    kv_ref[:, :head_dim] = rotate(k_lin, cos_ref[...], sin_ref[...]).astype(jnp.bfloat16)
    kv_ref[:, head_dim:] = dot(h_norm, wv_ref[...], NN).astype(jnp.bfloat16)


def entry_barrier(peers):
    barrier = pltpu.get_barrier_semaphore()
    for peer in peers:
        pl.semaphore_signal(barrier, inc=1, device_id={'cp': peer}, device_id_type=pl.DeviceIdType.MESH)
    pl.semaphore_wait(barrier, len(peers))


def remote(src, dst, send_sem, recv_sem, peer):
    return pltpu.make_async_remote_copy(src_ref=src, dst_ref=dst, send_sem=send_sem, recv_sem=recv_sem,
                                        device_id={'cp': peer}, device_id_type=pl.DeviceIdType.MESH)


def ring_place(n_dev):
    me = lax.axis_index('cp')
    n_chip = n_dev // 2
    chip, core = lax.div(me, 2), lax.rem(me, 2)
    after = lax.rem(chip + 1, n_chip) * 2 + core
    before = lax.rem(chip + n_chip - 1, n_chip) * 2 + core
    partner = chip * 2 + 1 - core
    return n_chip, chip, core, (after, before), partner


def chunk_at(chip, step, way, n_chip):
    if way == 0:
        return lax.rem(chip + 2 * n_chip - 1 - step, n_chip)
    return lax.rem(chip + 1 + step, n_chip)


class RingReduce:
    def __init__(self, n_chip, peers, make_local, local_scr, slots, send_sems, recv_sems, first_buf=None):
        self.n_chip, self.peers, self.make_local, self.first_buf = n_chip, peers, make_local, first_buf
        self.local_scr, self.slots, self.send_sems, self.recv_sems = local_scr, slots, send_sems, recv_sems
        self.each = [(sub, way) for sub in range(slots.shape[2]) for way in range(2)]

    def hop(self, step, way, sub, first=False):
        buf = self.local_scr if self.first_buf is None else self.first_buf
        src = buf.at[way, sub] if first else self.slots.at[way, step - 1, sub]
        return remote(src, self.slots.at[way, step, sub], self.send_sems.at[way, sub], self.recv_sems.at[way, step, sub], self.peers[way])

    def arrival(self, step, way, sub):
        slot = self.slots.at[way, step, sub]
        return remote(slot, slot, self.send_sems.at[way, sub], self.recv_sems.at[way, step, sub], self.peers[way])

    def serve(self, step, sub):
        for way in range(2):
            self.arrival(step - 1, way, sub).wait_recv()
            self.slots[way, step - 1, sub] = self.slots[way, step - 1, sub] + self.local_scr[way, sub]
            self.arrival(step - 1, way, sub).wait_send()
            self.hop(step, way, sub).start()

    def first(self):
        self.make_local(0)
        if self.first_buf is not None:
            self.first_buf[...] = self.local_scr[...]
        for sub, way in self.each:
            self.hop(0, way, sub, True).start()

    def middle(self, step, on_sum=None):
        after_first = isinstance(step, int) and step == 1
        if after_first:
            for sub, way in self.each:
                self.hop(0, way, sub, True).wait_send()
        self.make_local(step)
        for sub, way in self.each:
            self.hop(step - 1, way, sub, after_first).wait_recv()
            self.slots[way, step - 1, sub] = self.slots[way, step - 1, sub] + self.local_scr[way, sub]
            if not after_first:
                self.hop(step - 1, way, sub).wait_send()
            if on_sum is None:
                self.hop(step, way, sub).start()
            else:
                on_sum(way, sub)

    def last(self, on_sum):
        self.middle(self.n_chip - 1, on_sum)


class RingGather:
    def __init__(self, n_chip, peers, partner, own, place, n_sub, send_sems, recv_sems, mate_send, mate_recv):
        self.n_chip, self.peers, self.partner, self.own, self.place = n_chip, peers, partner, own, place
        self.send_sems, self.recv_sems, self.mate_send, self.mate_recv = send_sems, recv_sems, mate_send, mate_recv
        self.each = [(sub, way) for sub in range(n_sub) for way in range(2)]

    def onward(self, step, way, sub, first=False):
        src = self.own(way, sub) if first else self.place(step, way, sub)
        return remote(src, self.place(step, way, sub), self.send_sems.at[way, sub], self.recv_sems.at[way, step, sub], self.peers[way])

    def across(self, step, way, sub, first=False):
        src = self.own(way, sub) if first else self.place(step, way, sub)
        return remote(src, self.place(step, way, sub), self.mate_send.at[way, sub], self.mate_recv.at[way, step, sub], self.partner)

    def start_first(self, way, sub):
        self.onward(0, way, sub, True).start()
        self.across(0, way, sub, True).start()

    def first(self):
        for sub, way in self.each:
            self.start_first(way, sub)

    def middle(self, step, last=False):
        after_first = isinstance(step, int) and step == 1
        for sub, way in self.each:
            self.onward(step - 1, way, sub, after_first).wait_send()
            self.onward(step - 1, way, sub, after_first).wait_recv()
            if not last:
                self.onward(step, way, sub).start()
            self.across(step - 1, way, sub, after_first).wait_send()
            self.across(step, way, sub).start()

    def last(self):
        self.middle(self.n_chip - 1, True)

    def drain(self):
        for sub, way in self.each:
            self.across(self.n_chip - 1, way, sub).wait_send()

        def body(step, _):
            for sub, way in self.each:
                self.across(step, way, sub).wait_recv()

        lax.fori_loop(0, self.n_chip, body, None)


def owner_at(chip, step, way, n_chip):
    if way == 0:
        return lax.rem(chip + n_chip - step, n_chip)
    return lax.rem(chip + step, n_chip)


def causal_mask(shape, key_start, query_start, half_len):
    key_idx = key_start + lax.broadcasted_iota(jnp.int32, shape, 0)
    query_idx = query_start + lax.rem(lax.broadcasted_iota(jnp.int32, shape, 1), half_len)
    return key_idx <= query_idx


def forward_kernel(n_dev, kv_ref, cos_ref, sin_ref, h_ref, dy_ref, wq_ref, wo_ref, all_ref, q_ref, da_ref, a_ref, dyc_ref, lse_ref, delta_ref,
                   h_scr, dy_scr, kv_scr, q_scr, da_scr, qt_scr, a_scr, acc_scr, max_scr, sum_scr, wq_buf, wo_buf,
                   load_sems, out_sems, w_sems, swap_send, swap_recv, send_sems, recv_sems, mate_send, mate_recv):
    n_chip, chip, core, peers, partner = ring_place(n_dev)
    me = chip * 2 + core
    n_rows, dy_cols = h_scr.shape[0], dyc_ref.shape[1]
    n_seq, seq_len, kv_width = kv_scr.shape
    half_len = seq_len // (2 * n_dev)
    n_groups, rows, head_dim = q_scr.shape
    num_heads = rows // half_len
    scale = LOG2_E * head_dim ** -0.5

    def weights(head, slot):
        cols = pl.ds(pl.multiple_of(head * head_dim, head_dim), head_dim)
        return (pltpu.make_async_copy(wq_ref.at[:, cols], wq_buf.at[slot], w_sems.at[0, slot]),
                pltpu.make_async_copy(wo_ref.at[cols, :], wo_buf.at[slot], w_sems.at[1, slot]))

    loads = [pltpu.make_async_copy(h_ref, h_scr, load_sems.at[0]), pltpu.make_async_copy(dy_ref, dy_scr, load_sems.at[1])]
    for load in loads:
        load.start()
    for copy in weights(0, 0):
        copy.start()
    entry_barrier(peers + (partner,))

    def piece_rows(dev, way):
        piece = dev if way == 0 else 2 * n_dev - 1 - dev
        return pl.ds(pl.multiple_of(piece * half_len, half_len), half_len)

    def place(step, way, seq):
        return kv_scr.at[seq, piece_rows(owner_at(chip, step, way, n_chip) * 2 + core, way)]

    def own(way, seq):
        return kv_ref.at[pl.ds((2 * seq + way) * half_len, half_len)]

    ring = RingGather(n_chip, peers, partner, own, place, n_seq, send_sems, recv_sems, mate_send, mate_recv)
    ring.first()
    for seq in range(n_seq):
        for way in range(2):
            kv_scr[seq, piece_rows(me, way), :] = kv_ref[(2 * seq + way) * half_len:(2 * seq + way + 1) * half_len, :]
    max_scr[...] = jnp.full_like(max_scr, NEG_BIG)
    sum_scr[...] = jnp.zeros_like(sum_scr)
    acc_scr[...] = jnp.zeros_like(acc_scr)
    for load in loads:
        load.wait()

    def half_cols(which):
        return pl.ds(pl.multiple_of(which * dy_cols, dy_cols), dy_cols)

    dy_keep = pltpu.make_async_copy(dy_scr.at[:, half_cols(core)], dyc_ref.at[pl.ds(0, n_rows)], load_sems.at[2])
    dy_swap = remote(dy_scr.at[:, half_cols(1 - core)], dyc_ref.at[pl.ds(n_rows, n_rows)], swap_send.at[n_groups], swap_recv.at[n_groups], partner)
    dy_keep.start()
    dy_swap.start()

    def project(head, slot):
        @pl.when(head < num_heads)
        def _():
            for copy in weights(head, slot):
                copy.wait()

            @pl.when(head + 1 < num_heads)
            def _():
                for copy in weights(head + 1, 1 - slot):
                    copy.start()

            head_rows = pl.ds(pl.multiple_of(head * half_len, half_len), half_len)
            q_new = rotate(dot(h_scr[...], wq_buf[slot], NN), cos_ref[...], sin_ref[...]).astype(jnp.bfloat16)
            da_new = dot(dy_scr[...], wo_buf[slot], NT).astype(jnp.bfloat16)
            for group in range(n_groups):
                q_scr[group, head_rows, :] = q_new[group * half_len:(group + 1) * half_len, :]
                da_scr[group, head_rows, :] = da_new[group * half_len:(group + 1) * half_len, :]

    def block(seq, group, start, key_len, masked):
        index = 2 * seq + group
        keys = pl.ds(pl.multiple_of(start, half_len), key_len)
        scores = dot(kv_scr[seq, keys, :head_dim], qt_scr[index], NN) * scale
        if masked:
            piece = me if group == 0 else 2 * n_dev - 1 - me
            scores = jnp.where(causal_mask(scores.shape, start, piece * half_len, half_len), scores, NEG_BIG)
        old_max = max_scr[index]
        new_max = jnp.maximum(old_max, jnp.max(scores, axis=0, keepdims=True))
        rescale = jnp.exp2(old_max - new_max)
        probs = jnp.exp2(scores - new_max)
        max_scr[index] = new_max
        sum_scr[index] = sum_scr[index] * rescale + jnp.sum(probs, axis=0, keepdims=True)
        acc_scr[index] = acc_scr[index] * rescale + dot(kv_scr[seq, keys, head_dim:], probs.astype(jnp.bfloat16), TN)

    def attend_pair(pair, seq):
        chip_len = 2 * half_len
        for step in range(2):
            for way in range(2):
                ring.across(2 * pair + step, way, seq).wait_recv()
        front = owner_at(chip, 2 * pair, 0, n_chip)
        before = owner_at(chip, 2 * pair + 1, 0, n_chip)
        back = chip + 2 * pair

        @pl.when(front > 0)
        def _():
            block(seq, 1, before * chip_len, 2 * chip_len, False)

        @pl.when(front == 0)
        def _():
            lax.fori_loop(0, 2, lambda i, _: block(seq, 1, (front + i * (before - front)) * chip_len, chip_len, False), None)

        @pl.when(2 * pair < chip)
        def _():
            block(seq, 0, before * chip_len, 2 * chip_len, True)

        @pl.when(2 * pair == chip)
        def _():
            block(seq, 0, front * chip_len, chip_len, True)

        @pl.when(back + 1 < n_chip)
        def _():
            block(seq, 1, (n_dev - 2 - back) * chip_len, 2 * chip_len, True)

        @pl.when(back + 1 == n_chip)
        def _():
            block(seq, 1, (n_dev - 1 - back) * chip_len, chip_len, True)

    def project_two(step):
        lax.fori_loop(2 * step, 2 * step + 2, lambda head, _: project(head, lax.rem(head, 2)), None)

    project_two(0)
    ring.middle(1)

    def projecting(step, _):
        project_two(step)
        ring.middle(step + 1)

    lax.fori_loop(1, 3, projecting, None)
    lax.fori_loop(6, max(num_heads, 6), lambda head, _: project(head, lax.rem(head, 2)), None)
    for group in range(n_groups):
        qt_scr[group] = q_scr[group].T
    ring.middle(4)
    saves = [pltpu.make_async_copy(q_scr, q_ref, out_sems.at[0]), pltpu.make_async_copy(da_scr, da_ref, out_sems.at[1])]
    for save in saves:
        save.start()

    def attend(turn, _):
        attend_pair(lax.div(turn, n_seq), lax.rem(turn, n_seq))

        @pl.when(turn < n_chip - 6)
        def _():
            ring.middle(turn + 5)

        @pl.when(turn == n_chip - 6)
        def _():
            ring.last()

    lax.fori_loop(0, n_chip // 2 * n_seq, attend, None)
    for sub, way in ring.each:
        ring.across(n_chip - 1, way, sub).wait_send()
    saves.append(pltpu.make_async_copy(kv_scr, all_ref, out_sems.at[2]))
    saves[2].start()

    def finish(index, _):
        attn = (acc_scr[index] / sum_scr[index]).T.astype(jnp.bfloat16)
        lse_ref[index] = max_scr[index] + jnp.log2(sum_scr[index])
        prod = attn.astype(jnp.float32) * da_scr[index].astype(jnp.float32)
        prod = prod[:, :head_dim // 2] + prod[:, head_dim // 2:]
        delta_ref[index] = jnp.sum(prod.T, axis=0, keepdims=True)
        out_rows = pl.ds(pl.multiple_of(index * half_len, half_len), half_len)
        for head in range(num_heads):
            a_scr[out_rows, head * head_dim:(head + 1) * head_dim] = attn[head * half_len:(head + 1) * half_len, :]
        keep_group(index).start()
        swap_group(index).start()

    def keep_group(index):
        out_rows = pl.ds(pl.multiple_of(index * half_len, half_len), half_len)
        return pltpu.make_async_copy(a_scr.at[out_rows], a_ref.at[out_rows], out_sems.at[3 + index])

    def swap_group(index):
        out_rows = pl.ds(pl.multiple_of(index * half_len, half_len), half_len)
        far_rows = pl.ds(pl.multiple_of(n_rows + index * half_len, half_len), half_len)
        return remote(a_scr.at[out_rows], a_ref.at[far_rows], swap_send.at[index], swap_recv.at[index], partner)

    lax.fori_loop(0, n_groups, finish, None)
    dy_keep.wait()
    dy_swap.wait()
    for index in range(n_groups):
        keep_group(index).wait()
        swap_group(index).wait()
    for save in saves:
        save.wait()


def attend_grad_kernel(n_dev, q_ref, kv_ref, da_ref, lse_ref, delta_ref, cos_ref, sin_ref, a_ref, dy_ref, z_ref, wo_ref,
                       q_scr, da_scr, kv_scr, qt_scr, dat_scr, dq_scr, dkv_scr, mate_scr, kv_local, kv_slots, a_scr, dy_scr, wo_local, wo_slots,
                       load_sems, kv_send, kv_recv, mate_send, mate_recv, wo_send, wo_recv):
    n_chip, chip, core, peers, partner = ring_place(n_dev)
    me = chip * 2 + core
    rows, head_dim = q_scr.shape[1:]
    n_seq, seq_len, kv_width = dkv_scr.shape
    half_len = seq_len // (2 * n_dev)
    num_heads = rows // half_len
    q_width = num_heads * head_dim
    key_len = PIECES_PER_BLOCK * half_len
    scale = LOG2_E * head_dim ** -0.5
    loads = [
        pltpu.make_async_copy(a_ref, a_scr, load_sems.at[0]),
        pltpu.make_async_copy(dy_ref, dy_scr, load_sems.at[1]),
        pltpu.make_async_copy(q_ref, q_scr, load_sems.at[2]),
        pltpu.make_async_copy(da_ref, da_scr, load_sems.at[3]),
        pltpu.make_async_copy(kv_ref, kv_scr, load_sems.at[4]),
    ]
    for load in loads:
        load.start()
    entry_barrier(peers + (partner,))
    loads[0].wait()
    loads[1].wait()

    def wo_local_term(step):
        n_sub, sub_len = wo_local.shape[1:3]
        way_len = n_sub * sub_len
        for way in range(2):
            first = chunk_at(chip, step, way, n_chip) * (2 * way_len) + way * way_len
            part = dot(a_scr[:, pl.ds(pl.multiple_of(first, way_len), way_len)], dy_scr[...], TN)
            for sub in range(n_sub):
                wo_local[way, sub] = part[sub * sub_len:(sub + 1) * sub_len, :]

    def piece_rows(dev, sub):
        piece = dev if sub == 0 else 2 * n_dev - 1 - dev
        return pl.ds(pl.multiple_of(piece * half_len, half_len), half_len)

    def mate_copy(step, way, sub):
        dev = chunk_at(chip, step, way, n_chip) * 2 + 1 - core
        return remote(dkv_scr.at[way, piece_rows(dev, sub)], mate_scr.at[way, step, sub], mate_send.at[way, step, sub], mate_recv.at[way, step, sub], partner)

    def kv_local_term(step):
        for sub in range(2):
            for way in range(2):
                mate_copy(step, way, sub).wait_recv()
                dev = chunk_at(chip, step, way, n_chip) * 2 + core
                kv_local[way, sub] = dkv_scr[way, piece_rows(dev, sub), :] + mate_scr[way, step, sub]

    wo_ring = RingReduce(n_chip, peers, wo_local_term, wo_local, wo_slots, wo_send, wo_recv, wo_ref)
    kv_ring = RingReduce(n_chip, peers, kv_local_term, kv_local, kv_slots, kv_send, kv_recv)

    front_blocks = lax.div(me, PIECES_PER_BLOCK) + 1
    all_blocks = 2 * n_dev // PIECES_PER_BLOCK + 1
    chunk_blocks = 3

    def block_of(seq, turn):
        group = jnp.where(turn >= front_blocks, 1, 0)
        step = turn - group * front_blocks
        index = 2 * seq + group
        piece = me + group * (2 * n_dev - 1 - 2 * me)
        start = pl.multiple_of(step * key_len, key_len)
        keys = pl.ds(start, key_len)

        @pl.when(step == 0)
        def _():
            dq_scr[...] = jnp.zeros_like(dq_scr)
            qt_scr[...] = q_scr[index].T
            dat_scr[...] = da_scr[index].T

        k_blk, v_blk = kv_scr[seq, keys, :head_dim], kv_scr[seq, keys, head_dim:]
        probs = jnp.exp2(dot(k_blk, qt_scr[...], NN) * scale - lse_ref[index])
        probs = jnp.where(causal_mask(probs.shape, start, piece * half_len, half_len), probs, 0.0)
        d_scores = (probs * (dot(v_blk, dat_scr[...], NN) - delta_ref[index])).astype(jnp.bfloat16)
        dq_scr[...] += dot(k_blk, d_scores, TN)
        dkv_scr[seq, keys, :head_dim] += dot(d_scores, q_scr[index], NN) * head_dim ** -0.5
        dkv_scr[seq, keys, head_dim:] += dot(probs.astype(jnp.bfloat16), da_scr[index], NN)

        @pl.when(step == lax.div(piece, PIECES_PER_BLOCK))
        def _():
            dq = dq_scr[...].T * head_dim ** -0.5
            out_rows = pl.ds(pl.multiple_of(index * half_len, half_len), half_len)
            cos_t, sin_t = cos_ref[out_rows, :], sin_ref[out_rows, :]
            for head in range(num_heads):
                dq_head = dq[head * half_len:(head + 1) * half_len, :]
                z_ref[out_rows, head * head_dim:(head + 1) * head_dim] = rotate_back(dq_head, cos_t, sin_t).astype(jnp.bfloat16)

    n_chunks = all_blocks // chunk_blocks

    def chunk(turn, _):
        seq, part = lax.div(turn, n_chunks), lax.rem(turn, n_chunks)
        lax.fori_loop(part * chunk_blocks, (part + 1) * chunk_blocks, lambda at, _: block_of(seq, at), None)
        for way in range(n_seq):
            @pl.when(turn == (way + 1) * n_chunks - 1)
            def _():
                def send_mate(step, _):
                    for sub in range(2):
                        mate_copy(step, way, sub).start()

                lax.fori_loop(0, n_chip, send_mate, None)

        step, sub = lax.div(turn, 2) + 1, lax.rem(turn, 2)

        @pl.when(sub == 0)
        def _():
            wo_local_term(step)

        wo_ring.serve(step, sub)

    wo_ring.first()
    dkv_scr[...] = jnp.zeros_like(dkv_scr)
    for load in loads[2:]:
        load.wait()
    lax.fori_loop(0, n_seq * n_chunks, chunk, None)
    kv_ring.first()
    wo_ring.middle(4)
    kv_ring.middle(1)

    def both(step, _):
        wo_ring.middle(step + 3)
        kv_ring.middle(step)

    lax.fori_loop(2, n_chip - 4, both, None)

    def keep_wo(way, sub):
        wo_ref[way, sub] = wo_slots[way, n_chip - 2, sub]

    wo_ring.last(keep_wo)
    lax.fori_loop(n_chip - 4, n_chip - 1, lambda step, _: kv_ring.middle(step), None)

    def keep_kv(way, sub):
        out_rows = slice((2 * way + sub) * half_len, (2 * way + sub + 1) * half_len)
        total = kv_slots[way, n_chip - 2, sub]
        z_ref[out_rows, q_width:q_width + head_dim] = rotate_back(total[:, :head_dim], cos_ref[out_rows, :], sin_ref[out_rows, :]).astype(jnp.bfloat16)
        z_ref[out_rows, q_width + head_dim:] = total[:, head_dim:].astype(jnp.bfloat16)

    kv_ring.last(keep_kv)

    def mates_sent(step, _):
        for way in range(2):
            for sub in range(2):
                mate_copy(step, way, sub).wait_send()

    lax.fori_loop(0, n_chip, mates_sent, None)


def finish_kernel(n_dev, h_ref, z_ref, wo_part_ref, a_ref, x_ref, dy_ref, gain_ref, wq_ref, wo_ref, wk_ref, wv_ref,
                  gz_ref, gwo_ref, y_ref, dx_ref, ggain_ref,
                  h_scr, z_scr, zf_scr, a_scr, x_scr, dy_scr, dh_scr, wq_buf, wo_buf, gain_slots, local_scr, slots,
                  load_sems, w_sems, swap_send, swap_recv, send_sems, recv_sems, g1_send, g1_recv, m1_send, m1_recv,
                  g2_send, g2_recv, m2_send, m2_recv, keep_sems, gain_send, gain_recv):
    n_chip, chip, core, peers, partner = ring_place(n_dev)
    me = chip * 2 + core
    n_rows, model_dim = h_ref.shape
    core_width = z_scr.shape[1]
    q_width = a_ref.shape[1]
    head_dim = wk_ref.shape[1]
    n_sub, sub_len = local_scr.shape[1:3]
    way_len = n_sub * sub_len
    wo_sub_len, wo_width = wo_part_ref.shape[2:]
    wo_way_len = n_sub * wo_sub_len
    blk = model_dim // n_chip
    mine, other = pl.ds(0, n_rows), pl.ds(n_rows, n_rows)

    def cols(which, size):
        return pl.ds(pl.multiple_of(which * size, size), size)

    def wq_load(index, slot):
        return pltpu.make_async_copy(wq_ref.at[cols(index, blk), :], wq_buf.at[slot], w_sems.at[0, slot])

    def wo_load(index, slot):
        return pltpu.make_async_copy(wo_ref.at[:, cols(index, blk)], wo_buf.at[slot], w_sems.at[1, slot])

    loads = [
        pltpu.make_async_copy(h_ref, h_scr.at[mine], load_sems.at[0]),
        pltpu.make_async_copy(z_ref.at[:, cols(core, core_width)], z_scr.at[mine], load_sems.at[1]),
        pltpu.make_async_copy(z_ref, zf_scr, load_sems.at[2]),
        pltpu.make_async_copy(a_ref.at[mine], a_scr, load_sems.at[3]),
        pltpu.make_async_copy(x_ref, x_scr, load_sems.at[4]),
        pltpu.make_async_copy(dy_ref, dy_scr, load_sems.at[5]),
    ]
    for load in loads:
        load.start()
    wq_load(0, 0).start()
    wo_load(0, 0).start()
    barrier = pltpu.get_barrier_semaphore()
    for offset in range(1, n_dev):
        pl.semaphore_signal(barrier, inc=1, device_id={'cp': lax.rem(me + offset, n_dev)}, device_id_type=pl.DeviceIdType.MESH)
    pl.semaphore_wait(barrier, n_dev - 1)

    def wo_place(step, way, sub):
        first = owner_at(chip, step, way, n_chip) * (2 * wo_way_len) + way * wo_way_len + sub * wo_sub_len
        return gwo_ref.at[pl.ds(pl.multiple_of(first, wo_sub_len), wo_sub_len), cols(core, wo_width)]

    def z_place(step, way, sub):
        first = owner_at(chip, step, way, n_chip) * (2 * way_len) + way * way_len + sub * sub_len
        return gz_ref.at[pl.ds(pl.multiple_of(first, sub_len), sub_len), cols(core, core_width)]

    swaps = [
        remote(h_ref, h_scr.at[other], swap_send.at[0], swap_recv.at[0], partner),
        remote(z_ref.at[:, cols(1 - core, core_width)], z_scr.at[other], swap_send.at[1], swap_recv.at[1], partner),
    ]
    for swap in swaps:
        swap.start()
    wo_gather = RingGather(n_chip, peers, partner, lambda way, sub: wo_part_ref.at[way, sub], wo_place, n_sub, g1_send, g1_recv, m1_send, m1_recv)
    z_gather = RingGather(n_chip, peers, partner, lambda way, sub: slots.at[way, n_chip - 2, sub], z_place, n_sub, g2_send, g2_recv, m2_send, m2_recv)
    keeps = ([pltpu.make_async_copy(wo_part_ref.at[way, sub], wo_place(0, way, sub), keep_sems.at[0, way, sub]) for sub, way in wo_gather.each],
             [pltpu.make_async_copy(slots.at[way, n_chip - 2, sub], z_place(0, way, sub), keep_sems.at[1, way, sub]) for sub, way in wo_gather.each])
    wo_gather.first()
    for keep in keeps[0]:
        keep.start()

    def local_term(step):
        for way in range(2):
            first = chunk_at(chip, step, way, n_chip) * (2 * way_len) + way * way_len
            part = dot(h_scr[:, pl.ds(pl.multiple_of(first, way_len), way_len)], z_scr[...], TN)
            for sub in range(n_sub):
                local_scr[way, sub] = part[sub * sub_len:(sub + 1) * sub_len, :]

    z_ring = RingReduce(n_chip, peers, local_term, local_scr, slots, send_sems, recv_sems)

    def d_hidden(index, slot):
        wq_load(index, slot).wait()

        @pl.when(index + 1 < n_chip)
        def _():
            wq_load(index + 1, 1 - slot).start()

        rows = cols(index, blk)
        dh_scr[:, rows] = (dot(zf_scr[:, :q_width], wq_buf[slot], NT) + dot(zf_scr[:, q_width:q_width + head_dim], wk_ref[rows, :], NT)
                           + dot(zf_scr[:, q_width + head_dim:], wv_ref[rows, :], NT))

    def out_block(index, slot):
        wo_load(index, slot).wait()

        @pl.when(index + 1 < n_chip)
        def _():
            wo_load(index + 1, 1 - slot).start()

        where = cols(index, blk)
        o_blk = dot(a_scr[...], wo_buf[slot], NN).astype(jnp.bfloat16)
        y_ref[:, where] = (x_scr[:, where].astype(jnp.float32) + o_blk.astype(jnp.float32)).astype(jnp.bfloat16)

    def norm_grad(index, _):
        rows = pl.ds(pl.multiple_of(index * 32, 32), 32)
        x_float = x_scr[rows, :].astype(jnp.float32)
        centered = x_float - jnp.mean(x_float, axis=-1, keepdims=True)
        inv_std = lax.rsqrt(jnp.mean(centered * centered, axis=-1, keepdims=True) + NORM_EPS)
        x_hat = centered * inv_std
        d_h = dh_scr[rows, :]
        gain_slots[me] += jnp.sum(d_h * x_hat, axis=0, keepdims=True)
        d_hat = d_h * gain_ref[...]
        mean_d = jnp.mean(d_hat, axis=-1, keepdims=True)
        mean_dx = jnp.mean(d_hat * x_hat, axis=-1, keepdims=True)
        dx_ref[rows, :] = (dy_scr[rows, :].astype(jnp.float32) + inv_std * (d_hat - mean_d - x_hat * mean_dx)).astype(jnp.bfloat16)

    def gain_copy(offset):
        return remote(gain_slots.at[me], gain_slots.at[me], gain_send.at[offset], gain_recv.at[offset], lax.rem(me + offset, n_dev))

    loads[0].wait()
    loads[1].wait()
    for swap in swaps:
        swap.wait_recv()
    z_ring.first()
    for load in loads[2:]:
        load.wait()
    wo_gather.middle(1)
    z_ring.middle(1)
    d_hidden(0, 0)

    def phase_one(step, _):
        wo_gather.middle(step)
        z_ring.middle(step)
        d_hidden(step - 1, lax.rem(step - 1, 2))

    lax.fori_loop(2, n_chip - 1, phase_one, None)
    wo_gather.last()

    def pass_on(way, sub):
        z_gather.start_first(way, sub)
        keeps[1][2 * sub + way].start()

    z_ring.last(pass_on)
    d_hidden(n_chip - 2, (n_chip - 2) % 2)
    d_hidden(n_chip - 1, (n_chip - 1) % 2)
    gain_slots[me] = jnp.zeros(gain_slots.shape[1:], jnp.float32)
    lax.fori_loop(0, n_rows // 32, norm_grad, None)
    for offset in range(1, n_dev):
        gain_copy(offset).start()
    z_gather.middle(1)
    out_block(0, 0)
    out_block(1, 1)

    def phase_two(step, _):
        z_gather.middle(step)
        out_block(step, lax.rem(step, 2))

    lax.fori_loop(2, n_chip - 1, phase_two, None)
    out_block(n_chip - 1, (n_chip - 1) % 2)
    z_gather.last()
    for offset in range(1, n_dev):
        gain_copy(offset).wait_recv()
    total = gain_slots[0]
    for dev in range(1, n_dev):
        total = total + gain_slots[dev]
    ggain_ref[...] = total
    wo_gather.drain()
    z_gather.drain()
    for keep in keeps[0] + keeps[1]:
        keep.wait()
    for swap in swaps:
        swap.wait_send()
    for offset in range(1, n_dev):
        gain_copy(offset).wait_send()


def deliver_kernel(gz_ref, gwo_ref, y_ref, dx_ref, wq_out, wk_out, wv_out, wo_out, y_out, dx_out, gz_buf, gwo_buf, y_buf, dx_buf, in_sems, out_sems):
    n_blk, z_len, _ = gz_buf.shape
    wo_len = gwo_buf.shape[1]
    q_width, head_dim = wq_out.shape[1], wk_out.shape[1]
    jobs = []
    for i in range(n_blk):
        rows = pl.ds(i * z_len, z_len)
        parts = [(gz_buf.at[i, :, pl.ds(first, out.shape[1])], out.at[rows]) for out, first in ((wq_out, 0), (wk_out, q_width), (wv_out, q_width + head_dim))]
        jobs.append((gz_ref.at[rows], gz_buf.at[i], parts))
        rows = pl.ds(i * wo_len, wo_len)
        jobs.append((gwo_ref.at[rows], gwo_buf.at[i], [(gwo_buf.at[i], wo_out.at[rows])]))
    for src, buf, out in ((y_ref, y_buf, y_out), (dx_ref, dx_buf, dx_out)):
        jobs.append((src, buf, [(buf, out)]))
    reads = [pltpu.make_async_copy(src, buf, in_sems.at[i]) for i, (src, buf, _) in enumerate(jobs)]
    for read in reads:
        read.start()
    writes = []
    for read, (_, _, parts) in zip(reads, jobs):
        read.wait()
        for src, dst in parts:
            writes.append(pltpu.make_async_copy(src, dst, out_sems.at[len(writes)]))
            writes[-1].start()
    for write in writes:
        write.wait()


def solution(mesh):
    n_dev = mesh.shape['cp']
    n_chip, n_sub = n_dev // 2, 2

    def local_fn(tokens, positions, norm_gain, w_query, w_key, w_value, w_out, d_out):
        n_seq, blk_len, model_dim = tokens.shape
        head_dim = w_key.shape[1]
        num_heads = w_query.shape[1] // head_dim
        q_width, kv_width = num_heads * head_dim, 2 * head_dim
        half_len, half = blk_len // 2, head_dim // 2
        n_rows, n_groups = n_seq * blk_len, 2 * n_seq
        rows = num_heads * half_len
        seq_len = n_dev * blk_len
        bf16, f32 = jnp.bfloat16, jnp.float32
        dma = pltpu.SemaphoreType.DMA
        vmem = pl.BlockSpec(memory_space=pltpu.VMEM)
        hbm = pl.BlockSpec(memory_space=pl.ANY)
        params = pltpu.CompilerParams(vmem_limit_bytes=VMEM_LIMIT)

        def comm(ident):
            return pltpu.CompilerParams(vmem_limit_bytes=VMEM_LIMIT, collective_id=ident, has_side_effects=True)

        def shape(*dims, dtype=bf16):
            return jax.ShapeDtypeStruct(dims, dtype)

        def gather_sems():
            return [dma((2, n_sub)), dma((2, n_chip - 1, n_sub)), dma((2, n_sub)), dma((2, n_chip, n_sub))]

        x_flat = tokens.reshape(n_rows, model_dim)
        dy_flat = d_out.reshape(n_rows, model_dim)
        gain_row = norm_gain.reshape(1, model_dim)
        cos_t, sin_t = rope_tables(positions.reshape(n_rows), head_dim)
        h_flat, kv_flat = pl.pallas_call(
            norm_kv_kernel,
            out_shape=(shape(n_rows, model_dim), shape(n_rows, kv_width)),
            compiler_params=params, name='norm_kv',
        )(x_flat, gain_row, w_key, w_value, cos_t, sin_t)

        groups = (n_groups, rows, head_dim)
        kv_all, q_rows, da_rows, attn_chip, dy_chip, lse, delta = pl.pallas_call(
            functools.partial(forward_kernel, n_dev),
            in_specs=[vmem, vmem, vmem, hbm, hbm, hbm, hbm],
            out_specs=[hbm, hbm, hbm, hbm, hbm, vmem, vmem],
            out_shape=(shape(n_seq, seq_len, kv_width), shape(*groups), shape(*groups), shape(2 * n_rows, q_width), shape(2 * n_rows, model_dim // 2),
                       shape(n_groups, 1, rows, dtype=f32), shape(n_groups, 1, rows, dtype=f32)),
            scratch_shapes=[pltpu.VMEM((n_rows, model_dim), bf16), pltpu.VMEM((n_rows, model_dim), bf16), pltpu.VMEM((n_seq, seq_len, kv_width), bf16),
                            pltpu.VMEM(groups, bf16), pltpu.VMEM(groups, bf16), pltpu.VMEM((n_groups, head_dim, rows), bf16), pltpu.VMEM((n_rows, q_width), bf16),
                            pltpu.VMEM((n_groups, head_dim, rows), f32), pltpu.VMEM((n_groups, 1, rows), f32), pltpu.VMEM((n_groups, 1, rows), f32),
                            pltpu.VMEM((2, model_dim, head_dim), bf16), pltpu.VMEM((2, head_dim, model_dim), bf16),
                            dma((3,)), dma((3 + n_groups,)), dma((2, 2)), dma((n_groups + 1,)), dma((n_groups + 1,))] + gather_sems(),
            compiler_params=comm(0), name='forward',
        )(kv_flat, cos_t, sin_t, h_flat, dy_flat, w_query, w_out)

        z_width = q_width + kv_width
        wo_cols, wo_sub = model_dim // 2, q_width // (2 * n_chip * n_sub)
        z_flat, wo_part = pl.pallas_call(
            functools.partial(attend_grad_kernel, n_dev),
            in_specs=[hbm, hbm, hbm, vmem, vmem, vmem, vmem, hbm, hbm],
            out_specs=[vmem, vmem],
            out_shape=(shape(n_rows, z_width), shape(2, n_sub, wo_sub, wo_cols, dtype=f32)),
            scratch_shapes=[pltpu.VMEM((n_groups, rows, head_dim), bf16), pltpu.VMEM((n_groups, rows, head_dim), bf16),
                            pltpu.VMEM((n_seq, seq_len, kv_width), bf16), pltpu.VMEM((head_dim, rows), bf16), pltpu.VMEM((head_dim, rows), bf16), pltpu.VMEM((head_dim, rows), f32),
                            pltpu.VMEM((n_seq, seq_len, kv_width), f32), pltpu.VMEM((2, n_chip, 2, half_len, kv_width), f32),
                            pltpu.VMEM((2, 2, half_len, kv_width), f32), pltpu.VMEM((2, n_chip - 1, 2, half_len, kv_width), f32),
                            pltpu.VMEM((2 * n_rows, q_width), bf16), pltpu.VMEM((2 * n_rows, wo_cols), bf16),
                            pltpu.VMEM((2, n_sub, wo_sub, wo_cols), f32), pltpu.VMEM((2, n_chip - 1, n_sub, wo_sub, wo_cols), f32),
                            dma((5,)), dma((2, 2)), dma((2, n_chip - 1, 2)), dma((2, n_chip, 2)), dma((2, n_chip, 2)),
                            dma((2, n_sub)), dma((2, n_chip - 1, n_sub))],
            compiler_params=comm(1), name='attend_grad',
        )(q_rows, kv_all, da_rows, lse, delta, cos_t, sin_t, attn_chip, dy_chip)

        core_width, sub_len = z_width // 2, model_dim // (2 * n_chip * n_sub)
        blk = model_dim // n_chip
        grad_z, grad_wo, out_y, grad_x, grad_gain = pl.pallas_call(
            functools.partial(finish_kernel, n_dev),
            in_specs=[hbm] * 6 + [vmem, hbm, hbm, vmem, vmem],
            out_specs=[pl.BlockSpec(memory_space=pltpu.HBM), hbm, vmem, vmem, vmem],
            out_shape=(shape(model_dim, z_width, dtype=f32), shape(q_width, model_dim, dtype=f32), shape(n_rows, model_dim), shape(n_rows, model_dim),
                       shape(1, model_dim, dtype=f32)),
            scratch_shapes=[pltpu.VMEM((2 * n_rows, model_dim), bf16), pltpu.VMEM((2 * n_rows, core_width), bf16), pltpu.VMEM((n_rows, z_width), bf16),
                            pltpu.VMEM((n_rows, q_width), bf16), pltpu.VMEM((n_rows, model_dim), bf16), pltpu.VMEM((n_rows, model_dim), bf16),
                            pltpu.VMEM((n_rows, model_dim), f32), pltpu.VMEM((2, blk, q_width), bf16), pltpu.VMEM((2, q_width, blk), bf16),
                            pltpu.VMEM((n_dev, 1, model_dim), f32), pltpu.VMEM((2, n_sub, sub_len, core_width), f32),
                            pltpu.VMEM((2, n_chip - 1, n_sub, sub_len, core_width), f32),
                            dma((6,)), dma((2, 2)), dma((2,)), dma((2,)), dma((2, n_sub)), dma((2, n_chip - 1, n_sub))]
            + gather_sems() + gather_sems() + [dma((2, 2, n_sub)), dma((n_dev,)), dma((n_dev,))],
            compiler_params=comm(2), name='finish',
        )(h_flat, z_flat, wo_part, attn_chip, x_flat, dy_flat, gain_row, w_query, w_out, w_key, w_value)
        n_blk = n_dev
        grad_wq, grad_wk, grad_wv, grad_wo, out_y, grad_x = pl.pallas_call(
            deliver_kernel,
            in_specs=[hbm] * 4,
            out_specs=[hbm] * 6,
            out_shape=(shape(model_dim, q_width, dtype=f32), shape(model_dim, head_dim, dtype=f32), shape(model_dim, head_dim, dtype=f32),
                       shape(q_width, model_dim, dtype=f32), shape(n_rows, model_dim), shape(n_rows, model_dim)),
            scratch_shapes=[pltpu.VMEM((n_blk, model_dim // n_blk, z_width), f32), pltpu.VMEM((n_blk, q_width // n_blk, model_dim), f32),
                            pltpu.VMEM((n_rows, model_dim), bf16), pltpu.VMEM((n_rows, model_dim), bf16),
                            dma((2 * n_blk + 2,)), dma((4 * n_blk + 2,))],
            compiler_params=params, name='deliver',
        )(grad_z, grad_wo, out_y, grad_x)
        return out_y.reshape(tokens.shape), grad_x.reshape(tokens.shape), grad_wq, grad_wk, grad_wv, grad_wo, grad_gain.reshape(model_dim)

    seq_spec = P('dp', 'cp', None)
    rep_spec = P(None, None)
    part_spec = P('dp', None)
    return jax.shard_map(local_fn, mesh=mesh,
                         in_specs=(seq_spec, P('dp', 'cp'), P(None), rep_spec, rep_spec, rep_spec, rep_spec, seq_spec),
                         out_specs=(seq_spec, seq_spec, part_spec, part_spec, part_spec, part_spec, P('dp')),
                         check_vma=False)
```

```python
import functools

import jax
import jax.numpy as jnp
from jax import lax
from jax.experimental import pallas as pl
from jax.experimental.pallas import tpu as pltpu
from jax.sharding import PartitionSpec as P

NORM_EPS = 1e-6
ROPE_BASE = 10000.0
NEG_BIG = -1e30
LOG2_E = 1.4426950408889634
PIECES_PER_BLOCK = 4
VMEM_LIMIT = 60 * 1024 * 1024

NT = (((1,), (1,)), ((), ()))
TN = (((0,), (0,)), ((), ()))
NN = (((1,), (0,)), ((), ()))


def dot(lhs, rhs, dims):
    return lax.dot_general(lhs, rhs, dims, preferred_element_type=jnp.float32)


def rope_tables(positions, head_dim):
    half_dim = head_dim // 2
    inv_freq = ROPE_BASE ** (-(jnp.arange(half_dim, dtype=jnp.float32) * (2.0 / head_dim)))
    angles = positions.astype(jnp.float32)[..., None] * inv_freq
    return jnp.cos(angles), jnp.sin(angles)


def rotate(values, cos_t, sin_t):
    half_dim = values.shape[-1] // 2
    front_half, back_half = values[..., :half_dim], values[..., half_dim:]
    return jnp.concatenate([front_half * cos_t - back_half * sin_t, back_half * cos_t + front_half * sin_t], axis=-1)


def rotate_back(grad_vals, cos_t, sin_t):
    half_dim = grad_vals.shape[-1] // 2
    front_half, back_half = grad_vals[..., :half_dim], grad_vals[..., half_dim:]
    return jnp.concatenate([front_half * cos_t + back_half * sin_t, back_half * cos_t - front_half * sin_t], axis=-1)


def norm_kv_kernel(x_ref, gain_ref, wk_ref, wv_ref, cos_ref, sin_ref, h_ref, kv_ref):
    head_dim = wk_ref.shape[1]
    x_float = x_ref[...].astype(jnp.float32)
    centered = x_float - jnp.mean(x_float, axis=-1, keepdims=True)
    inv_std = lax.rsqrt(jnp.mean(centered * centered, axis=-1, keepdims=True) + NORM_EPS)
    h_norm = (centered * inv_std * gain_ref[...]).astype(jnp.bfloat16)
    h_ref[...] = h_norm
    k_lin = dot(h_norm, wk_ref[...], NN)
    kv_ref[:, :head_dim] = rotate(k_lin, cos_ref[...], sin_ref[...]).astype(jnp.bfloat16)
    kv_ref[:, head_dim:] = dot(h_norm, wv_ref[...], NN).astype(jnp.bfloat16)


def entry_barrier(peers):
    barrier = pltpu.get_barrier_semaphore()
    for peer in peers:
        pl.semaphore_signal(barrier, inc=1, device_id={'cp': peer}, device_id_type=pl.DeviceIdType.MESH)
    pl.semaphore_wait(barrier, len(peers))


def remote(src, dst, send_sem, recv_sem, peer):
    return pltpu.make_async_remote_copy(src_ref=src, dst_ref=dst, send_sem=send_sem, recv_sem=recv_sem,
                                        device_id={'cp': peer}, device_id_type=pl.DeviceIdType.MESH)


def ring_place(n_dev):
    me = lax.axis_index('cp')
    n_chip = n_dev // 2
    chip, core = lax.div(me, 2), lax.rem(me, 2)
    after = lax.rem(chip + 1, n_chip) * 2 + core
    before = lax.rem(chip + n_chip - 1, n_chip) * 2 + core
    partner = chip * 2 + 1 - core
    return n_chip, chip, core, (after, before), partner


def chunk_at(chip, step, way, n_chip):
    if way == 0:
        return lax.rem(chip + 2 * n_chip - 1 - step, n_chip)
    return lax.rem(chip + 1 + step, n_chip)


class RingReduce:
    def __init__(self, n_chip, peers, make_local, local_scr, slots, send_sems, recv_sems, first_buf=None):
        self.n_chip, self.peers, self.make_local, self.first_buf = n_chip, peers, make_local, first_buf
        self.local_scr, self.slots, self.send_sems, self.recv_sems = local_scr, slots, send_sems, recv_sems
        self.each = [(sub, way) for sub in range(slots.shape[2]) for way in range(2)]

    def hop(self, step, way, sub, first=False):
        buf = self.local_scr if self.first_buf is None else self.first_buf
        src = buf.at[way, sub] if first else self.slots.at[way, step - 1, sub]
        return remote(src, self.slots.at[way, step, sub], self.send_sems.at[way, sub], self.recv_sems.at[way, step, sub], self.peers[way])

    def arrival(self, step, way, sub):
        slot = self.slots.at[way, step, sub]
        return remote(slot, slot, self.send_sems.at[way, sub], self.recv_sems.at[way, step, sub], self.peers[way])

    def serve(self, step, sub):
        for way in range(2):
            self.arrival(step - 1, way, sub).wait_recv()
            self.slots[way, step - 1, sub] = self.slots[way, step - 1, sub] + self.local_scr[way, sub]
            self.arrival(step - 1, way, sub).wait_send()
            self.hop(step, way, sub).start()

    def first(self):
        self.make_local(0)
        if self.first_buf is not None:
            self.first_buf[...] = self.local_scr[...]
        for sub, way in self.each:
            self.hop(0, way, sub, True).start()

    def middle(self, step, on_sum=None):
        after_first = isinstance(step, int) and step == 1
        if after_first:
            for sub, way in self.each:
                self.hop(0, way, sub, True).wait_send()
        self.make_local(step)
        for sub, way in self.each:
            self.hop(step - 1, way, sub, after_first).wait_recv()
            self.slots[way, step - 1, sub] = self.slots[way, step - 1, sub] + self.local_scr[way, sub]
            if not after_first:
                self.hop(step - 1, way, sub).wait_send()
            if on_sum is None:
                self.hop(step, way, sub).start()
            else:
                on_sum(way, sub)

    def last(self, on_sum):
        self.middle(self.n_chip - 1, on_sum)


class RingGather:
    def __init__(self, n_chip, peers, partner, own, place, n_sub, send_sems, recv_sems, mate_send, mate_recv):
        self.n_chip, self.peers, self.partner, self.own, self.place = n_chip, peers, partner, own, place
        self.send_sems, self.recv_sems, self.mate_send, self.mate_recv = send_sems, recv_sems, mate_send, mate_recv
        self.each = [(sub, way) for sub in range(n_sub) for way in range(2)]

    def onward(self, step, way, sub, first=False):
        src = self.own(way, sub) if first else self.place(step, way, sub)
        return remote(src, self.place(step, way, sub), self.send_sems.at[way, sub], self.recv_sems.at[way, step, sub], self.peers[way])

    def across(self, step, way, sub, first=False):
        src = self.own(way, sub) if first else self.place(step, way, sub)
        return remote(src, self.place(step, way, sub), self.mate_send.at[way, sub], self.mate_recv.at[way, step, sub], self.partner)

    def start_first(self, way, sub):
        self.onward(0, way, sub, True).start()
        self.across(0, way, sub, True).start()

    def first(self):
        for sub, way in self.each:
            self.start_first(way, sub)

    def middle(self, step, last=False):
        after_first = isinstance(step, int) and step == 1
        for sub, way in self.each:
            self.onward(step - 1, way, sub, after_first).wait_send()
            self.onward(step - 1, way, sub, after_first).wait_recv()
            if not last:
                self.onward(step, way, sub).start()
            self.across(step - 1, way, sub, after_first).wait_send()
            self.across(step, way, sub).start()

    def last(self):
        self.middle(self.n_chip - 1, True)

    def serve(self, step, sub):
        for way in range(2):
            self.onward(step - 1, way, sub).wait_recv()
            self.onward(step - 1, way, sub).wait_send()

            @pl.when(step < self.n_chip - 1)
            def _():
                self.onward(step, way, sub).start()

            self.across(step - 1, way, sub).wait_send()
            self.across(step, way, sub).start()

    def drain(self):
        for sub, way in self.each:
            self.across(self.n_chip - 1, way, sub).wait_send()

        def body(step, _):
            for sub, way in self.each:
                self.across(step, way, sub).wait_recv()

        lax.fori_loop(0, self.n_chip, body, None)


def owner_at(chip, step, way, n_chip):
    if way == 0:
        return lax.rem(chip + n_chip - step, n_chip)
    return lax.rem(chip + step, n_chip)


def causal_mask(shape, key_start, query_start, half_len):
    key_idx = key_start + lax.broadcasted_iota(jnp.int32, shape, 0)
    query_idx = query_start + lax.rem(lax.broadcasted_iota(jnp.int32, shape, 1), half_len)
    return key_idx <= query_idx


def forward_kernel(n_dev, kv_ref, cos_ref, sin_ref, h_ref, dy_ref, wq_ref, wo_ref, all_ref, q_ref, da_ref, a_ref, dyc_ref, lse_ref, delta_ref,
                   h_scr, dy_scr, kv_scr, q_scr, da_scr, qt_scr, a_scr, acc_scr, max_scr, sum_scr, wq_buf, wo_buf,
                   load_sems, out_sems, w_sems, swap_send, swap_recv, send_sems, recv_sems, mate_send, mate_recv):
    n_chip, chip, core, peers, partner = ring_place(n_dev)
    me = chip * 2 + core
    n_rows, dy_cols = h_scr.shape[0], dyc_ref.shape[1]
    n_seq, seq_len, kv_width = kv_scr.shape
    half_len = seq_len // (2 * n_dev)
    n_groups, rows, head_dim = q_scr.shape
    num_heads = rows // half_len
    scale = LOG2_E * head_dim ** -0.5

    def weights(head, slot):
        cols = pl.ds(pl.multiple_of(head * head_dim, head_dim), head_dim)
        return (pltpu.make_async_copy(wq_ref.at[:, cols], wq_buf.at[slot], w_sems.at[0, slot]),
                pltpu.make_async_copy(wo_ref.at[cols, :], wo_buf.at[slot], w_sems.at[1, slot]))

    loads = [pltpu.make_async_copy(h_ref, h_scr, load_sems.at[0]), pltpu.make_async_copy(dy_ref, dy_scr, load_sems.at[1])]
    for load in loads:
        load.start()
    for copy in weights(0, 0):
        copy.start()
    entry_barrier(peers + (partner,))

    def piece_rows(dev, way):
        piece = dev if way == 0 else 2 * n_dev - 1 - dev
        return pl.ds(pl.multiple_of(piece * half_len, half_len), half_len)

    def place(step, way, seq):
        return kv_scr.at[seq, piece_rows(owner_at(chip, step, way, n_chip) * 2 + core, way)]

    def own(way, seq):
        return kv_ref.at[pl.ds((2 * seq + way) * half_len, half_len)]

    ring = RingGather(n_chip, peers, partner, own, place, n_seq, send_sems, recv_sems, mate_send, mate_recv)
    ring.first()
    for seq in range(n_seq):
        for way in range(2):
            kv_scr[seq, piece_rows(me, way), :] = kv_ref[(2 * seq + way) * half_len:(2 * seq + way + 1) * half_len, :]
    max_scr[...] = jnp.full_like(max_scr, NEG_BIG)
    sum_scr[...] = jnp.zeros_like(sum_scr)
    acc_scr[...] = jnp.zeros_like(acc_scr)
    for load in loads:
        load.wait()

    def half_cols(which):
        return pl.ds(pl.multiple_of(which * dy_cols, dy_cols), dy_cols)

    dy_keep = pltpu.make_async_copy(dy_scr.at[:, half_cols(core)], dyc_ref.at[pl.ds(0, n_rows)], load_sems.at[2])
    dy_swap = remote(dy_scr.at[:, half_cols(1 - core)], dyc_ref.at[pl.ds(n_rows, n_rows)], swap_send.at[n_groups], swap_recv.at[n_groups], partner)
    dy_keep.start()
    dy_swap.start()

    def project(head, slot):
        for copy in weights(head, slot):
            copy.wait()

        @pl.when(head + 1 < num_heads)
        def _():
            for copy in weights(head + 1, 1 - slot):
                copy.start()

        head_rows = pl.ds(pl.multiple_of(head * half_len, half_len), half_len)
        q_new = rotate(dot(h_scr[...], wq_buf[slot], NN), cos_ref[...], sin_ref[...]).astype(jnp.bfloat16)
        da_new = dot(dy_scr[...], wo_buf[slot], NT).astype(jnp.bfloat16)
        for group in range(n_groups):
            q_scr[group, head_rows, :] = q_new[group * half_len:(group + 1) * half_len, :]
            da_scr[group, head_rows, :] = da_new[group * half_len:(group + 1) * half_len, :]

    def block(seq, group, start, key_len, masked):
        index = 2 * seq + group
        keys = pl.ds(pl.multiple_of(start, half_len), key_len)
        scores = dot(kv_scr[seq, keys, :head_dim], qt_scr[index], NN) * scale
        if masked:
            piece = me if group == 0 else 2 * n_dev - 1 - me
            scores = jnp.where(causal_mask(scores.shape, start, piece * half_len, half_len), scores, NEG_BIG)
        old_max = max_scr[index]
        new_max = jnp.maximum(old_max, jnp.max(scores, axis=0, keepdims=True))
        rescale = jnp.exp2(old_max - new_max)
        probs = jnp.exp2(scores - new_max)
        max_scr[index] = new_max
        sum_scr[index] = sum_scr[index] * rescale + jnp.sum(probs, axis=0, keepdims=True)
        acc_scr[index] = acc_scr[index] * rescale + dot(kv_scr[seq, keys, head_dim:], probs.astype(jnp.bfloat16), TN)

    def attend_pair(pair, seq):
        chip_len = 2 * half_len
        for step in range(2):
            for way in range(2):
                ring.across(2 * pair + step, way, seq).wait_recv()
        front = owner_at(chip, 2 * pair, 0, n_chip)
        before = owner_at(chip, 2 * pair + 1, 0, n_chip)
        back = chip + 2 * pair

        @pl.when(front > 0)
        def _():
            block(seq, 1, before * chip_len, 2 * chip_len, False)

        @pl.when(front == 0)
        def _():
            lax.fori_loop(0, 2, lambda i, _: block(seq, 1, (front + i * (before - front)) * chip_len, chip_len, False), None)

        @pl.when(2 * pair < chip)
        def _():
            block(seq, 0, before * chip_len, 2 * chip_len, True)

        @pl.when(2 * pair == chip)
        def _():
            block(seq, 0, front * chip_len, chip_len, True)

        @pl.when(back + 1 < n_chip)
        def _():
            block(seq, 1, (n_dev - 2 - back) * chip_len, 2 * chip_len, True)

        @pl.when(back + 1 == n_chip)
        def _():
            block(seq, 1, (n_dev - 1 - back) * chip_len, chip_len, True)

    saves = [pltpu.make_async_copy(q_scr, q_ref, out_sems.at[0]), pltpu.make_async_copy(da_scr, da_ref, out_sems.at[1])]

    def attend(turn):
        attend_pair(lax.div(turn, n_seq), lax.rem(turn, n_seq))

    def work(turn, _):
        @pl.when(turn < num_heads)
        def _():
            project(turn, lax.rem(turn, 2))

        @pl.when(turn == n_chip - 1)
        def _():
            for group in range(n_groups):
                qt_scr[group] = q_scr[group].T
            for save in saves:
                save.start()

        @pl.when(turn >= n_chip)
        def _():
            attend(turn - n_chip)

        @pl.when(turn < n_seq * (n_chip - 1))
        def _():
            ring.serve(lax.div(turn, n_seq) + 1, lax.rem(turn, n_seq))

    lax.fori_loop(0, n_chip + n_chip // 2 * n_seq, work, None)
    for sub, way in ring.each:
        ring.across(n_chip - 1, way, sub).wait_send()
    saves.append(pltpu.make_async_copy(kv_scr, all_ref, out_sems.at[2]))
    saves[2].start()

    def finish(index, _):
        attn = (acc_scr[index] / sum_scr[index]).T.astype(jnp.bfloat16)
        lse_ref[index] = max_scr[index] + jnp.log2(sum_scr[index])
        prod = attn.astype(jnp.float32) * da_scr[index].astype(jnp.float32)
        prod = prod[:, :head_dim // 2] + prod[:, head_dim // 2:]
        delta_ref[index] = jnp.sum(prod.T, axis=0, keepdims=True)
        out_rows = pl.ds(pl.multiple_of(index * half_len, half_len), half_len)
        for head in range(num_heads):
            a_scr[out_rows, head * head_dim:(head + 1) * head_dim] = attn[head * half_len:(head + 1) * half_len, :]
        keep_group(index).start()
        swap_group(index).start()

    def keep_group(index):
        out_rows = pl.ds(pl.multiple_of(index * half_len, half_len), half_len)
        return pltpu.make_async_copy(a_scr.at[out_rows], a_ref.at[out_rows], out_sems.at[3 + index])

    def swap_group(index):
        out_rows = pl.ds(pl.multiple_of(index * half_len, half_len), half_len)
        far_rows = pl.ds(pl.multiple_of(n_rows + index * half_len, half_len), half_len)
        return remote(a_scr.at[out_rows], a_ref.at[far_rows], swap_send.at[index], swap_recv.at[index], partner)

    lax.fori_loop(0, n_groups, finish, None)
    dy_keep.wait()
    dy_swap.wait()
    for index in range(n_groups):
        keep_group(index).wait()
        swap_group(index).wait()
    for save in saves:
        save.wait()


def attend_grad_kernel(n_dev, q_ref, kv_ref, da_ref, lse_ref, delta_ref, cos_ref, sin_ref, a_ref, dy_ref, z_ref, wo_ref,
                       q_scr, da_scr, kv_scr, qt_scr, dat_scr, dq_scr, dkv_scr, mate_scr, kv_local, kv_slots, a_scr, dy_scr, wo_local, wo_slots,
                       load_sems, kv_send, kv_recv, mate_send, mate_recv, wo_send, wo_recv):
    n_chip, chip, core, peers, partner = ring_place(n_dev)
    me = chip * 2 + core
    rows, head_dim = q_scr.shape[1:]
    n_seq, seq_len, kv_width = dkv_scr.shape
    half_len = seq_len // (2 * n_dev)
    num_heads = rows // half_len
    q_width = num_heads * head_dim
    key_len = PIECES_PER_BLOCK * half_len
    scale = LOG2_E * head_dim ** -0.5
    loads = [
        pltpu.make_async_copy(a_ref, a_scr, load_sems.at[0]),
        pltpu.make_async_copy(dy_ref, dy_scr, load_sems.at[1]),
        pltpu.make_async_copy(q_ref, q_scr, load_sems.at[2]),
        pltpu.make_async_copy(da_ref, da_scr, load_sems.at[3]),
        pltpu.make_async_copy(kv_ref, kv_scr, load_sems.at[4]),
    ]
    for load in loads:
        load.start()
    entry_barrier(peers + (partner,))
    loads[0].wait()
    loads[1].wait()

    def wo_local_term(step):
        n_sub, sub_len = wo_local.shape[1:3]
        way_len = n_sub * sub_len
        for way in range(2):
            first = chunk_at(chip, step, way, n_chip) * (2 * way_len) + way * way_len
            part = dot(a_scr[:, pl.ds(pl.multiple_of(first, way_len), way_len)], dy_scr[...], TN)
            for sub in range(n_sub):
                wo_local[way, sub] = part[sub * sub_len:(sub + 1) * sub_len, :]

    def piece_rows(dev, sub):
        piece = dev if sub == 0 else 2 * n_dev - 1 - dev
        return pl.ds(pl.multiple_of(piece * half_len, half_len), half_len)

    def mate_copy(step, way, sub):
        dev = chunk_at(chip, step, way, n_chip) * 2 + 1 - core
        return remote(dkv_scr.at[way, piece_rows(dev, sub)], mate_scr.at[way, step, sub], mate_send.at[way, step, sub], mate_recv.at[way, step, sub], partner)

    def kv_local_term(step):
        for sub in range(2):
            for way in range(2):
                mate_copy(step, way, sub).wait_recv()
                dev = chunk_at(chip, step, way, n_chip) * 2 + core
                kv_local[way, sub] = dkv_scr[way, piece_rows(dev, sub), :] + mate_scr[way, step, sub]

    wo_ring = RingReduce(n_chip, peers, wo_local_term, wo_local, wo_slots, wo_send, wo_recv, wo_ref)
    kv_ring = RingReduce(n_chip, peers, kv_local_term, kv_local, kv_slots, kv_send, kv_recv)

    front_blocks = lax.div(me, PIECES_PER_BLOCK) + 1
    all_blocks = 2 * n_dev // PIECES_PER_BLOCK + 1
    chunk_blocks = 3

    def block_of(seq, turn):
        group = jnp.where(turn >= front_blocks, 1, 0)
        step = turn - group * front_blocks
        index = 2 * seq + group
        piece = me + group * (2 * n_dev - 1 - 2 * me)
        start = pl.multiple_of(step * key_len, key_len)
        keys = pl.ds(start, key_len)

        @pl.when(step == 0)
        def _():
            dq_scr[...] = jnp.zeros_like(dq_scr)
            qt_scr[...] = q_scr[index].T
            dat_scr[...] = da_scr[index].T

        k_blk, v_blk = kv_scr[seq, keys, :head_dim], kv_scr[seq, keys, head_dim:]
        probs = jnp.exp2(dot(k_blk, qt_scr[...], NN) * scale - lse_ref[index])
        probs = jnp.where(causal_mask(probs.shape, start, piece * half_len, half_len), probs, 0.0)
        d_scores = (probs * (dot(v_blk, dat_scr[...], NN) - delta_ref[index])).astype(jnp.bfloat16)
        dq_scr[...] += dot(k_blk, d_scores, TN)
        dkv_scr[seq, keys, :head_dim] += dot(d_scores, q_scr[index], NN) * head_dim ** -0.5
        dkv_scr[seq, keys, head_dim:] += dot(probs.astype(jnp.bfloat16), da_scr[index], NN)

        @pl.when(step == lax.div(piece, PIECES_PER_BLOCK))
        def _():
            dq = dq_scr[...].T * head_dim ** -0.5
            out_rows = pl.ds(pl.multiple_of(index * half_len, half_len), half_len)
            cos_t, sin_t = cos_ref[out_rows, :], sin_ref[out_rows, :]
            for head in range(num_heads):
                dq_head = dq[head * half_len:(head + 1) * half_len, :]
                z_ref[out_rows, head * head_dim:(head + 1) * head_dim] = rotate_back(dq_head, cos_t, sin_t).astype(jnp.bfloat16)

    n_chunks = all_blocks // chunk_blocks

    def chunk(turn, _):
        seq, part = lax.div(turn, n_chunks), lax.rem(turn, n_chunks)
        lax.fori_loop(part * chunk_blocks, (part + 1) * chunk_blocks, lambda at, _: block_of(seq, at), None)
        for way in range(n_seq):
            @pl.when(turn == (way + 1) * n_chunks - 1)
            def _():
                def send_mate(step, _):
                    for sub in range(2):
                        mate_copy(step, way, sub).start()

                lax.fori_loop(0, n_chip, send_mate, None)

        step, sub = lax.div(turn, 2) + 1, lax.rem(turn, 2)

        @pl.when(sub == 0)
        def _():
            wo_local_term(step)

        wo_ring.serve(step, sub)

    wo_ring.first()
    dkv_scr[...] = jnp.zeros_like(dkv_scr)
    for load in loads[2:]:
        load.wait()
    lax.fori_loop(0, n_seq * n_chunks, chunk, None)
    kv_ring.first()
    wo_ring.middle(4)
    kv_ring.middle(1)

    def both(step, _):
        wo_ring.middle(step + 3)
        kv_ring.middle(step)

    lax.fori_loop(2, n_chip - 4, both, None)

    def keep_wo(way, sub):
        wo_ref[way, sub] = wo_slots[way, n_chip - 2, sub]

    wo_ring.last(keep_wo)
    lax.fori_loop(n_chip - 4, n_chip - 1, lambda step, _: kv_ring.middle(step), None)

    def keep_kv(way, sub):
        out_rows = slice((2 * way + sub) * half_len, (2 * way + sub + 1) * half_len)
        total = kv_slots[way, n_chip - 2, sub]
        z_ref[out_rows, q_width:q_width + head_dim] = rotate_back(total[:, :head_dim], cos_ref[out_rows, :], sin_ref[out_rows, :]).astype(jnp.bfloat16)
        z_ref[out_rows, q_width + head_dim:] = total[:, head_dim:].astype(jnp.bfloat16)

    kv_ring.last(keep_kv)

    def mates_sent(step, _):
        for way in range(2):
            for sub in range(2):
                mate_copy(step, way, sub).wait_send()

    lax.fori_loop(0, n_chip, mates_sent, None)


def finish_kernel(n_dev, h_ref, z_ref, wo_part_ref, a_ref, x_ref, dy_ref, gain_ref, wq_ref, wo_ref, wk_ref, wv_ref,
                  gz_ref, gwo_ref, y_ref, dx_ref, ggain_ref,
                  h_scr, z_scr, zf_scr, a_scr, x_scr, dy_scr, dh_scr, wq_buf, wo_buf, gain_slots, local_scr, slots,
                  load_sems, w_sems, swap_send, swap_recv, send_sems, recv_sems, g1_send, g1_recv, m1_send, m1_recv,
                  g2_send, g2_recv, m2_send, m2_recv, keep_sems, gain_send, gain_recv):
    n_chip, chip, core, peers, partner = ring_place(n_dev)
    me = chip * 2 + core
    n_rows, model_dim = h_ref.shape
    core_width = z_scr.shape[1]
    q_width = a_ref.shape[1]
    head_dim = wk_ref.shape[1]
    n_sub, sub_len = local_scr.shape[1:3]
    way_len = n_sub * sub_len
    wo_sub_len, wo_width = wo_part_ref.shape[2:]
    wo_way_len = n_sub * wo_sub_len
    blk = model_dim // n_chip
    mine, other = pl.ds(0, n_rows), pl.ds(n_rows, n_rows)

    def cols(which, size):
        return pl.ds(pl.multiple_of(which * size, size), size)

    def wq_load(index, slot):
        return pltpu.make_async_copy(wq_ref.at[cols(index, blk), :], wq_buf.at[slot], w_sems.at[0, slot])

    def wo_load(index, slot):
        return pltpu.make_async_copy(wo_ref.at[:, cols(index, blk)], wo_buf.at[slot], w_sems.at[1, slot])

    loads = [
        pltpu.make_async_copy(h_ref, h_scr.at[mine], load_sems.at[0]),
        pltpu.make_async_copy(z_ref.at[:, cols(core, core_width)], z_scr.at[mine], load_sems.at[1]),
        pltpu.make_async_copy(z_ref, zf_scr, load_sems.at[2]),
        pltpu.make_async_copy(a_ref.at[mine], a_scr, load_sems.at[3]),
        pltpu.make_async_copy(x_ref, x_scr, load_sems.at[4]),
        pltpu.make_async_copy(dy_ref, dy_scr, load_sems.at[5]),
    ]
    for load in loads:
        load.start()
    wq_load(0, 0).start()
    wo_load(0, 0).start()
    barrier = pltpu.get_barrier_semaphore()
    for offset in range(1, n_dev):
        pl.semaphore_signal(barrier, inc=1, device_id={'cp': lax.rem(me + offset, n_dev)}, device_id_type=pl.DeviceIdType.MESH)
    pl.semaphore_wait(barrier, n_dev - 1)

    def wo_place(step, way, sub):
        first = owner_at(chip, step, way, n_chip) * (2 * wo_way_len) + way * wo_way_len + sub * wo_sub_len
        return gwo_ref.at[pl.ds(pl.multiple_of(first, wo_sub_len), wo_sub_len), cols(core, wo_width)]

    def z_place(step, way, sub):
        first = owner_at(chip, step, way, n_chip) * (2 * way_len) + way * way_len + sub * sub_len
        return gz_ref.at[pl.ds(pl.multiple_of(first, sub_len), sub_len), cols(core, core_width)]

    swaps = [
        remote(h_ref, h_scr.at[other], swap_send.at[0], swap_recv.at[0], partner),
        remote(z_ref.at[:, cols(1 - core, core_width)], z_scr.at[other], swap_send.at[1], swap_recv.at[1], partner),
    ]
    for swap in swaps:
        swap.start()
    wo_gather = RingGather(n_chip, peers, partner, lambda way, sub: wo_part_ref.at[way, sub], wo_place, n_sub, g1_send, g1_recv, m1_send, m1_recv)
    z_gather = RingGather(n_chip, peers, partner, lambda way, sub: slots.at[way, n_chip - 2, sub], z_place, n_sub, g2_send, g2_recv, m2_send, m2_recv)
    keeps = ([pltpu.make_async_copy(wo_part_ref.at[way, sub], wo_place(0, way, sub), keep_sems.at[0, way, sub]) for sub, way in wo_gather.each],
             [pltpu.make_async_copy(slots.at[way, n_chip - 2, sub], z_place(0, way, sub), keep_sems.at[1, way, sub]) for sub, way in wo_gather.each])
    wo_gather.first()
    for keep in keeps[0]:
        keep.start()

    def local_term(step):
        for way in range(2):
            first = chunk_at(chip, step, way, n_chip) * (2 * way_len) + way * way_len
            part = dot(h_scr[:, pl.ds(pl.multiple_of(first, way_len), way_len)], z_scr[...], TN)
            for sub in range(n_sub):
                local_scr[way, sub] = part[sub * sub_len:(sub + 1) * sub_len, :]

    z_ring = RingReduce(n_chip, peers, local_term, local_scr, slots, send_sems, recv_sems)

    def d_hidden(index, slot):
        wq_load(index, slot).wait()

        @pl.when(index + 1 < n_chip)
        def _():
            wq_load(index + 1, 1 - slot).start()

        rows = cols(index, blk)
        dh_scr[:, rows] = (dot(zf_scr[:, :q_width], wq_buf[slot], NT) + dot(zf_scr[:, q_width:q_width + head_dim], wk_ref[rows, :], NT)
                           + dot(zf_scr[:, q_width + head_dim:], wv_ref[rows, :], NT))

    def out_block(index, slot):
        wo_load(index, slot).wait()

        @pl.when(index + 1 < n_chip)
        def _():
            wo_load(index + 1, 1 - slot).start()

        where = cols(index, blk)
        o_blk = dot(a_scr[...], wo_buf[slot], NN).astype(jnp.bfloat16)
        y_ref[:, where] = (x_scr[:, where].astype(jnp.float32) + o_blk.astype(jnp.float32)).astype(jnp.bfloat16)

    def norm_grad(index, _):
        rows = pl.ds(pl.multiple_of(index * 32, 32), 32)
        x_float = x_scr[rows, :].astype(jnp.float32)
        centered = x_float - jnp.mean(x_float, axis=-1, keepdims=True)
        inv_std = lax.rsqrt(jnp.mean(centered * centered, axis=-1, keepdims=True) + NORM_EPS)
        x_hat = centered * inv_std
        d_h = dh_scr[rows, :]
        gain_slots[me] += jnp.sum(d_h * x_hat, axis=0, keepdims=True)
        d_hat = d_h * gain_ref[...]
        mean_d = jnp.mean(d_hat, axis=-1, keepdims=True)
        mean_dx = jnp.mean(d_hat * x_hat, axis=-1, keepdims=True)
        dx_ref[rows, :] = (dy_scr[rows, :].astype(jnp.float32) + inv_std * (d_hat - mean_d - x_hat * mean_dx)).astype(jnp.bfloat16)

    def gain_copy(offset):
        return remote(gain_slots.at[me], gain_slots.at[me], gain_send.at[offset], gain_recv.at[offset], lax.rem(me + offset, n_dev))

    loads[0].wait()
    loads[1].wait()
    for swap in swaps:
        swap.wait_recv()
    z_ring.first()
    for load in loads[2:]:
        load.wait()
    wo_gather.middle(1)
    z_ring.middle(1)
    d_hidden(0, 0)

    def phase_one(step, _):
        wo_gather.middle(step)
        z_ring.middle(step)
        d_hidden(step - 1, lax.rem(step - 1, 2))

    lax.fori_loop(2, n_chip - 1, phase_one, None)
    wo_gather.last()

    def pass_on(way, sub):
        z_gather.start_first(way, sub)
        keeps[1][2 * sub + way].start()

    z_ring.last(pass_on)
    d_hidden(n_chip - 2, (n_chip - 2) % 2)
    d_hidden(n_chip - 1, (n_chip - 1) % 2)
    gain_slots[me] = jnp.zeros(gain_slots.shape[1:], jnp.float32)
    lax.fori_loop(0, n_rows // 32, norm_grad, None)
    for offset in range(1, n_dev):
        gain_copy(offset).start()
    z_gather.middle(1)
    out_block(0, 0)
    out_block(1, 1)

    def phase_two(step, _):
        z_gather.middle(step)
        out_block(step, lax.rem(step, 2))

    lax.fori_loop(2, n_chip - 1, phase_two, None)
    out_block(n_chip - 1, (n_chip - 1) % 2)
    z_gather.last()
    for offset in range(1, n_dev):
        gain_copy(offset).wait_recv()
    total = gain_slots[0]
    for dev in range(1, n_dev):
        total = total + gain_slots[dev]
    ggain_ref[...] = total
    wo_gather.drain()
    z_gather.drain()
    for keep in keeps[0] + keeps[1]:
        keep.wait()
    for swap in swaps:
        swap.wait_send()
    for offset in range(1, n_dev):
        gain_copy(offset).wait_send()


def deliver_kernel(gz_ref, gwo_ref, y_ref, dx_ref, wq_out, wk_out, wv_out, wo_out, y_out, dx_out, gz_buf, gwo_buf, y_buf, dx_buf, in_sems, out_sems):
    n_blk, z_len, _ = gz_buf.shape
    wo_len = gwo_buf.shape[1]
    q_width, head_dim = wq_out.shape[1], wk_out.shape[1]
    jobs = []
    for i in range(n_blk):
        rows = pl.ds(i * z_len, z_len)
        parts = [(gz_buf.at[i, :, pl.ds(first, out.shape[1])], out.at[rows]) for out, first in ((wq_out, 0), (wk_out, q_width), (wv_out, q_width + head_dim))]
        jobs.append((gz_ref.at[rows], gz_buf.at[i], parts))
        rows = pl.ds(i * wo_len, wo_len)
        jobs.append((gwo_ref.at[rows], gwo_buf.at[i], [(gwo_buf.at[i], wo_out.at[rows])]))
    for src, buf, out in ((y_ref, y_buf, y_out), (dx_ref, dx_buf, dx_out)):
        jobs.append((src, buf, [(buf, out)]))
    reads = [pltpu.make_async_copy(src, buf, in_sems.at[i]) for i, (src, buf, _) in enumerate(jobs)]
    for read in reads:
        read.start()
    writes = []
    for read, (_, _, parts) in zip(reads, jobs):
        read.wait()
        for src, dst in parts:
            writes.append(pltpu.make_async_copy(src, dst, out_sems.at[len(writes)]))
            writes[-1].start()
    for write in writes:
        write.wait()


def solution(mesh):
    n_dev = mesh.shape['cp']
    n_chip, n_sub = n_dev // 2, 2

    def local_fn(tokens, positions, norm_gain, w_query, w_key, w_value, w_out, d_out):
        n_seq, blk_len, model_dim = tokens.shape
        head_dim = w_key.shape[1]
        num_heads = w_query.shape[1] // head_dim
        q_width, kv_width = num_heads * head_dim, 2 * head_dim
        half_len, half = blk_len // 2, head_dim // 2
        n_rows, n_groups = n_seq * blk_len, 2 * n_seq
        rows = num_heads * half_len
        seq_len = n_dev * blk_len
        bf16, f32 = jnp.bfloat16, jnp.float32
        dma = pltpu.SemaphoreType.DMA
        vmem = pl.BlockSpec(memory_space=pltpu.VMEM)
        hbm = pl.BlockSpec(memory_space=pl.ANY)
        params = pltpu.CompilerParams(vmem_limit_bytes=VMEM_LIMIT)

        def comm(ident):
            return pltpu.CompilerParams(vmem_limit_bytes=VMEM_LIMIT, collective_id=ident, has_side_effects=True)

        def shape(*dims, dtype=bf16):
            return jax.ShapeDtypeStruct(dims, dtype)

        def gather_sems():
            return [dma((2, n_sub)), dma((2, n_chip - 1, n_sub)), dma((2, n_sub)), dma((2, n_chip, n_sub))]

        x_flat = tokens.reshape(n_rows, model_dim)
        dy_flat = d_out.reshape(n_rows, model_dim)
        gain_row = norm_gain.reshape(1, model_dim)
        cos_t, sin_t = rope_tables(positions.reshape(n_rows), head_dim)
        h_flat, kv_flat = pl.pallas_call(
            norm_kv_kernel,
            out_shape=(shape(n_rows, model_dim), shape(n_rows, kv_width)),
            compiler_params=params, name='norm_kv',
        )(x_flat, gain_row, w_key, w_value, cos_t, sin_t)

        groups = (n_groups, rows, head_dim)
        kv_all, q_rows, da_rows, attn_chip, dy_chip, lse, delta = pl.pallas_call(
            functools.partial(forward_kernel, n_dev),
            in_specs=[vmem, vmem, vmem, hbm, hbm, hbm, hbm],
            out_specs=[hbm, hbm, hbm, hbm, hbm, vmem, vmem],
            out_shape=(shape(n_seq, seq_len, kv_width), shape(*groups), shape(*groups), shape(2 * n_rows, q_width), shape(2 * n_rows, model_dim // 2),
                       shape(n_groups, 1, rows, dtype=f32), shape(n_groups, 1, rows, dtype=f32)),
            scratch_shapes=[pltpu.VMEM((n_rows, model_dim), bf16), pltpu.VMEM((n_rows, model_dim), bf16), pltpu.VMEM((n_seq, seq_len, kv_width), bf16),
                            pltpu.VMEM(groups, bf16), pltpu.VMEM(groups, bf16), pltpu.VMEM((n_groups, head_dim, rows), bf16), pltpu.VMEM((n_rows, q_width), bf16),
                            pltpu.VMEM((n_groups, head_dim, rows), f32), pltpu.VMEM((n_groups, 1, rows), f32), pltpu.VMEM((n_groups, 1, rows), f32),
                            pltpu.VMEM((2, model_dim, head_dim), bf16), pltpu.VMEM((2, head_dim, model_dim), bf16),
                            dma((3,)), dma((3 + n_groups,)), dma((2, 2)), dma((n_groups + 1,)), dma((n_groups + 1,))] + gather_sems(),
            compiler_params=comm(0), name='forward',
        )(kv_flat, cos_t, sin_t, h_flat, dy_flat, w_query, w_out)

        z_width = q_width + kv_width
        wo_cols, wo_sub = model_dim // 2, q_width // (2 * n_chip * n_sub)
        z_flat, wo_part = pl.pallas_call(
            functools.partial(attend_grad_kernel, n_dev),
            in_specs=[hbm, hbm, hbm, vmem, vmem, vmem, vmem, hbm, hbm],
            out_specs=[vmem, vmem],
            out_shape=(shape(n_rows, z_width), shape(2, n_sub, wo_sub, wo_cols, dtype=f32)),
            scratch_shapes=[pltpu.VMEM((n_groups, rows, head_dim), bf16), pltpu.VMEM((n_groups, rows, head_dim), bf16),
                            pltpu.VMEM((n_seq, seq_len, kv_width), bf16), pltpu.VMEM((head_dim, rows), bf16), pltpu.VMEM((head_dim, rows), bf16), pltpu.VMEM((head_dim, rows), f32),
                            pltpu.VMEM((n_seq, seq_len, kv_width), f32), pltpu.VMEM((2, n_chip, 2, half_len, kv_width), f32),
                            pltpu.VMEM((2, 2, half_len, kv_width), f32), pltpu.VMEM((2, n_chip - 1, 2, half_len, kv_width), f32),
                            pltpu.VMEM((2 * n_rows, q_width), bf16), pltpu.VMEM((2 * n_rows, wo_cols), bf16),
                            pltpu.VMEM((2, n_sub, wo_sub, wo_cols), f32), pltpu.VMEM((2, n_chip - 1, n_sub, wo_sub, wo_cols), f32),
                            dma((5,)), dma((2, 2)), dma((2, n_chip - 1, 2)), dma((2, n_chip, 2)), dma((2, n_chip, 2)),
                            dma((2, n_sub)), dma((2, n_chip - 1, n_sub))],
            compiler_params=comm(1), name='attend_grad',
        )(q_rows, kv_all, da_rows, lse, delta, cos_t, sin_t, attn_chip, dy_chip)

        core_width, sub_len = z_width // 2, model_dim // (2 * n_chip * n_sub)
        blk = model_dim // n_chip
        grad_z, grad_wo, out_y, grad_x, grad_gain = pl.pallas_call(
            functools.partial(finish_kernel, n_dev),
            in_specs=[hbm] * 6 + [vmem, hbm, hbm, vmem, vmem],
            out_specs=[pl.BlockSpec(memory_space=pltpu.HBM), hbm, vmem, vmem, vmem],
            out_shape=(shape(model_dim, z_width, dtype=f32), shape(q_width, model_dim, dtype=f32), shape(n_rows, model_dim), shape(n_rows, model_dim),
                       shape(1, model_dim, dtype=f32)),
            scratch_shapes=[pltpu.VMEM((2 * n_rows, model_dim), bf16), pltpu.VMEM((2 * n_rows, core_width), bf16), pltpu.VMEM((n_rows, z_width), bf16),
                            pltpu.VMEM((n_rows, q_width), bf16), pltpu.VMEM((n_rows, model_dim), bf16), pltpu.VMEM((n_rows, model_dim), bf16),
                            pltpu.VMEM((n_rows, model_dim), f32), pltpu.VMEM((2, blk, q_width), bf16), pltpu.VMEM((2, q_width, blk), bf16),
                            pltpu.VMEM((n_dev, 1, model_dim), f32), pltpu.VMEM((2, n_sub, sub_len, core_width), f32),
                            pltpu.VMEM((2, n_chip - 1, n_sub, sub_len, core_width), f32),
                            dma((6,)), dma((2, 2)), dma((2,)), dma((2,)), dma((2, n_sub)), dma((2, n_chip - 1, n_sub))]
            + gather_sems() + gather_sems() + [dma((2, 2, n_sub)), dma((n_dev,)), dma((n_dev,))],
            compiler_params=comm(2), name='finish',
        )(h_flat, z_flat, wo_part, attn_chip, x_flat, dy_flat, gain_row, w_query, w_out, w_key, w_value)
        n_blk = n_dev
        grad_wq, grad_wk, grad_wv, grad_wo, out_y, grad_x = pl.pallas_call(
            deliver_kernel,
            in_specs=[hbm] * 4,
            out_specs=[hbm] * 6,
            out_shape=(shape(model_dim, q_width, dtype=f32), shape(model_dim, head_dim, dtype=f32), shape(model_dim, head_dim, dtype=f32),
                       shape(q_width, model_dim, dtype=f32), shape(n_rows, model_dim), shape(n_rows, model_dim)),
            scratch_shapes=[pltpu.VMEM((n_blk, model_dim // n_blk, z_width), f32), pltpu.VMEM((n_blk, q_width // n_blk, model_dim), f32),
                            pltpu.VMEM((n_rows, model_dim), bf16), pltpu.VMEM((n_rows, model_dim), bf16),
                            dma((2 * n_blk + 2,)), dma((4 * n_blk + 2,))],
            compiler_params=params, name='deliver',
        )(grad_z, grad_wo, out_y, grad_x)
        return out_y.reshape(tokens.shape), grad_x.reshape(tokens.shape), grad_wq, grad_wk, grad_wv, grad_wo, grad_gain.reshape(model_dim)

    seq_spec = P('dp', 'cp', None)
    rep_spec = P(None, None)
    part_spec = P('dp', None)
    return jax.shard_map(local_fn, mesh=mesh,
                         in_specs=(seq_spec, P('dp', 'cp'), P(None), rep_spec, rep_spec, rep_spec, rep_spec, seq_spec),
                         out_specs=(seq_spec, seq_spec, part_spec, part_spec, part_spec, part_spec, P('dp')),
                         check_vma=False)
```
